32 devices in a mesh: dom: 8 (over z, y), rep: 4 (over x, core).
Axes of the slice: x: 2, y: 2, z: 4, core: 2. Of those that a mesh axis runs over, the one named last changes fastest.
Arguments:
- ns_shape: bfloat16 [64, 256], replicated, may hold values from -0.75 to 0.75
- nm_shape: bfloat16 [64, 256], replicated, may hold values from -0.75 to 0.75
- sec_disp: bfloat16 [64, 262144], P(None, ('dom', 'rep')), may hold values from -6 to 6
- mst_disp: bfloat16 [64, 262144], P(None, ('dom', 'rep')), may hold values from -6 to 6
- gap_offset: float32 [262144], P(('dom', 'rep')), may hold values from -6 to 6
- quad_weight: float32 [256], replicated, may hold values from 0.25 to 4
- jacobian: float32 [262144], P(('dom', 'rep')), may hold values from 0.0005 to 0.005
- segment_slot: int32 [262144], P(('dom', 'rep')), may hold values from 0 to 1279, as said below
- face_id: int32 [262144], P(('dom', 'rep')), may hold values from 0 to 1073741823
- search_rank: int32 [262144], P(('dom', 'rep')), may hold values from 0 to 3
- live_rows: int32 [32], P(('dom', 'rep')), may hold values from 1024 to 8192, as said below
Outputs:
- contact_force: bfloat16 [64, 262144], P(None, ('dom', 'rep'))
- seg_pen: float32 [8192], P('dom')
- seg_face: int32 [8192], P('dom')
- seg_gap: float32 [8192], P('dom')
- mean_gap: float32 [], replicated
The draws below stay inside these ranges and needn't reach their ends.
Inputs may be any that keep to these rules, and one draw needn't show every extreme that they name: `segment_slot`: A row's segment is (1024 times the dom index of its device plus its slot) modulo 8192; slots of 1024 or more reach the next dom index's first 256 segments. `live_rows`: entry b counts the live rows of the device with flat index b (dom-major); they are that device's first rows, the rest are padding; some device is full in every draw.
All inputs are finite; a program needn't handle non-finite values.
Results may differ from the reference program's by a relative error of at most 0.0055.
Values sent between devices are 32-bit elements; how exact they have to be, the bound alone decides.
A program may use at most 64 MiB of HBM per device.

```python
import math
import jax
import jax.numpy as jnp
from jax import lax

P_SIZE = 256
K = 64
ROWS_DEV = 8192
SEG_DEV = 1024
SPILL = 256
SEGS = 8192
ROWS = 262144
N_REP = 4
DEVICES = 32


def draw_live_rows(key, part):
    first_key = jax.random.fold_in(key, 11)
    second_key = jax.random.fold_in(key, 23)
    counts = jax.random.randint(first_key, (DEVICES,), ROWS_DEV // 8, ROWS_DEV + 1, dtype=jnp.int32)
    full_device = jax.random.randint(second_key, (), 0, DEVICES, dtype=jnp.int32)
    return jnp.where(jnp.arange(DEVICES, dtype=jnp.int32) == full_device, ROWS_DEV, counts).astype(jnp.int32)


def draw_segment_slot(key, part):
    window_len = SEG_DEV + SPILL
    dom_count = DEVICES // N_REP
    vacant = jax.random.randint(jax.random.fold_in(key, 31), (SEGS,), 0, 8, dtype=jnp.int32) == 0
    forced = jax.random.randint(jax.random.fold_in(key, 37), (), 0, SEGS, dtype=jnp.int32)
    vacant = vacant | (jnp.arange(SEGS, dtype=jnp.int32) == forced)
    dom_ids = jnp.arange(dom_count, dtype=jnp.int32)
    window_ids = ((dom_ids[:, None] * SEG_DEV + jnp.arange(window_len, dtype=jnp.int32)[None, :]) % SEGS).astype(jnp.int32)
    blocked = vacant[window_ids].astype(jnp.int32)
    order = jnp.argsort(blocked, axis=1, stable=True).astype(jnp.int32)
    allowed = jnp.maximum(window_len - jnp.sum(blocked, axis=1), 1).astype(jnp.int32)
    row_dom = (jnp.arange(ROWS, dtype=jnp.int32) // (ROWS_DEV * N_REP)).astype(jnp.int32)
    raw_pick = jax.random.randint(jax.random.fold_in(key, 41), (ROWS,), 0, 1 << 24, dtype=jnp.int32)
    pick = (raw_pick % allowed[row_dom]).astype(jnp.int32)
    return order[row_dom, pick].astype(jnp.int32)


def set_ends(drawn, own_key, least, top_value):
    longest = drawn.shape.index(max(drawn.shape))
    spots = []
    for shift in (0, 1):
        where = [jax.random.randint(jax.random.fold_in(own_key, axis), (), 0, length) for axis, length in enumerate(drawn.shape)]
        where[longest] = (where[longest] + shift) % drawn.shape[longest]
        spots.append(tuple(where))
    return drawn.at[spots[0]].set(least).at[spots[1]].set(top_value)


def levels(stream_key, extent, cuts, least, high):
    level, own = 1.0, jax.random.fold_in(stream_key, 6)
    for dim, shards_of in cuts:
        steps = jnp.exp(jax.random.uniform(jax.random.fold_in(own, dim), (shards_of,), jnp.float32, least / len(cuts), high / len(cuts)))
        level = level * jnp.repeat(steps, extent[dim] // shards_of).reshape([-1 if axis == dim else 1 for axis in range(len(extent))])
    return level


def centred(key, extent, scale, most, pieces=(), held_as=jnp.bfloat16):
    result = scale * jax.random.normal(key, extent, jnp.float32)
    if pieces:
        result = result * levels(key, extent, pieces, -0.22, 0.18)
    return jnp.clip(result, -most, most).astype(held_as)


def setup_inputs(seed: int = 0) -> dict:
    key_of = jax.random.split(jax.random.key(seed), 12)
    return {
        "ns_shape": centred(key_of[0], (K, P_SIZE), K ** -0.5, 0.75),
        "nm_shape": centred(key_of[1], (K, P_SIZE), K ** -0.5, 0.75),
        "sec_disp": centred(key_of[2], (K, ROWS), 1.0, 6.0, ((1, 32),)),
        "mst_disp": centred(key_of[3], (K, ROWS), 1.0, 6.0, ((1, 32),)),
        "gap_offset": centred(key_of[4], (ROWS,), 1.0, 6.0, ((0, 32),), jnp.float32),
        "quad_weight": jnp.clip(jnp.exp(jax.random.uniform(key_of[5], (P_SIZE,), jnp.float32, math.log(0.25), math.log(4.0))), 0.25, 4.0),
        "jacobian": jnp.clip(jnp.exp(math.log(0.005) - 2.30258502 * jax.random.uniform(key_of[6], (ROWS,), jnp.float32) ** levels(key_of[6], (ROWS,), ((0, 32),), -0.2, 0.2)), 0.0005, 0.005),
        "segment_slot": draw_segment_slot(jax.random.fold_in(key_of[11], 71), 0),
        "face_id": set_ends(jax.random.randint(key_of[8], (ROWS,), 0, 1073741824), jax.random.fold_in(key_of[8], 1), 0, 1073741823).astype(jnp.int32),
        "search_rank": set_ends(jax.random.randint(key_of[9], (ROWS,), 0, 4), jax.random.fold_in(key_of[9], 1), 0, 3).astype(jnp.int32),
        "live_rows": draw_live_rows(jax.random.fold_in(key_of[11], 71), 0),
    }


PENALTY = 400.0
LOWEST_FILL = -1.0e30
FACE_LIMIT = 1073741824


def project(shape_table, displace):
    return lax.dot_general(shape_table, displace, (((0,), (0,)), ((), ())), preferred_element_type=jnp.float32)


def window_stats(gap_field, jac_row, weights, slots, faces, ranks, live, window_len):
    row_pen = jnp.max(-gap_field, axis=0)
    row_gap = jac_row * jnp.dot(weights, gap_field, precision=lax.Precision.HIGHEST)
    row_area = jac_row * jnp.sum(weights)
    penalty_max = jnp.maximum(jax.ops.segment_max(jnp.where(live, row_pen, LOWEST_FILL), slots, num_segments=window_len), LOWEST_FILL)
    best_rank = jnp.maximum(jax.ops.segment_max(jnp.where(live, ranks, -1), slots, num_segments=window_len), -1).astype(jnp.int32)
    chosen = jnp.where(live & (ranks == best_rank[slots]), faces, FACE_LIMIT).astype(jnp.int32)
    lowest_face = jnp.minimum(jax.ops.segment_min(chosen, slots, num_segments=window_len), FACE_LIMIT).astype(jnp.int32)
    gap_sum = jax.ops.segment_sum(jnp.where(live, row_gap, 0.0), slots, num_segments=window_len)
    area_sum = jax.ops.segment_sum(jnp.where(live, row_area, 0.0), slots, num_segments=window_len)
    return penalty_max, best_rank, lowest_face, gap_sum, area_sum


def reference(ns_shape, nm_shape, sec_disp, mst_disp, gap_offset, quad_weight, jacobian, segment_slot, face_id, search_rank, live_rows):
    row_count = ROWS_DEV
    window_len = SEG_DEV + SPILL

    def blocks(values):
        return values.reshape(DEVICES, row_count)

    sec_blocks = sec_disp.reshape(K, DEVICES, row_count).transpose(1, 0, 2)
    mst_blocks = mst_disp.reshape(K, DEVICES, row_count).transpose(1, 0, 2)

    def one_block(block):
        sec_part, mst_part, offset, jac_row, slots, faces, ranks, live_count = block
        gap_field = project(ns_shape, sec_part) - project(nm_shape, mst_part) + offset[None, :]
        live = jnp.arange(row_count, dtype=jnp.int32) < live_count
        load = jnp.where(live[None, :], quad_weight[:, None] * jac_row[None, :] * PENALTY * jnp.maximum(-gap_field, 0.0), 0.0).astype(jnp.bfloat16)
        force = jnp.dot(ns_shape, load, preferred_element_type=jnp.float32).astype(jnp.bfloat16)
        stats = window_stats(gap_field, jac_row, quad_weight, slots, faces, ranks, live, window_len)
        return (force,) + stats

    outputs = lax.map(one_block, (sec_blocks, mst_blocks, blocks(gap_offset), blocks(jacobian), blocks(segment_slot), blocks(face_id), blocks(search_rank), live_rows))
    force_blocks, penalty_max, best_rank, lowest_face, gap_sum, area_sum = outputs
    contact_force = force_blocks.transpose(1, 0, 2).reshape(K, DEVICES * row_count)
    dom_index = (jnp.arange(DEVICES, dtype=jnp.int32) // N_REP).astype(jnp.int32)
    seg_ids = ((dom_index[:, None] * SEG_DEV + jnp.arange(window_len, dtype=jnp.int32)[None, :]) % SEGS).astype(jnp.int32).reshape(-1)
    seg_max = jnp.maximum(jax.ops.segment_max(penalty_max.reshape(-1), seg_ids, num_segments=SEGS), LOWEST_FILL)
    seg_rank = jnp.maximum(jax.ops.segment_max(best_rank.reshape(-1), seg_ids, num_segments=SEGS), -1).astype(jnp.int32)
    chosen = jnp.where(best_rank.reshape(-1) == seg_rank[seg_ids], lowest_face.reshape(-1), FACE_LIMIT).astype(jnp.int32)
    seg_low = jnp.minimum(jax.ops.segment_min(chosen, seg_ids, num_segments=SEGS), FACE_LIMIT).astype(jnp.int32)
    seg_pen = jnp.where(seg_rank < 0, jnp.float32(0.0), seg_max)
    seg_face = jnp.where(seg_rank < 0, -1, seg_low).astype(jnp.int32)
    seg_gap = jax.ops.segment_sum(gap_sum.reshape(-1), seg_ids, num_segments=SEGS)
    mean_gap = jnp.sum(gap_sum) / jnp.sum(area_sum)
    return contact_force, seg_pen, seg_face, seg_gap, mean_gap
```

```python
import functools

import jax
import jax.numpy as jnp
from jax import lax
from jax.experimental import pallas as pl
from jax.experimental.pallas import tpu as pltpu
from jax.sharding import PartitionSpec as P

SEG_DEV = 1024
SPILL = 256
LANES = 128
SUB = 8
GROUPS = (SEG_DEV + SPILL) // LANES
OWN_GROUPS = SEG_DEV // LANES
SPILL_GROUPS = SPILL // LANES
PAD_GROUPS = 16

PENALTY = 400.0
LOWEST_FILL = -1e30
FACE_LIMIT = 1073741824
FACE_MASK = FACE_LIMIT - 1
KEY_LOW = -2147483648
MESH = pl.DeviceIdType.MESH
TILE = 256
DEPTH = 16
UNROLL = 16
EXTRA = 16


def split3(x):
    a = x.astype(jnp.bfloat16)
    rest = x - a.astype(jnp.float32)
    b = rest.astype(jnp.bfloat16)
    c = (rest - b.astype(jnp.float32)).astype(jnp.bfloat16)
    return a, b, c


def row(ref, at):
    return ref[pl.ds(at, SUB, stride=0), :]


def pull_groups(gs, depth0, depth, code_ref, slot_ref, pen_ref, key_ref, packs):
    all_lines = code_ref.shape[0]
    blocks = depth // SUB
    sub = lax.broadcasted_iota(jnp.int32, (SUB, LANES), 0)
    wants = [(sub + (depth0 + SUB * b)) * PAD_GROUPS + g for g in gs for b in range(blocks)]
    count = len(wants)

    def pull(i, carry):
        los, pens, keys = (list(part) for part in carry)
        code, slot, pen, key = (row(ref, i) for ref in (code_ref, slot_ref, pen_ref, key_ref))
        for b in range(count):
            hit = code == wants[b]
            los[b] = jnp.where(hit, slot, los[b])
            pens[b] = jnp.where(hit, pen, pens[b])
            keys[b] = jnp.where(hit, key, keys[b])
        return tuple(los), tuple(pens), tuple(keys)

    none = jnp.full((SUB, LANES), -1, jnp.int32)
    empty = jnp.full((SUB, LANES), LOWEST_FILL, jnp.float32)
    start = ((none,) * count, (empty,) * count, (none,) * count)
    pulled = lax.fori_loop(0, all_lines, pull, start, unroll=8)
    for ref, parts in zip(packs, pulled):
        for b in range(count):
            ref[SUB * b : SUB * (b + 1), :] = parts[b]


def match_group(g, at, depth, packs):
    lane_lo, lane_pen, lane_key = packs
    sub = lax.broadcasted_iota(jnp.int32, (SUB, LANES), 0)
    empty = jnp.full((SUB, LANES), LOWEST_FILL, jnp.float32)
    low = jnp.full((SUB, LANES), KEY_LOW, jnp.int32)
    tiles = LANES // SUB
    half = tiles // 2
    pens, keys = [], []
    for part in range(2):
        marks = [sub + (g * LANES + SUB * (part * half + q)) for q in range(half)]
        best_pen, best_key = [empty] * half, [low] * half
        for j in range(depth):
            lo, pen, key = row(lane_lo, at + j), row(lane_pen, at + j), row(lane_key, at + j)
            for q in range(half):
                hit = lo == marks[q]
                best_pen[q] = jnp.maximum(best_pen[q], jnp.where(hit, pen, LOWEST_FILL))
                best_key[q] = jnp.maximum(best_key[q], jnp.where(hit, key, KEY_LOW))
        pens += best_pen
        keys += best_key
    top = jnp.max(jnp.concatenate(pens, axis=0).T, axis=0, keepdims=True)
    best = jnp.max(jnp.concatenate(keys, axis=0).T, axis=0, keepdims=True)
    return top, best


def project(wt, x_ref, off_ref, tile):
    cols = pl.ds(tile * TILE, TILE)
    per_tile = TILE // LANES
    offset = jnp.concatenate([row(off_ref, tile * per_tile + i) for i in range(per_tile)], axis=1)
    sub = lax.broadcasted_iota(jnp.int32, (SUB, TILE), 0)
    a, b, c = (part.astype(jnp.float32) for part in split3(offset))
    extra = jnp.where(sub == 0, a, jnp.where(sub == 1, b, jnp.where(sub == 2, c, 0.0)))
    extra = jnp.concatenate([extra, jnp.zeros((EXTRA - SUB, TILE), jnp.float32)], axis=0)
    x = jnp.concatenate([x_ref[:, cols], extra.astype(jnp.bfloat16)], axis=0)
    return jnp.dot(wt, x, preferred_element_type=jnp.float32)


def store_pen(pen_ref, tile, gap):
    per_tile = TILE // LANES
    pen = -jnp.min(gap, axis=0, keepdims=True)
    for i in range(per_tile):
        pen_ref[pl.ds(tile * per_tile + i, 1), :] = pen[:, i * LANES : (i + 1) * LANES]


def prep_kernel(
    live_h, ns_h, nm_h, qw_h, sec_h, mst_h, off_h, jac_h, slot_h, face_h, rank_h,
    x_ref, wt_ref, nq_ref, off_ref, jl_ref, slot_ref, code_ref, key_ref, over_pen, over_key, area_ref,
    live_s, ns_ref, nm_ref, qw_ref, jac_ref, face_ref, rank_ref, pen_ref, packs, s_small, s_big,
):
    lines = slot_ref.shape[0]
    k_size, p_size = ns_ref.shape
    rows = x_ref.shape[1]

    small = [
        pltpu.make_async_copy(source, held, s_small.at[i])
        for i, (source, held) in enumerate((
            (slot_h, slot_ref), (live_h, live_s), (ns_h, ns_ref), (nm_h, nm_ref), (qw_h, qw_ref),
            (face_h, face_ref), (rank_h, rank_ref), (jac_h, jac_ref), (off_h, off_ref),
        ))
    ]
    for copy in small:
        copy.start()
    parts = 4
    for i in range(parts):
        cols = pl.ds(i * (rows // parts), rows // parts)
        pltpu.make_async_copy(sec_h.at[:, cols], x_ref.at[0:k_size, cols], s_big).start()
        pltpu.make_async_copy(mst_h.at[:, cols], x_ref.at[k_size:, cols], s_big).start()
    for copy in small:
        copy.wait()

    row_id = (
        lax.broadcasted_iota(jnp.int32, (lines, LANES), 0) * LANES
        + lax.broadcasted_iota(jnp.int32, (lines, LANES), 1)
    )
    alive = row_id < live_s[0]
    group = jnp.where(alive, slot_ref[...] >> 7, -1)
    before = (
        lax.broadcasted_iota(jnp.int32, (lines, lines), 1)
        < lax.broadcasted_iota(jnp.int32, (lines, lines), 0)
    )
    before = jnp.where(before, 1.0, 0.0).astype(jnp.bfloat16)
    code = jnp.full((lines, LANES), -1, jnp.int32)
    for g in range(GROUPS):
        mine = group == g
        place = jnp.dot(
            before, jnp.where(mine, 1.0, 0.0).astype(jnp.bfloat16),
            preferred_element_type=jnp.float32,
        ).astype(jnp.int32)
        code = jnp.where(mine, place * PAD_GROUPS + g, code)
    code_ref[...] = code
    worst = jnp.max(code)

    w = jnp.concatenate([ns_ref[...], -nm_ref[...]], axis=0).astype(jnp.float32)
    qrow = qw_ref[...]
    wt = w.T
    qmat = jnp.broadcast_to(qrow, (LANES, p_size)).T
    v = jnp.sum(wt * qmat, axis=0, keepdims=True)
    qsum = jnp.sum(qmat, axis=0, keepdims=True)
    depth = wt_ref.shape[1]
    pick = lax.broadcasted_iota(jnp.int32, (EXTRA, depth), 0)
    column = lax.broadcasted_iota(jnp.int32, (p_size, depth - 2 * k_size), 1)
    wt_ref[0:p_size, 0 : 2 * k_size] = wt.astype(jnp.bfloat16)
    wt_ref[0:p_size, 2 * k_size :] = jnp.where(column < 3, 1.0, 0.0).astype(jnp.bfloat16)
    lane_row = lax.broadcasted_iota(jnp.int32, (1, LANES), 1)
    tail = jnp.where(lane_row < 3, qsum, 0.0)[:, : depth - 2 * k_size]
    a, b, c = (part.astype(jnp.float32) for part in split3(jnp.concatenate([v, tail], axis=1)))
    stacked = jnp.where(pick == 0, a, jnp.where(pick == 1, b, jnp.where(pick == 2, c, 0.0)))
    wt_ref[p_size:, :] = stacked.astype(jnp.bfloat16)
    scaled = ns_ref[...].astype(jnp.float32) * qrow
    top = scaled.astype(jnp.bfloat16)
    low = (scaled - top.astype(jnp.float32)).astype(jnp.bfloat16)
    nq_ref[...] = jnp.concatenate([top, low], axis=0)

    key_ref[...] = ((rank_ref[...] - 2) << 30) + (FACE_MASK - face_ref[...])
    jl = jnp.where(alive, jac_ref[...], 0.0)
    jl_ref[...] = jl
    area_ref[...] = jnp.sum(jl, axis=0, keepdims=True) * jnp.sum(qrow, axis=1, keepdims=True)
    over_pen[...] = jnp.full(over_pen.shape, LOWEST_FILL, jnp.float32)
    over_key[...] = jnp.full(over_key.shape, KEY_LOW, jnp.int32)

    pltpu.make_async_copy(x_ref, x_ref, s_big).wait()

    @pl.when(worst >= DEPTH * PAD_GROUPS)
    def _():
        weights = wt_ref[...]

        def fill(tile, carry):
            store_pen(pen_ref, tile, project(weights, x_ref, off_ref, tile)[:p_size])
            return carry

        lax.fori_loop(0, rows // TILE, fill, 0)

        def one(worst):
            code = face_ref[...]
            g = worst & (PAD_GROUPS - 1)
            low = (worst >> 4) & -SUB
            pull_groups([g], low, SUB, face_ref, slot_ref, pen_ref, key_ref, packs)
            top, best = match_group(g, 0, SUB, packs)
            at = pl.ds(g, 1)
            over_pen[at, :] = jnp.maximum(over_pen[at, :], top)
            over_key[at, :] = jnp.maximum(over_key[at, :], best)
            done = ((code & (PAD_GROUPS - 1)) == g) & (code >= low * PAD_GROUPS)
            code = jnp.where(done, -1, code)
            face_ref[...] = code
            return jnp.max(code)

        face_ref[...] = code_ref[...]
        lax.while_loop(lambda worst: worst >= DEPTH * PAD_GROUPS, one, worst)


def main_kernel(
    n_dom, n_rep,
    x_ref, wt_ref, nq_ref, off_ref, jl_ref, slot_ref, code_ref, key_ref, over_pen, over_key, area_ref,
    force_ref, out_pen, out_face, out_gap, out_mean,
    load_ref, pen_ref, seg_ref, packs, raw_pen, raw_key,
    sp_sf, sp_si, ow_sf, ow_si, t1_s, t2_s, sp_f, sp_i, ow_f, ow_i, t1_d, t2_d,
    s_spf, r_spf, s_spi, r_spi, s_owf, r_owf, s_owi, r_owi, s_t1, r_t1, s_t2, r_t2,
):
    dom = lax.axis_index("dom")
    rep = lax.axis_index("rep")
    k_size = force_ref.shape[0]
    rows = force_ref.shape[1]
    p_size = load_ref.shape[0]
    per_tile = TILE // LANES
    tiles = rows // TILE

    def dev(d, r):
        return {"dom": lax.rem(d + n_dom, n_dom), "rep": lax.rem(r + n_rep, n_rep)}

    barrier = pltpu.get_barrier_semaphore()
    count = n_dom * n_rep
    me = dom * n_rep + rep

    def greet_peer(j, carry):
        flat = lax.rem(me + j, count)
        pl.semaphore_signal(
            barrier, inc=1, device_id=dev(lax.div(flat, n_rep), lax.rem(flat, n_rep)), device_id_type=MESH
        )
        return carry

    lax.fori_loop(1, count, greet_peer, 0)

    wt = wt_ref[...]
    hi_id = lax.broadcasted_iota(jnp.int32, (PAD_GROUPS, TILE), 0)
    lo_id = lax.broadcasted_iota(jnp.int32, (LANES, TILE), 0)

    def wide_row(ref, tile):
        return jnp.concatenate([row(ref, tile * per_tile + i) for i in range(per_tile)], axis=1)

    def batch(step, seg_total):
        first = step * UNROLL
        for i in range(UNROLL):
            tile = first + i
            cols = pl.ds(tile * TILE, TILE)
            field = project(wt, x_ref, off_ref, tile)
            gap = field[:p_size]
            load_ref[:, cols] = jnp.minimum(gap.astype(jnp.bfloat16), 0)
            store_pen(pen_ref, tile, gap)
            row_gap = wide_row(jl_ref, tile)[0:1] * jnp.sum(field[p_size : p_size + SUB], axis=0, keepdims=True)
            slot = wide_row(slot_ref, tile)[0:1]
            spread = jnp.where(hi_id == (slot >> 7), row_gap, 0.0)
            left = jnp.concatenate(split3(spread)[:2], axis=0)
            right = jnp.where(lo_id == (slot & (LANES - 1)), 1.0, 0.0).astype(jnp.bfloat16)
            seg_total = seg_total + lax.dot_general(
                left, right, (((1,), (1,)), ((), ())), preferred_element_type=jnp.float32
            )
        return seg_total

    seg_total = lax.fori_loop(0, tiles // UNROLL, batch, jnp.zeros((2 * PAD_GROUPS, LANES), jnp.float32))
    seg = seg_total[:PAD_GROUPS] + seg_total[PAD_GROUPS:]
    seg_ref[...] = seg
    total_gap = jnp.sum(jnp.sum(seg, axis=0, keepdims=True), axis=1, keepdims=True)
    total_area = jnp.sum(area_ref[...], axis=1, keepdims=True)
    lane = lax.broadcasted_iota(jnp.int32, (1, LANES), 1)
    t1_s[...] = jnp.where(lane == 0, total_gap, jnp.where(lane == 1, total_area, 0.0))

    def scan(gs, base):
        pull_groups(gs, 0, DEPTH, code_ref, slot_ref, pen_ref, key_ref, packs)
        for i, g in enumerate(gs):
            top, best = match_group(g, i * DEPTH, DEPTH, packs)
            raw_pen[base + i : base + i + 1, :] = jnp.maximum(top, over_pen[g : g + 1, :])
            raw_key[base + i : base + i + 1, :] = jnp.maximum(best, over_key[g : g + 1, :])

    def decode(top, best):
        none = top < LOWEST_FILL * 0.5
        rank = jnp.where(none, -1, (best >> 30) + 2)
        face = jnp.where(none, FACE_LIMIT, FACE_MASK - (best & FACE_MASK))
        return rank, face

    scan(range(OWN_GROUPS, GROUPS), 0)
    top = raw_pen[0:SPILL_GROUPS, :]
    rank, face = decode(top, raw_key[0:SPILL_GROUPS, :])
    sp_sf[0:SPILL_GROUPS, :] = top
    sp_sf[SPILL_GROUPS:, :] = seg_ref[OWN_GROUPS:GROUPS, :]
    sp_si[0:SPILL_GROUPS, :] = rank
    sp_si[SPILL_GROUPS:, :] = face

    pl.semaphore_wait(barrier, count - 1)

    def spill_copy(j):
        where = dev(dom + 1, rep + j)
        return (
            pltpu.make_async_remote_copy(
                src_ref=sp_sf, dst_ref=sp_f.at[rep], send_sem=s_spf, recv_sem=r_spf,
                device_id=where, device_id_type=MESH,
            ),
            pltpu.make_async_remote_copy(
                src_ref=sp_si, dst_ref=sp_i.at[rep], send_sem=s_spi, recv_sem=r_spi,
                device_id=where, device_id_type=MESH,
            ),
        )

    for j in range(n_rep):
        for copy in spill_copy(j):
            copy.start()

    mate = rep + 1 - 2 * lax.rem(rep, 2)
    first_copy = pltpu.make_async_remote_copy(
        src_ref=t1_s, dst_ref=t1_d, send_sem=s_t1, recv_sem=r_t1,
        device_id=dev(dom, mate), device_id_type=MESH,
    )
    first_copy.start()

    half = OWN_GROUPS // 2
    scan(range(half), 0)

    first_copy.wait_recv()
    pairs = count // 2
    pair = lax.div(me, 2)
    both = t1_s[...] + t1_d[...]
    t2_s[...] = both
    t2_d[pl.ds(pair, 1), :] = both

    def pair_copy(j):
        other = lax.rem(pair + j, pairs)
        flat = other * 2 + lax.rem(rep, 2)
        return pltpu.make_async_remote_copy(
            src_ref=t2_s, dst_ref=t2_d.at[pl.ds(pair, 1), :], send_sem=s_t2, recv_sem=r_t2,
            device_id=dev(lax.div(flat, n_rep), lax.rem(flat, n_rep)), device_id_type=MESH,
        )

    def start_pair(j, carry):
        pair_copy(j).start()
        return carry

    lax.fori_loop(1, pairs, start_pair, 0)

    scan(range(half, OWN_GROUPS), half)
    top = raw_pen[...]
    rank, face = decode(top, raw_key[...])
    ow_sf[0] = top
    ow_sf[1] = seg_ref[:OWN_GROUPS, :]
    ow_si[0] = rank
    ow_si[1] = face

    def own_copy(j):
        where = dev(dom, rep + j)
        return (
            pltpu.make_async_remote_copy(
                src_ref=ow_sf, dst_ref=ow_f.at[rep], send_sem=s_owf, recv_sem=r_owf,
                device_id=where, device_id_type=MESH,
            ),
            pltpu.make_async_remote_copy(
                src_ref=ow_si, dst_ref=ow_i.at[rep], send_sem=s_owi, recv_sem=r_owi,
                device_id=where, device_id_type=MESH,
            ),
        )

    for j in range(1, n_rep):
        for copy in own_copy(j):
            copy.start()
    ow_f[rep] = ow_sf[...]
    ow_i[rep] = ow_si[...]

    nq = nq_ref[...]

    def push(step, carry):
        for i in range(4):
            tile = step * 4 + i
            cols = pl.ds(tile * TILE, TILE)
            force = jnp.dot(nq, load_ref[:, cols], preferred_element_type=jnp.float32)
            scale = wide_row(jl_ref, tile)[0:1] * -PENALTY
            force_ref[:, cols] = ((force[:k_size] + force[k_size:]) * scale).astype(jnp.bfloat16)
        return carry

    lax.fori_loop(0, tiles // 4, push, 0)

    def encode(rank, face):
        return jnp.where(rank < 0, KEY_LOW, ((rank - 2) << 30) + (FACE_MASK - face))

    def settle(ref, sem):
        pltpu.make_async_copy(ref, ref, sem).wait()

    settle(ow_f.at[pl.ds(0, n_rep - 1)], r_owf)
    settle(ow_i.at[pl.ds(0, n_rep - 1)], r_owi)
    pen_o, gap_o = ow_f[0, 0], ow_f[0, 1]
    key_o = encode(ow_i[0, 0], ow_i[0, 1])
    for r in range(1, n_rep):
        pen_o = jnp.maximum(pen_o, ow_f[r, 0])
        gap_o = gap_o + ow_f[r, 1]
        key_o = jnp.maximum(key_o, encode(ow_i[r, 0], ow_i[r, 1]))

    settle(t2_d.at[pl.ds(0, pairs - 1), :], r_t2)
    whole = jnp.sum(t2_d[...], axis=0, keepdims=True)
    out_mean[...] = whole[:, 0:1] / whole[:, 1:2]

    settle(sp_f, r_spf)
    settle(sp_i, r_spi)
    g = SPILL_GROUPS
    pen_s, gap_s = sp_f[0, 0:g], sp_f[0, g:]
    key_s = encode(sp_i[0, 0:g], sp_i[0, g:])
    for r in range(1, n_rep):
        pen_s = jnp.maximum(pen_s, sp_f[r, 0:g])
        gap_s = gap_s + sp_f[r, g:]
        key_s = jnp.maximum(key_s, encode(sp_i[r, 0:g], sp_i[r, g:]))

    def finish(at, pen, key, gap):
        none = pen < LOWEST_FILL * 0.5
        out_pen[at, :] = jnp.where(none, 0.0, pen)
        out_face[at, :] = jnp.where(none, -1, FACE_MASK - (key & FACE_MASK))
        out_gap[at, :] = jnp.where(none, 0.0, gap)

    finish(
        slice(0, g), jnp.maximum(pen_o[:g], pen_s), jnp.maximum(key_o[:g], key_s), gap_o[:g] + gap_s
    )
    finish(slice(g, OWN_GROUPS), pen_o[g:], key_o[g:], gap_o[g:])

    settle(sp_f, s_spf)
    settle(sp_i, s_spi)
    settle(ow_f.at[pl.ds(0, n_rep - 1)], s_owf)
    settle(ow_i.at[pl.ds(0, n_rep - 1)], s_owi)
    first_copy.wait_send()
    settle(t2_d.at[pl.ds(0, pairs - 1), :], s_t2)


def finish_kernel(*refs):
    count = (len(refs) - 1) // 2
    sems = refs[-1]
    copies = [pltpu.make_async_copy(refs[i], refs[count + i], sems.at[i]) for i in range(count)]
    for copy in copies:
        copy.start()
    for copy in copies:
        copy.wait()


def solution(mesh):
    n_dom, n_rep = mesh.shape["dom"], mesh.shape["rep"]
    vmem = pl.BlockSpec(memory_space=pltpu.VMEM)
    anywhere = pl.BlockSpec(memory_space=pl.ANY)
    dma = pltpu.SemaphoreType.DMA

    def kept(x):
        return pltpu.with_memory_space_constraint(x, pltpu.VMEM)

    def shards(ns, nm, sec, mst, off, qw, jac, slot, face, rank, live):
        k_size, p_size = ns.shape
        rows = sec.shape[1]
        lines = rows // LANES
        depth = 2 * k_size + EXTRA
        f32, i32, bf16 = jnp.float32, jnp.int32, jnp.bfloat16

        off, jac, slot, face, rank = (x.reshape(lines, LANES) for x in (off, jac, slot, face, rank))

        def packs(groups):
            deep = groups * DEPTH + SUB
            return [pltpu.VMEM((deep, LANES), t) for t in (i32, f32, i32)]

        held = pl.pallas_call(
            prep_kernel,
            out_shape=(
                pltpu.VMEM((2 * k_size, rows), bf16),
                pltpu.VMEM((p_size + EXTRA, depth), bf16),
                pltpu.VMEM((2 * k_size, p_size), bf16),
                pltpu.VMEM((lines, LANES), f32),
                pltpu.VMEM((lines, LANES), f32),
                pltpu.VMEM((lines, LANES), i32),
                pltpu.VMEM((lines, LANES), i32),
                pltpu.VMEM((lines, LANES), i32),
                pltpu.VMEM((PAD_GROUPS, LANES), f32),
                pltpu.VMEM((PAD_GROUPS, LANES), i32),
                pltpu.VMEM((1, LANES), f32),
            ),
            in_specs=[anywhere] * 11,
            out_specs=(vmem,) * 11,
            scratch_shapes=[
                pltpu.SMEM((1,), i32),
                pltpu.VMEM((k_size, p_size), bf16),
                pltpu.VMEM((k_size, p_size), bf16),
                pltpu.VMEM((1, p_size), f32),
                pltpu.VMEM((lines, LANES), f32),
                pltpu.VMEM((lines, LANES), i32),
                pltpu.VMEM((lines, LANES), i32),
                pltpu.VMEM((lines, LANES), f32),
                packs(1),
                dma((9,)),
                dma,
            ],
        )(live, ns, nm, qw.reshape(1, p_size), sec, mst, off, jac, slot, face, rank)

        spill = (2 * SPILL_GROUPS, LANES)
        own = (2, OWN_GROUPS, LANES)
        pairs = n_dom * n_rep // 2
        results = pl.pallas_call(
            functools.partial(main_kernel, n_dom, n_rep),
            out_shape=(
                pltpu.VMEM((k_size, rows), bf16),
                pltpu.VMEM((OWN_GROUPS, LANES), f32),
                pltpu.VMEM((OWN_GROUPS, LANES), i32),
                pltpu.VMEM((OWN_GROUPS, LANES), f32),
                pltpu.VMEM((1, 1), f32),
            ),
            in_specs=[vmem] * 11,
            out_specs=(vmem,) * 5,
            scratch_shapes=[
                pltpu.VMEM((p_size, rows), bf16),
                pltpu.VMEM((lines, LANES), f32),
                pltpu.VMEM((PAD_GROUPS, LANES), f32),
                packs(OWN_GROUPS // 2),
                pltpu.VMEM((OWN_GROUPS, LANES), f32),
                pltpu.VMEM((OWN_GROUPS, LANES), i32),
                pltpu.VMEM(spill, f32),
                pltpu.VMEM(spill, i32),
                pltpu.VMEM(own, f32),
                pltpu.VMEM(own, i32),
                pltpu.VMEM((1, LANES), f32),
                pltpu.VMEM((1, LANES), f32),
                pltpu.VMEM((n_rep,) + spill, f32),
                pltpu.VMEM((n_rep,) + spill, i32),
                pltpu.VMEM((n_rep,) + own, f32),
                pltpu.VMEM((n_rep,) + own, i32),
                pltpu.VMEM((1, LANES), f32),
                pltpu.VMEM((pairs, LANES), f32),
            ] + [dma] * 12,
            compiler_params=pltpu.CompilerParams(collective_id=0, has_side_effects=True),
        )(*(kept(x) for x in held))

        force, seg_pen, seg_face, seg_gap, mean = pl.pallas_call(
            finish_kernel,
            out_shape=tuple(jax.ShapeDtypeStruct(x.shape, x.dtype) for x in results),
            in_specs=[vmem] * 5,
            out_specs=(anywhere,) * 5,
            scratch_shapes=[dma((5,))],
        )(*(kept(x) for x in results))
        seg_pen, seg_face, seg_gap = (x.reshape(SEG_DEV) for x in (seg_pen, seg_face, seg_gap))
        return force, seg_pen, seg_face, seg_gap, mean.reshape(())

    rows_spec, wide_spec = P(("dom", "rep")), P(None, ("dom", "rep"))
    return jax.shard_map(
        shards,
        mesh=mesh,
        in_specs=(P(), P(), wide_spec, wide_spec, rows_spec, P()) + (rows_spec,) * 5,
        out_specs=(wide_spec, P("dom"), P("dom"), P("dom"), P()),
        check_vma=False,
    )
```

```python
import functools

import jax
import jax.numpy as jnp
from jax import lax
from jax.experimental import pallas as pl
from jax.experimental.pallas import tpu as pltpu
from jax.sharding import PartitionSpec as P

SEG_DEV = 1024
SPILL = 256
LANES = 128
SUB = 8
WIDTH = 64
PER_ROW = LANES // WIDTH
GROUPS = (SEG_DEV + SPILL) // WIDTH
OWN_GROUPS = SEG_DEV // WIDTH
SPILL_GROUPS = SPILL // WIDTH
OWN_ROWS = SEG_DEV // LANES
SPILL_ROWS = SPILL // LANES
ALL_ROWS = 16
CODE = 32

PENALTY = 400.0
LOWEST_FILL = -1e30
FACE_LIMIT = 1073741824
FACE_MASK = FACE_LIMIT - 1
KEY_LOW = -2147483648
MESH = pl.DeviceIdType.MESH
TILE = 256
DEPTH = 12
BATCH = 4
UNROLL = 16
CHAINS = 4
FORCE_UNROLL = 8
EXTRA = 16
VMEM_LIMIT = 32 << 20


def split3(x):
    a = x.astype(jnp.bfloat16)
    rest = x - a.astype(jnp.float32)
    b = rest.astype(jnp.bfloat16)
    c = (rest - b.astype(jnp.float32)).astype(jnp.bfloat16)
    return a, b, c


def row(ref, at):
    return ref[pl.ds(at, SUB, stride=0), :]


def pull_groups(first, count, depth0, depth, code_ref, sources, packs):
    all_lines = code_ref.shape[0]
    sub = lax.broadcasted_iota(jnp.int32, (SUB, LANES), 0)
    blocks = -(-count * depth // SUB)
    wants = []
    for b in range(blocks):
        line = sub + SUB * b
        want = jnp.full((SUB, LANES), -2, jnp.int32)
        for q in range(count):
            inside = (line >= q * depth) & (line < (q + 1) * depth)
            want = jnp.where(inside, (line + (depth0 - q * depth)) * CODE + (first + q), want)
        wants.append(want)
    fills = (-1, LOWEST_FILL, -1, 0.0)

    def pull(i, carry):
        parts = [list(part) for part in carry]
        code = row(code_ref, i)
        values = [row(ref, i) for ref in sources]
        for b in range(blocks):
            hit = code == wants[b]
            for part, value in zip(parts, values):
                part[b] = jnp.where(hit, value, part[b])
        return tuple(tuple(part) for part in parts)

    start = tuple(
        (jnp.full((SUB, LANES), fill, ref.dtype),) * blocks for fill, ref in zip(fills, sources)
    )
    pulled = lax.fori_loop(0, all_lines, pull, start, unroll=8)
    for ref, parts in zip(packs, pulled):
        for b in range(blocks):
            ref[SUB * b : SUB * (b + 1), :] = parts[b]


def match_group(g, at, depth, packs):
    sub = lax.broadcasted_iota(jnp.int32, (SUB, LANES), 0)
    tiles = WIDTH // SUB
    marks = [sub + (g * WIDTH + SUB * q) for q in range(tiles)]
    pens = [jnp.full((SUB, LANES), LOWEST_FILL, jnp.float32)] * tiles
    keys = [jnp.full((SUB, LANES), KEY_LOW, jnp.int32)] * tiles
    gaps = [jnp.zeros((SUB, LANES), jnp.float32)] * tiles
    for j in range(depth):
        slot, pen, key, gap = (row(ref, at + j) for ref in packs)
        for q in range(tiles):
            hit = slot == marks[q]
            pens[q] = jnp.maximum(pens[q], jnp.where(hit, pen, LOWEST_FILL))
            keys[q] = jnp.maximum(keys[q], jnp.where(hit, key, KEY_LOW))
            gaps[q] = gaps[q] + jnp.where(hit, gap, 0.0)
    return pens, keys, gaps


def across(parts):
    pens, keys, gaps = (jnp.concatenate(sum(lists, []), axis=0).T for lists in zip(*parts))
    return (
        jnp.max(pens, axis=0, keepdims=True),
        jnp.max(keys, axis=0, keepdims=True),
        jnp.sum(gaps, axis=0, keepdims=True),
    )


def project(wt, x_ref, off_ref, tile):
    cols = pl.ds(tile * TILE, TILE)
    per_tile = TILE // LANES
    offset = jnp.concatenate([row(off_ref, tile * per_tile + i) for i in range(per_tile)], axis=1)
    sub = lax.broadcasted_iota(jnp.int32, (SUB, TILE), 0)
    a, b, c = (part.astype(jnp.float32) for part in split3(offset))
    extra = jnp.where(sub == 0, a, jnp.where(sub == 1, b, jnp.where(sub == 2, c, 0.0)))
    extra = jnp.concatenate([extra, jnp.zeros((EXTRA - SUB, TILE), jnp.float32)], axis=0)
    x = jnp.concatenate([x_ref[:, cols], extra.astype(jnp.bfloat16)], axis=0)
    return jnp.dot(wt, x, preferred_element_type=jnp.float32)


def store_row(ref, tile, value):
    per_tile = TILE // LANES
    for i in range(per_tile):
        ref[pl.ds(tile * per_tile + i, 1), :] = value[:, i * LANES : (i + 1) * LANES]


def reduce_field(field, p_size, tile, pen_ref, gap_ref):
    low = [field[SUB * j : SUB * (j + 1)] for j in range(CHAINS)]
    for j in range(CHAINS, p_size // SUB):
        low[j % CHAINS] = jnp.minimum(low[j % CHAINS], field[SUB * j : SUB * (j + 1)])
    store_row(pen_ref, tile, -jnp.min(functools.reduce(jnp.minimum, low), axis=0, keepdims=True))
    store_row(gap_ref, tile, jnp.sum(field[p_size : p_size + SUB], axis=0, keepdims=True))


def prep_kernel(
    live_h, ns_h, nm_h, qw_h, sec_h, mst_h, off_h, jac_h, slot_h, face_h, rank_h,
    x_ref, wt_ref, nq_ref, off_ref, jl_ref, slot_ref, code_ref, key_ref, over_pen, over_key, over_gap, area_ref,
    live_s, ns_ref, nm_ref, qw_ref, jac_ref, face_ref, rank_ref, pen_ref, gap_ref, packs, s_small, s_big,
):
    lines = slot_ref.shape[0]
    k_size, p_size = ns_ref.shape
    rows = x_ref.shape[1]

    small = [
        pltpu.make_async_copy(source, held, s_small.at[i])
        for i, (source, held) in enumerate((
            (slot_h, slot_ref), (live_h, live_s), (ns_h, ns_ref), (nm_h, nm_ref), (qw_h, qw_ref),
            (face_h, face_ref), (rank_h, rank_ref), (jac_h, jac_ref), (off_h, off_ref),
        ))
    ]
    for copy in small:
        copy.start()
    for base, source in ((0, sec_h), (k_size, mst_h)):
        for at in range(0, k_size, 2 * SUB):
            pltpu.make_async_copy(
                source.at[at : at + 2 * SUB, :], x_ref.at[base + at : base + at + 2 * SUB, :], s_big
            ).start()
    for copy in small:
        copy.wait()

    row_id = (
        lax.broadcasted_iota(jnp.int32, (lines, LANES), 0) * LANES
        + lax.broadcasted_iota(jnp.int32, (lines, LANES), 1)
    )
    alive = row_id < live_s[...]
    group = jnp.where(alive, slot_ref[...] // WIDTH, -1)
    before = (
        lax.broadcasted_iota(jnp.int32, (lines, lines), 1)
        < lax.broadcasted_iota(jnp.int32, (lines, lines), 0)
    )
    before = jnp.where(before, 1.0, 0.0).astype(jnp.bfloat16)
    place = jnp.zeros((lines, LANES), jnp.float32)
    for g in range(0, GROUPS, 2):
        mine = [group == g, group == g + 1]
        seen = jnp.concatenate([jnp.where(m, 1.0, 0.0).astype(jnp.bfloat16) for m in mine], axis=1)
        found = jnp.dot(before, seen, preferred_element_type=jnp.float32)
        place = jnp.where(mine[0], found[:, :LANES], jnp.where(mine[1], found[:, LANES:], place))
    code = jnp.where(alive, place.astype(jnp.int32) * CODE + group, -1)
    code_ref[...] = code
    worst = jnp.max(code)

    w = jnp.concatenate([ns_ref[...], -nm_ref[...]], axis=0).astype(jnp.float32)
    qrow = qw_ref[...]
    wt = w.T
    qmat = jnp.broadcast_to(qrow, (LANES, p_size)).T
    v = jnp.sum(wt * qmat, axis=0, keepdims=True)
    qsum = jnp.sum(qmat, axis=0, keepdims=True)
    depth = wt_ref.shape[1]
    pick = lax.broadcasted_iota(jnp.int32, (EXTRA, depth), 0)
    column = lax.broadcasted_iota(jnp.int32, (p_size, depth - 2 * k_size), 1)
    wt_ref[0:p_size, 0 : 2 * k_size] = wt.astype(jnp.bfloat16)
    wt_ref[0:p_size, 2 * k_size :] = jnp.where(column < 3, 1.0, 0.0).astype(jnp.bfloat16)
    lane_row = lax.broadcasted_iota(jnp.int32, (1, LANES), 1)
    tail = jnp.where(lane_row < 3, qsum, 0.0)[:, : depth - 2 * k_size]
    a, b, c = (part.astype(jnp.float32) for part in split3(jnp.concatenate([v, tail], axis=1)))
    stacked = jnp.where(pick == 0, a, jnp.where(pick == 1, b, jnp.where(pick == 2, c, 0.0)))
    wt_ref[p_size:, :] = stacked.astype(jnp.bfloat16)
    scaled = ns_ref[...].astype(jnp.float32) * qrow
    top = scaled.astype(jnp.bfloat16)
    low = (scaled - top.astype(jnp.float32)).astype(jnp.bfloat16)
    nq_ref[...] = jnp.concatenate([top, low], axis=0)

    key_ref[...] = ((rank_ref[...] - 2) << 30) + (FACE_MASK - face_ref[...])
    jl = jnp.where(alive, jac_ref[...], 0.0)
    jl_ref[...] = jl
    area_ref[...] = jnp.sum(jl, axis=0, keepdims=True) * jnp.sum(qrow, axis=1, keepdims=True)
    over_pen[...] = jnp.full(over_pen.shape, LOWEST_FILL, jnp.float32)
    over_key[...] = jnp.full(over_key.shape, KEY_LOW, jnp.int32)
    over_gap[...] = jnp.zeros(over_gap.shape, jnp.float32)

    pltpu.make_async_copy(x_ref, x_ref, s_big).wait()

    @pl.when(worst >= DEPTH * CODE)
    def _():
        weights = wt_ref[...]

        def fill(tile, carry):
            reduce_field(project(weights, x_ref, off_ref, tile), p_size, tile, pen_ref, gap_ref)
            return carry

        lax.fori_loop(0, rows // TILE, fill, 0)
        gap_ref[...] = gap_ref[...] * jl_ref[...]
        face_ref[...] = code_ref[...]

        def one(worst):
            code = face_ref[...]
            g = worst & (CODE - 1)
            low = jnp.maximum((worst // CODE) & -SUB, DEPTH)
            pull_groups(g, 1, low, SUB, face_ref, (slot_ref, pen_ref, key_ref, gap_ref), packs)
            found = match_group(g, 0, SUB, packs)
            odd = jnp.full((SUB, LANES), g & 1, jnp.int32)
            fills = (LOWEST_FILL, KEY_LOW, 0.0)
            parts = [
                tuple([jnp.where(odd == side, x, fill) for x in part] for part, fill in zip(found, fills))
                for side in range(PER_ROW)
            ]
            pen, key, gap = across(parts)
            at = pl.ds(g // PER_ROW, 1)
            over_pen[at, :] = jnp.maximum(over_pen[at, :], pen)
            over_key[at, :] = jnp.maximum(over_key[at, :], key)
            over_gap[at, :] = over_gap[at, :] + gap
            done = ((code & (CODE - 1)) == g) & (code >= low * CODE)
            code = jnp.where(done, -1, code)
            face_ref[...] = code
            return jnp.max(code)

        lax.while_loop(lambda worst: worst >= DEPTH * CODE, one, worst)


def main_kernel(
    n_dom, n_rep,
    x_ref, wt_ref, nq_ref, off_ref, jl_ref, slot_ref, code_ref, key_ref, over_pen, over_key, over_gap, area_ref,
    force_ref, out_pen, out_face, out_gap, out_mean,
    load_ref, pen_ref, gap_ref, packs, raw_pen, raw_key, raw_gap,
    sp_sf, sp_si, ow_sf, ow_si, t1_s, t2_s, sp_f, sp_i, ow_f, ow_i, t1_d, t2_d,
    s_spf, r_spf, s_spi, r_spi, s_owf, r_owf, s_owi, r_owi, s_t1, r_t1, s_t2, r_t2, inside,
):
    dom = lax.axis_index("dom")
    rep = lax.axis_index("rep")
    k_size = force_ref.shape[0]
    rows = force_ref.shape[1]
    p_size = load_ref.shape[0]
    per_tile = TILE // LANES
    tiles = rows // TILE
    count = n_dom * n_rep
    me = dom * n_rep + rep

    def dev(d, r):
        return {"dom": lax.rem(d + n_dom, n_dom), "rep": lax.rem(r + n_rep, n_rep)}

    def flat_dev(flat):
        return dev(lax.div(flat, n_rep), lax.rem(flat, n_rep))

    barrier = pltpu.get_barrier_semaphore()

    def signal(sem, first, last):
        def one(flat, carry):
            pl.semaphore_signal(sem, inc=1, device_id=flat_dev(flat), device_id_type=MESH)
            return carry

        lax.fori_loop(first, last, one, 0)

    signal(barrier, me + 1, count)
    signal(barrier, dom * n_rep, me)
    signal(barrier, jnp.maximum(dom - 1, 0) * n_rep, dom * n_rep)

    wt = wt_ref[...]

    def wide_row(ref, tile):
        return jnp.concatenate([row(ref, tile * per_tile + i) for i in range(per_tile)], axis=1)

    def batch(step, carry):
        for i in range(UNROLL):
            tile = step * UNROLL + i
            cols = pl.ds(tile * TILE, TILE)
            field = project(wt, x_ref, off_ref, tile)
            for at in range(0, p_size, 2 * SUB):
                load_ref[at : at + 2 * SUB, cols] = jnp.minimum(field[at : at + 2 * SUB].astype(jnp.bfloat16), 0)
            reduce_field(field, p_size, tile, pen_ref, gap_ref)
        return carry

    lax.fori_loop(0, tiles // UNROLL, batch, 0)
    row_gap = gap_ref[...] * jl_ref[...]
    gap_ref[...] = row_gap
    total_gap = jnp.sum(jnp.sum(row_gap, axis=0, keepdims=True), axis=1, keepdims=True)
    total_area = jnp.sum(area_ref[...], axis=1, keepdims=True)
    lane = lax.broadcasted_iota(jnp.int32, (1, LANES), 1)
    t1_s[...] = jnp.where(lane == 0, total_gap, jnp.where(lane == 1, total_area, 0.0))

    after = n_rep * jnp.where(dom < n_dom - 1, 1, 0)
    pl.semaphore_wait(barrier, me + (n_rep - 1 - rep) + after)
    signal(inside, 0, me)

    mate = rep + 1 - 2 * lax.rem(rep, 2)
    first_copy = pltpu.make_async_remote_copy(
        src_ref=t1_s, dst_ref=t1_d, send_sem=s_t1, recv_sem=r_t1,
        device_id=dev(dom, mate), device_id_type=MESH,
    )
    first_copy.start()

    def scan(first, base):
        pull_groups(first, BATCH, 0, DEPTH, code_ref, (slot_ref, pen_ref, key_ref, gap_ref), packs)
        for i in range(BATCH // PER_ROW):
            parts = [
                match_group(first + i * PER_ROW + j, (i * PER_ROW + j) * DEPTH, DEPTH, packs) for j in range(PER_ROW)
            ]
            pen, key, gap = across(parts)
            over = pl.ds(first // PER_ROW + i, 1)
            at = pl.ds(base + i, 1)
            raw_pen[at, :] = jnp.maximum(pen, over_pen[over, :])
            raw_key[at, :] = jnp.maximum(key, over_key[over, :])
            raw_gap[at, :] = gap + over_gap[over, :]

    def decode(top, best):
        none = top < LOWEST_FILL * 0.5
        rank = jnp.where(none, -1, (best >> 30) + 2)
        face = jnp.where(none, FACE_LIMIT, FACE_MASK - (best & FACE_MASK))
        return rank, face

    scan(OWN_GROUPS, 0)
    part = slice(0, SPILL_ROWS)
    rank, face = decode(raw_pen[part, :], raw_key[part, :])
    sp_sf[0:SPILL_ROWS, :] = raw_pen[part, :]
    sp_sf[SPILL_ROWS:, :] = raw_gap[part, :]
    sp_si[0:SPILL_ROWS, :] = rank
    sp_si[SPILL_ROWS:, :] = face

    def spill_copy(j):
        where = dev(dom + 1, rep + j)
        return (
            pltpu.make_async_remote_copy(
                src_ref=sp_sf, dst_ref=sp_f.at[rep], send_sem=s_spf, recv_sem=r_spf,
                device_id=where, device_id_type=MESH,
            ),
            pltpu.make_async_remote_copy(
                src_ref=sp_si, dst_ref=sp_i.at[rep], send_sem=s_spi, recv_sem=r_spi,
                device_id=where, device_id_type=MESH,
            ),
        )

    for j in range(n_rep):
        for copy in spill_copy(j):
            copy.start()

    first_copy.wait_recv()
    pairs = count // 2
    pair = lax.div(me, 2)
    both = t1_s[...] + t1_d[...]
    t2_s[...] = both
    t2_d[pl.ds(pair, 1), :] = both

    def send_pairs(first, last):
        def one(other, carry):
            pltpu.make_async_remote_copy(
                src_ref=t2_s, dst_ref=t2_d.at[pl.ds(pair, 1), :], send_sem=s_t2, recv_sem=r_t2,
                device_id=flat_dev(other * 2 + lax.rem(rep, 2)), device_id_type=MESH,
            ).start()
            return carry

        lax.fori_loop(first, last, one, 0)

    send_pairs(0, pair)

    def own_scan(i, carry):
        scan(i * BATCH, i * (BATCH // PER_ROW))
        return carry

    lax.fori_loop(0, OWN_GROUPS // BATCH, own_scan, 0)
    rank, face = decode(raw_pen[...], raw_key[...])
    ow_sf[0] = raw_pen[...]
    ow_sf[1] = raw_gap[...]
    ow_si[0] = rank
    ow_si[1] = face

    def own_copy(j):
        where = dev(dom, rep + j)
        return (
            pltpu.make_async_remote_copy(
                src_ref=ow_sf, dst_ref=ow_f.at[rep], send_sem=s_owf, recv_sem=r_owf,
                device_id=where, device_id_type=MESH,
            ),
            pltpu.make_async_remote_copy(
                src_ref=ow_si, dst_ref=ow_i.at[rep], send_sem=s_owi, recv_sem=r_owi,
                device_id=where, device_id_type=MESH,
            ),
        )

    for j in range(1, n_rep):
        for copy in own_copy(j):
            copy.start()
    ow_f[rep] = ow_sf[...]
    ow_i[rep] = ow_si[...]

    nq = nq_ref[...]

    def push(step, carry):
        for i in range(FORCE_UNROLL):
            tile = step * FORCE_UNROLL + i
            cols = pl.ds(tile * TILE, TILE)
            force = jnp.dot(nq, load_ref[:, cols], preferred_element_type=jnp.float32)
            scale = wide_row(jl_ref, tile)[0:1] * -PENALTY
            force_ref[:, cols] = ((force[:k_size] + force[k_size:]) * scale).astype(jnp.bfloat16)
        return carry

    lax.fori_loop(0, tiles // FORCE_UNROLL, push, 0)

    @pl.when(me < count - 1)
    def _():
        pl.semaphore_wait(inside, count - 1 - me)

    send_pairs(pair + 1, pairs)

    def encode(rank, face):
        return jnp.where(rank < 0, KEY_LOW, ((rank - 2) << 30) + (FACE_MASK - face))

    def settle(ref, sem):
        pltpu.make_async_copy(ref, ref, sem).wait()

    settle(ow_f.at[pl.ds(0, n_rep - 1)], r_owf)
    settle(ow_i.at[pl.ds(0, n_rep - 1)], r_owi)
    pen_o, gap_o = ow_f[0, 0], ow_f[0, 1]
    key_o = encode(ow_i[0, 0], ow_i[0, 1])
    for r in range(1, n_rep):
        pen_o = jnp.maximum(pen_o, ow_f[r, 0])
        gap_o = gap_o + ow_f[r, 1]
        key_o = jnp.maximum(key_o, encode(ow_i[r, 0], ow_i[r, 1]))

    settle(sp_f, s_spf)
    settle(sp_i, s_spi)
    settle(ow_f.at[pl.ds(0, n_rep - 1)], s_owf)
    settle(ow_i.at[pl.ds(0, n_rep - 1)], s_owi)
    first_copy.wait_send()
    settle(t2_d.at[pl.ds(0, pairs - 1), :], s_t2)

    settle(t2_d.at[pl.ds(0, pairs - 1), :], r_t2)
    whole = jnp.sum(t2_d[...], axis=0, keepdims=True)
    out_mean[...] = whole[:, 0:1] / whole[:, 1:2]

    settle(sp_f, r_spf)
    settle(sp_i, r_spi)
    g = SPILL_ROWS
    pen_s, gap_s = sp_f[0, 0:g], sp_f[0, g:]
    key_s = encode(sp_i[0, 0:g], sp_i[0, g:])
    for r in range(1, n_rep):
        pen_s = jnp.maximum(pen_s, sp_f[r, 0:g])
        gap_s = gap_s + sp_f[r, g:]
        key_s = jnp.maximum(key_s, encode(sp_i[r, 0:g], sp_i[r, g:]))

    def finish(at, pen, key, gap):
        none = pen < LOWEST_FILL * 0.5
        out_pen[at, :] = jnp.where(none, 0.0, pen)
        out_face[at, :] = jnp.where(none, -1, FACE_MASK - (key & FACE_MASK))
        out_gap[at, :] = jnp.where(none, 0.0, gap)

    finish(
        slice(0, g), jnp.maximum(pen_o[:g], pen_s), jnp.maximum(key_o[:g], key_s), gap_o[:g] + gap_s
    )
    finish(slice(g, OWN_ROWS), pen_o[g:], key_o[g:], gap_o[g:])


def finish_kernel(force_ref, pen_ref, face_ref, gap_ref, mean_ref, force_h, pen_h, face_h, gap_h, mean_h, sems, s_force):
    copies = [
        pltpu.make_async_copy(held, out, sems.at[i])
        for i, (held, out) in enumerate((
            (pen_ref, pen_h), (face_ref, face_h), (gap_ref, gap_h), (mean_ref, mean_h)
        ))
    ]
    for at in range(0, force_ref.shape[0], SUB):
        part = (slice(at, at + SUB), slice(None))
        pltpu.make_async_copy(force_ref.at[part], force_h.at[part], s_force).start()
    for copy in copies:
        copy.start()
    for copy in copies:
        copy.wait()
    pltpu.make_async_copy(force_ref, force_h, s_force).wait()


def solution(mesh):
    n_dom, n_rep = mesh.shape["dom"], mesh.shape["rep"]
    vmem = pl.BlockSpec(memory_space=pltpu.VMEM)
    anywhere = pl.BlockSpec(memory_space=pl.ANY)
    dma = pltpu.SemaphoreType.DMA

    def kept(x):
        return pltpu.with_memory_space_constraint(x, pltpu.VMEM)

    def streamed(x):
        return pltpu.with_memory_space_constraint(x, pltpu.HBM)

    def shards(ns, nm, sec, mst, off, qw, jac, slot, face, rank, live):
        k_size, p_size = ns.shape
        rows = sec.shape[1]
        lines = rows // LANES
        depth = 2 * k_size + EXTRA
        f32, i32, bf16 = jnp.float32, jnp.int32, jnp.bfloat16

        off, jac, slot, face, rank = (x.reshape(lines, LANES) for x in (off, jac, slot, face, rank))

        def packs(deep):
            return [pltpu.VMEM((deep + SUB, LANES), t) for t in (i32, f32, i32, f32)]

        held = pl.pallas_call(
            prep_kernel,
            out_shape=(
                pltpu.VMEM((2 * k_size, rows), bf16),
                pltpu.VMEM((p_size + EXTRA, depth), bf16),
                pltpu.VMEM((2 * k_size, p_size), bf16),
                pltpu.VMEM((lines, LANES), f32),
                pltpu.VMEM((lines, LANES), f32),
                pltpu.VMEM((lines, LANES), i32),
                pltpu.VMEM((lines, LANES), i32),
                pltpu.VMEM((lines, LANES), i32),
                pltpu.VMEM((ALL_ROWS, LANES), f32),
                pltpu.VMEM((ALL_ROWS, LANES), i32),
                pltpu.VMEM((ALL_ROWS, LANES), f32),
                pltpu.VMEM((1, LANES), f32),
            ),
            in_specs=[anywhere] * 11,
            out_specs=(vmem,) * 12,
            scratch_shapes=[
                pltpu.VMEM((1, 1), i32),
                pltpu.VMEM((k_size, p_size), bf16),
                pltpu.VMEM((k_size, p_size), bf16),
                pltpu.VMEM((1, p_size), f32),
                pltpu.VMEM((lines, LANES), f32),
                pltpu.VMEM((lines, LANES), i32),
                pltpu.VMEM((lines, LANES), i32),
                pltpu.VMEM((lines, LANES), f32),
                pltpu.VMEM((lines, LANES), f32),
                packs(SUB),
                dma((9,)),
                dma,
            ],
            compiler_params=pltpu.CompilerParams(vmem_limit_bytes=VMEM_LIMIT),
        )(
            live.reshape(1, 1),
            *(streamed(x) for x in (ns, nm, qw.reshape(1, p_size), sec, mst, off, jac, slot, face, rank)),
        )

        spill = (2 * SPILL_ROWS, LANES)
        own = (2, OWN_ROWS, LANES)
        pairs = n_dom * n_rep // 2
        results = pl.pallas_call(
            functools.partial(main_kernel, n_dom, n_rep),
            out_shape=(
                pltpu.VMEM((k_size, rows), bf16),
                pltpu.VMEM((OWN_ROWS, LANES), f32),
                pltpu.VMEM((OWN_ROWS, LANES), i32),
                pltpu.VMEM((OWN_ROWS, LANES), f32),
                pltpu.VMEM((1, 1), f32),
            ),
            in_specs=[vmem] * 12,
            out_specs=(vmem,) * 5,
            scratch_shapes=[
                pltpu.VMEM((p_size, rows), bf16),
                pltpu.VMEM((lines, LANES), f32),
                pltpu.VMEM((lines, LANES), f32),
                packs(BATCH * DEPTH),
                pltpu.VMEM((OWN_ROWS, LANES), f32),
                pltpu.VMEM((OWN_ROWS, LANES), i32),
                pltpu.VMEM((OWN_ROWS, LANES), f32),
                pltpu.VMEM(spill, f32),
                pltpu.VMEM(spill, i32),
                pltpu.VMEM(own, f32),
                pltpu.VMEM(own, i32),
                pltpu.VMEM((1, LANES), f32),
                pltpu.VMEM((1, LANES), f32),
                pltpu.VMEM((n_rep,) + spill, f32),
                pltpu.VMEM((n_rep,) + spill, i32),
                pltpu.VMEM((n_rep,) + own, f32),
                pltpu.VMEM((n_rep,) + own, i32),
                pltpu.VMEM((1, LANES), f32),
                pltpu.VMEM((pairs, LANES), f32),
            ] + [dma] * 12 + [pltpu.SemaphoreType.REGULAR],
            compiler_params=pltpu.CompilerParams(
                collective_id=0, has_side_effects=True, vmem_limit_bytes=VMEM_LIMIT
            ),
        )(*(kept(x) for x in held))

        force, seg_pen, seg_face, seg_gap, mean = pl.pallas_call(
            finish_kernel,
            out_shape=tuple(jax.ShapeDtypeStruct(x.shape, x.dtype) for x in results),
            in_specs=[vmem] * 5,
            out_specs=(anywhere,) * 5,
            scratch_shapes=[dma((4,)), dma],
            compiler_params=pltpu.CompilerParams(vmem_limit_bytes=VMEM_LIMIT),
        )(*(kept(x) for x in results))
        seg_pen, seg_face, seg_gap = (x.reshape(SEG_DEV) for x in (seg_pen, seg_face, seg_gap))
        return force, seg_pen, seg_face, seg_gap, mean.reshape(())

    rows_spec, wide_spec = P(("dom", "rep")), P(None, ("dom", "rep"))
    return jax.shard_map(
        shards,
        mesh=mesh,
        in_specs=(P(), P(), wide_spec, wide_spec, rows_spec, P()) + (rows_spec,) * 5,
        out_specs=(wide_spec, P("dom"), P("dom"), P("dom"), P()),
        check_vma=False,
    )
```

```python
import functools

import jax
import jax.numpy as jnp
from jax import lax
from jax.experimental import pallas as pl
from jax.experimental.pallas import tpu as pltpu
from jax.sharding import PartitionSpec as P

SEG_DEV = 1024
SPILL = 256
LANES = 128
SUB = 8
WIDTH = 64
PER_ROW = LANES // WIDTH
GROUPS = (SEG_DEV + SPILL) // WIDTH
OWN_GROUPS = SEG_DEV // WIDTH
SPILL_GROUPS = SPILL // WIDTH
OWN_ROWS = SEG_DEV // LANES
SPILL_ROWS = SPILL // LANES
ALL_ROWS = 16
CODE = 32

PENALTY = 400.0
LOWEST_FILL = -1e30
FACE_LIMIT = 1073741824
FACE_MASK = FACE_LIMIT - 1
KEY_LOW = -2147483648
MESH = pl.DeviceIdType.MESH
TILE = 256
DEPTH = 12
BATCH = 4
UNROLL = 16
CHAINS = 4
FORCE_UNROLL = 8
LOOP_UNROLL = 4
EXTRA = 16
VMEM_LIMIT = 32 << 20


def split3(x):
    a = x.astype(jnp.bfloat16)
    rest = x - a.astype(jnp.float32)
    b = rest.astype(jnp.bfloat16)
    c = (rest - b.astype(jnp.float32)).astype(jnp.bfloat16)
    return a, b, c


def row(ref, at):
    return ref[pl.ds(at, SUB, stride=0), :]


def pull_groups(first, count, depth0, depth, code_ref, sources, packs):
    all_lines = code_ref.shape[0]
    sub = lax.broadcasted_iota(jnp.int32, (SUB, LANES), 0)
    blocks = -(-count * depth // SUB)
    wants = []
    for b in range(blocks):
        line = sub + SUB * b
        want = jnp.full((SUB, LANES), -2, jnp.int32)
        for q in range(count):
            inside = (line >= q * depth) & (line < (q + 1) * depth)
            want = jnp.where(inside, (line + (depth0 - q * depth)) * CODE + (first + q), want)
        wants.append(want)
    fills = (-1, LOWEST_FILL, -1, 0.0)

    def pull(i, carry):
        parts = [list(part) for part in carry]
        code = row(code_ref, i)
        values = [row(ref, i) for ref in sources]
        for b in range(blocks):
            hit = code == wants[b]
            for part, value in zip(parts, values):
                part[b] = jnp.where(hit, value, part[b])
        return tuple(tuple(part) for part in parts)

    start = tuple(
        (jnp.full((SUB, LANES), fill, ref.dtype),) * blocks for fill, ref in zip(fills, sources)
    )
    pulled = lax.fori_loop(0, all_lines, pull, start, unroll=8)
    for ref, parts in zip(packs, pulled):
        for b in range(blocks):
            ref[SUB * b : SUB * (b + 1), :] = parts[b]


def match_group(g, at, depth, packs, unroll):
    sub = lax.broadcasted_iota(jnp.int32, (SUB, LANES), 0)
    tiles = WIDTH // SUB
    marks = [sub + (g * WIDTH + SUB * q) for q in range(tiles)]
    start = (
        (jnp.full((SUB, LANES), LOWEST_FILL, jnp.float32),) * tiles,
        (jnp.full((SUB, LANES), KEY_LOW, jnp.int32),) * tiles,
        (jnp.zeros((SUB, LANES), jnp.float32),) * tiles,
    )

    def one(j, carry):
        pens, keys, gaps = (list(part) for part in carry)
        slot, pen, key, gap = (row(ref, at + j) for ref in packs)
        for q in range(tiles):
            hit = slot == marks[q]
            pens[q] = jnp.maximum(pens[q], jnp.where(hit, pen, LOWEST_FILL))
            keys[q] = jnp.maximum(keys[q], jnp.where(hit, key, KEY_LOW))
            gaps[q] = gaps[q] + jnp.where(hit, gap, 0.0)
        return tuple(pens), tuple(keys), tuple(gaps)

    if unroll == depth:
        for j in range(depth):
            start = one(j, start)
        return start
    return lax.fori_loop(0, depth, one, start, unroll=unroll)


def keep_group(accs, side, parts):
    for ref, part in zip(accs, parts):
        for q in range(WIDTH // SUB):
            at = side * WIDTH + q * SUB
            ref[at : at + SUB, :] = part[q]


def across(accs):
    pens, keys, gaps = (ref[...].T for ref in accs)
    return (
        jnp.max(pens, axis=0, keepdims=True),
        jnp.max(keys, axis=0, keepdims=True),
        jnp.sum(gaps, axis=0, keepdims=True),
    )


def project(wt, x_ref, off_ref, tile):
    cols = pl.ds(tile * TILE, TILE)
    per_tile = TILE // LANES
    offset = jnp.concatenate([row(off_ref, tile * per_tile + i) for i in range(per_tile)], axis=1)
    sub = lax.broadcasted_iota(jnp.int32, (SUB, TILE), 0)
    a, b, c = (part.astype(jnp.float32) for part in split3(offset))
    extra = jnp.where(sub == 0, a, jnp.where(sub == 1, b, jnp.where(sub == 2, c, 0.0)))
    extra = jnp.concatenate([extra, jnp.zeros((EXTRA - SUB, TILE), jnp.float32)], axis=0)
    x = jnp.concatenate([x_ref[:, cols], extra.astype(jnp.bfloat16)], axis=0)
    return jnp.dot(wt, x, preferred_element_type=jnp.float32)


def store_row(ref, tile, value):
    per_tile = TILE // LANES
    for i in range(per_tile):
        ref[pl.ds(tile * per_tile + i, 1), :] = value[:, i * LANES : (i + 1) * LANES]


def reduce_field(field, p_size, tile, pen_ref, gap_ref):
    low = [field[SUB * j : SUB * (j + 1)] for j in range(CHAINS)]
    for j in range(CHAINS, p_size // SUB):
        low[j % CHAINS] = jnp.minimum(low[j % CHAINS], field[SUB * j : SUB * (j + 1)])
    store_row(pen_ref, tile, -jnp.min(functools.reduce(jnp.minimum, low), axis=0, keepdims=True))
    store_row(gap_ref, tile, jnp.sum(field[p_size : p_size + SUB], axis=0, keepdims=True))


def prep_kernel(
    live_h, ns_h, nm_h, qw_h, sec_h, mst_h, off_h, jac_h, slot_h, face_h, rank_h,
    x_ref, wt_ref, nq_ref, off_ref, jl_ref, slot_ref, code_ref, key_ref, over_pen, over_key, over_gap, area_ref,
    live_s, ns_ref, nm_ref, qw_ref, jac_ref, face_ref, rank_ref, pen_ref, gap_ref, packs, accs, s_small, s_big,
):
    lines = slot_ref.shape[0]
    k_size, p_size = ns_ref.shape
    rows = x_ref.shape[1]

    small = [
        pltpu.make_async_copy(source, held, s_small.at[i])
        for i, (source, held) in enumerate((
            (slot_h, slot_ref), (live_h, live_s), (ns_h, ns_ref), (nm_h, nm_ref), (qw_h, qw_ref),
            (face_h, face_ref), (rank_h, rank_ref), (jac_h, jac_ref), (off_h, off_ref),
        ))
    ]
    for copy in small:
        copy.start()
    for base, source in ((0, sec_h), (k_size, mst_h)):
        for at in range(0, k_size, 2 * SUB):
            pltpu.make_async_copy(
                source.at[at : at + 2 * SUB, :], x_ref.at[base + at : base + at + 2 * SUB, :], s_big
            ).start()
    for copy in small:
        copy.wait()

    row_id = (
        lax.broadcasted_iota(jnp.int32, (lines, LANES), 0) * LANES
        + lax.broadcasted_iota(jnp.int32, (lines, LANES), 1)
    )
    alive = row_id < live_s[...]
    group = jnp.where(alive, slot_ref[...] // WIDTH, -1)
    before = (
        lax.broadcasted_iota(jnp.int32, (lines, lines), 1)
        < lax.broadcasted_iota(jnp.int32, (lines, lines), 0)
    )
    before = jnp.where(before, 1.0, 0.0).astype(jnp.bfloat16)
    place = jnp.zeros((lines, LANES), jnp.float32)
    for g in range(0, GROUPS, 2):
        mine = [group == g, group == g + 1]
        seen = jnp.concatenate([jnp.where(m, 1.0, 0.0).astype(jnp.bfloat16) for m in mine], axis=1)
        found = jnp.dot(before, seen, preferred_element_type=jnp.float32)
        place = jnp.where(mine[0], found[:, :LANES], jnp.where(mine[1], found[:, LANES:], place))
    code = jnp.where(alive, place.astype(jnp.int32) * CODE + group, -1)
    code_ref[...] = code
    worst = jnp.max(code)

    w = jnp.concatenate([ns_ref[...], -nm_ref[...]], axis=0).astype(jnp.float32)
    qrow = qw_ref[...]
    wt = w.T
    qmat = jnp.broadcast_to(qrow, (LANES, p_size)).T
    v = jnp.sum(wt * qmat, axis=0, keepdims=True)
    qsum = jnp.sum(qmat, axis=0, keepdims=True)
    depth = wt_ref.shape[1]
    pick = lax.broadcasted_iota(jnp.int32, (EXTRA, depth), 0)
    column = lax.broadcasted_iota(jnp.int32, (p_size, depth - 2 * k_size), 1)
    wt_ref[0:p_size, 0 : 2 * k_size] = wt.astype(jnp.bfloat16)
    wt_ref[0:p_size, 2 * k_size :] = jnp.where(column < 3, 1.0, 0.0).astype(jnp.bfloat16)
    lane_row = lax.broadcasted_iota(jnp.int32, (1, LANES), 1)
    tail = jnp.where(lane_row < 3, qsum, 0.0)[:, : depth - 2 * k_size]
    a, b, c = (part.astype(jnp.float32) for part in split3(jnp.concatenate([v, tail], axis=1)))
    stacked = jnp.where(pick == 0, a, jnp.where(pick == 1, b, jnp.where(pick == 2, c, 0.0)))
    wt_ref[p_size:, :] = stacked.astype(jnp.bfloat16)
    scaled = ns_ref[...].astype(jnp.float32) * qrow
    top = scaled.astype(jnp.bfloat16)
    low = (scaled - top.astype(jnp.float32)).astype(jnp.bfloat16)
    nq_ref[...] = jnp.concatenate([top, low], axis=0)

    key_ref[...] = ((rank_ref[...] - 2) << 30) + (FACE_MASK - face_ref[...])
    jl = jnp.where(alive, jac_ref[...], 0.0)
    jl_ref[...] = jl
    area_ref[...] = jnp.sum(jl, axis=0, keepdims=True) * jnp.sum(qrow, axis=1, keepdims=True)
    over_pen[...] = jnp.full(over_pen.shape, LOWEST_FILL, jnp.float32)
    over_key[...] = jnp.full(over_key.shape, KEY_LOW, jnp.int32)
    over_gap[...] = jnp.zeros(over_gap.shape, jnp.float32)

    pltpu.make_async_copy(x_ref, x_ref, s_big).wait()

    @pl.when(worst >= DEPTH * CODE)
    def _():
        weights = wt_ref[...]

        def fill(tile, carry):
            reduce_field(project(weights, x_ref, off_ref, tile), p_size, tile, pen_ref, gap_ref)
            return carry

        lax.fori_loop(0, rows // TILE, fill, 0)
        gap_ref[...] = gap_ref[...] * jl_ref[...]
        face_ref[...] = code_ref[...]

        def one(worst):
            code = face_ref[...]
            g = worst & (CODE - 1)
            low = jnp.maximum((worst // CODE) & -SUB, DEPTH)
            pull_groups(g, 1, low, SUB, face_ref, (slot_ref, pen_ref, key_ref, gap_ref), packs)
            found = match_group(g, 0, SUB, packs, 2)
            odd = jnp.full((SUB, LANES), g & 1, jnp.int32)
            for side in range(PER_ROW):
                keep_group(accs, side, [
                    [jnp.where(odd == side, x, fill) for x in part]
                    for part, fill in zip(found, (LOWEST_FILL, KEY_LOW, 0.0))
                ])
            pen, key, gap = across(accs)
            at = pl.ds(g // PER_ROW, 1)
            over_pen[at, :] = jnp.maximum(over_pen[at, :], pen)
            over_key[at, :] = jnp.maximum(over_key[at, :], key)
            over_gap[at, :] = over_gap[at, :] + gap
            done = ((code & (CODE - 1)) == g) & (code >= low * CODE)
            code = jnp.where(done, -1, code)
            face_ref[...] = code
            return jnp.max(code)

        lax.while_loop(lambda worst: worst >= DEPTH * CODE, one, worst)


def main_kernel(
    n_dom, n_rep,
    x_ref, wt_ref, nq_ref, off_ref, jl_ref, slot_ref, code_ref, key_ref, over_pen, over_key, over_gap, area_ref,
    force_ref, out_pen, out_face, out_gap, out_mean,
    load_ref, pen_ref, gap_ref, packs, even_accs, odd_accs, raw_pen, raw_key, raw_gap,
    sp_sf, sp_si, ow_sf, ow_si, t1_s, t2_s, sp_f, sp_i, ow_f, ow_i, t1_d, t2_d,
    s_spf, r_spf, s_spi, r_spi, s_owf, r_owf, s_owi, r_owi, s_t1, r_t1, s_t2, r_t2, inside,
):
    dom = lax.axis_index("dom")
    rep = lax.axis_index("rep")
    k_size = force_ref.shape[0]
    rows = force_ref.shape[1]
    p_size = load_ref.shape[0]
    per_tile = TILE // LANES
    tiles = rows // TILE
    count = n_dom * n_rep
    me = dom * n_rep + rep

    def dev(d, r):
        return {"dom": lax.rem(d + n_dom, n_dom), "rep": lax.rem(r + n_rep, n_rep)}

    def flat_dev(flat):
        return dev(lax.div(flat, n_rep), lax.rem(flat, n_rep))

    barrier = pltpu.get_barrier_semaphore()

    def signal(sem, first, last):
        def one(flat, carry):
            pl.semaphore_signal(sem, inc=1, device_id=flat_dev(flat), device_id_type=MESH)
            return carry

        lax.fori_loop(first, last, one, 0)

    signal(barrier, me + 1, count)
    signal(barrier, dom * n_rep, me)
    signal(barrier, jnp.maximum(dom - 1, 0) * n_rep, dom * n_rep)

    wt = wt_ref[...]

    def wide_row(ref, tile):
        return jnp.concatenate([row(ref, tile * per_tile + i) for i in range(per_tile)], axis=1)

    def batch(step, carry):
        for i in range(UNROLL):
            tile = step * UNROLL + i
            cols = pl.ds(tile * TILE, TILE)
            field = project(wt, x_ref, off_ref, tile)
            for at in range(0, p_size, 2 * SUB):
                load_ref[at : at + 2 * SUB, cols] = jnp.minimum(field[at : at + 2 * SUB].astype(jnp.bfloat16), 0)
            reduce_field(field, p_size, tile, pen_ref, gap_ref)
        return carry

    lax.fori_loop(0, tiles // UNROLL, batch, 0)
    row_gap = gap_ref[...] * jl_ref[...]
    gap_ref[...] = row_gap
    total_gap = jnp.sum(jnp.sum(row_gap, axis=0, keepdims=True), axis=1, keepdims=True)
    total_area = jnp.sum(area_ref[...], axis=1, keepdims=True)
    lane = lax.broadcasted_iota(jnp.int32, (1, LANES), 1)
    t1_s[...] = jnp.where(lane == 0, total_gap, jnp.where(lane == 1, total_area, 0.0))

    after = n_rep * jnp.where(dom < n_dom - 1, 1, 0)
    pl.semaphore_wait(barrier, me + (n_rep - 1 - rep) + after)
    signal(inside, 0, me)

    mate = rep + 1 - 2 * lax.rem(rep, 2)
    first_copy = pltpu.make_async_remote_copy(
        src_ref=t1_s, dst_ref=t1_d, send_sem=s_t1, recv_sem=r_t1,
        device_id=dev(dom, mate), device_id_type=MESH,
    )
    first_copy.start()

    def pull_batch(first):
        pull_groups(first, BATCH, 0, DEPTH, code_ref, (slot_ref, pen_ref, key_ref, gap_ref), packs)

    def match_pair(first, i, accs, last_accs, over, at):
        g = first + i * PER_ROW
        keep_group(accs, 0, match_group(g, i * PER_ROW * DEPTH, DEPTH, packs, LOOP_UNROLL))
        if last_accs is not None:
            close_pair(last_accs, over, at)
        keep_group(accs, 1, match_group(g + 1, (i * PER_ROW + 1) * DEPTH, DEPTH, packs, DEPTH))

    def close_pair(accs, over, at):
        pen, key, gap = across(accs)
        over, at = pl.ds(over, 1), pl.ds(at, 1)
        raw_pen[at, :] = jnp.maximum(pen, over_pen[over, :])
        raw_key[at, :] = jnp.maximum(key, over_key[over, :])
        raw_gap[at, :] = gap + over_gap[over, :]

    def decode(top, best):
        none = top < LOWEST_FILL * 0.5
        rank = jnp.where(none, -1, (best >> 30) + 2)
        face = jnp.where(none, FACE_LIMIT, FACE_MASK - (best & FACE_MASK))
        return rank, face

    pull_batch(OWN_GROUPS)
    match_pair(OWN_GROUPS, 0, even_accs, None, 0, 0)
    match_pair(OWN_GROUPS, 1, odd_accs, even_accs, OWN_ROWS, 0)
    close_pair(odd_accs, OWN_ROWS + 1, 1)
    part = slice(0, SPILL_ROWS)
    rank, face = decode(raw_pen[part, :], raw_key[part, :])
    sp_sf[0:SPILL_ROWS, :] = raw_pen[part, :]
    sp_sf[SPILL_ROWS:, :] = raw_gap[part, :]
    sp_si[0:SPILL_ROWS, :] = rank
    sp_si[SPILL_ROWS:, :] = face

    def spill_copy(j):
        where = dev(dom + 1, rep + j)
        return (
            pltpu.make_async_remote_copy(
                src_ref=sp_sf, dst_ref=sp_f.at[rep], send_sem=s_spf, recv_sem=r_spf,
                device_id=where, device_id_type=MESH,
            ),
            pltpu.make_async_remote_copy(
                src_ref=sp_si, dst_ref=sp_i.at[rep], send_sem=s_spi, recv_sem=r_spi,
                device_id=where, device_id_type=MESH,
            ),
        )

    for j in range(n_rep):
        for copy in spill_copy(j):
            copy.start()

    first_copy.wait_recv()
    pairs = count // 2
    pair = lax.div(me, 2)
    both = t1_s[...] + t1_d[...]
    t2_s[...] = both
    t2_d[pl.ds(pair, 1), :] = both

    def send_pairs(first, last):
        def one(other, carry):
            pltpu.make_async_remote_copy(
                src_ref=t2_s, dst_ref=t2_d.at[pl.ds(pair, 1), :], send_sem=s_t2, recv_sem=r_t2,
                device_id=flat_dev(other * 2 + lax.rem(rep, 2)), device_id_type=MESH,
            ).start()
            return carry

        lax.fori_loop(first, last, one, 0)

    send_pairs(0, pair)

    def send_up():
        @pl.when(me < count - 1)
        def _():
            pl.semaphore_wait(inside, count - 1 - me)

        send_pairs(pair + 1, pairs)

    late = me >= count // 2

    @pl.when(late)
    def _():
        send_up()

    def own_scan(i, carry):
        first = i * BATCH
        last = lax.rem(2 * i + OWN_ROWS - 1, OWN_ROWS)
        pull_batch(first)
        match_pair(first, 0, even_accs, odd_accs, last, last)
        match_pair(first, 1, odd_accs, even_accs, 2 * i, 2 * i)
        return carry

    lax.fori_loop(0, OWN_GROUPS // BATCH, own_scan, 0)
    close_pair(odd_accs, OWN_ROWS - 1, OWN_ROWS - 1)
    rank, face = decode(raw_pen[...], raw_key[...])
    ow_sf[0] = raw_pen[...]
    ow_sf[1] = raw_gap[...]
    ow_si[0] = rank
    ow_si[1] = face

    def own_copy(j):
        where = dev(dom, rep + j)
        return (
            pltpu.make_async_remote_copy(
                src_ref=ow_sf, dst_ref=ow_f.at[rep], send_sem=s_owf, recv_sem=r_owf,
                device_id=where, device_id_type=MESH,
            ),
            pltpu.make_async_remote_copy(
                src_ref=ow_si, dst_ref=ow_i.at[rep], send_sem=s_owi, recv_sem=r_owi,
                device_id=where, device_id_type=MESH,
            ),
        )

    for j in range(1, n_rep):
        for copy in own_copy(j):
            copy.start()
    ow_f[rep] = ow_sf[...]
    ow_i[rep] = ow_si[...]

    @pl.when(jnp.logical_not(late))
    def _():
        send_up()

    nq = nq_ref[...]

    def push(step, carry):
        for i in range(FORCE_UNROLL):
            tile = step * FORCE_UNROLL + i
            cols = pl.ds(tile * TILE, TILE)
            force = jnp.dot(nq, load_ref[:, cols], preferred_element_type=jnp.float32)
            scale = wide_row(jl_ref, tile)[0:1] * -PENALTY
            force_ref[:, cols] = ((force[:k_size] + force[k_size:]) * scale).astype(jnp.bfloat16)
        return carry

    lax.fori_loop(0, tiles // FORCE_UNROLL, push, 0)

    def encode(rank, face):
        return jnp.where(rank < 0, KEY_LOW, ((rank - 2) << 30) + (FACE_MASK - face))

    def settle(ref, sem):
        pltpu.make_async_copy(ref, ref, sem).wait()

    settle(ow_f.at[pl.ds(0, n_rep - 1)], r_owf)
    settle(ow_i.at[pl.ds(0, n_rep - 1)], r_owi)
    pen_o, gap_o = ow_f[0, 0], ow_f[0, 1]
    key_o = encode(ow_i[0, 0], ow_i[0, 1])
    for r in range(1, n_rep):
        pen_o = jnp.maximum(pen_o, ow_f[r, 0])
        gap_o = gap_o + ow_f[r, 1]
        key_o = jnp.maximum(key_o, encode(ow_i[r, 0], ow_i[r, 1]))

    settle(sp_f, s_spf)
    settle(sp_i, s_spi)
    settle(ow_f.at[pl.ds(0, n_rep - 1)], s_owf)
    settle(ow_i.at[pl.ds(0, n_rep - 1)], s_owi)
    first_copy.wait_send()
    settle(t2_d.at[pl.ds(0, pairs - 1), :], s_t2)

    settle(t2_d.at[pl.ds(0, pairs - 1), :], r_t2)
    whole = jnp.sum(t2_d[...], axis=0, keepdims=True)
    out_mean[...] = whole[:, 0:1] / whole[:, 1:2]

    settle(sp_f, r_spf)
    settle(sp_i, r_spi)
    g = SPILL_ROWS
    pen_s, gap_s = sp_f[0, 0:g], sp_f[0, g:]
    key_s = encode(sp_i[0, 0:g], sp_i[0, g:])
    for r in range(1, n_rep):
        pen_s = jnp.maximum(pen_s, sp_f[r, 0:g])
        gap_s = gap_s + sp_f[r, g:]
        key_s = jnp.maximum(key_s, encode(sp_i[r, 0:g], sp_i[r, g:]))

    def finish(at, pen, key, gap):
        none = pen < LOWEST_FILL * 0.5
        out_pen[at, :] = jnp.where(none, 0.0, pen)
        out_face[at, :] = jnp.where(none, -1, FACE_MASK - (key & FACE_MASK))
        out_gap[at, :] = jnp.where(none, 0.0, gap)

    finish(
        slice(0, g), jnp.maximum(pen_o[:g], pen_s), jnp.maximum(key_o[:g], key_s), gap_o[:g] + gap_s
    )
    finish(slice(g, OWN_ROWS), pen_o[g:], key_o[g:], gap_o[g:])


def finish_kernel(force_ref, pen_ref, face_ref, gap_ref, mean_ref, force_h, pen_h, face_h, gap_h, mean_h, sems, s_force):
    copies = [
        pltpu.make_async_copy(held, out, sems.at[i])
        for i, (held, out) in enumerate((
            (pen_ref, pen_h), (face_ref, face_h), (gap_ref, gap_h), (mean_ref, mean_h)
        ))
    ]
    for at in range(0, force_ref.shape[0], SUB):
        part = (slice(at, at + SUB), slice(None))
        pltpu.make_async_copy(force_ref.at[part], force_h.at[part], s_force).start()
    for copy in copies:
        copy.start()
    for copy in copies:
        copy.wait()
    pltpu.make_async_copy(force_ref, force_h, s_force).wait()


def solution(mesh):
    n_dom, n_rep = mesh.shape["dom"], mesh.shape["rep"]
    vmem = pl.BlockSpec(memory_space=pltpu.VMEM)
    anywhere = pl.BlockSpec(memory_space=pl.ANY)
    dma = pltpu.SemaphoreType.DMA

    def kept(x):
        return pltpu.with_memory_space_constraint(x, pltpu.VMEM)

    def streamed(x):
        return pltpu.with_memory_space_constraint(x, pltpu.HBM)

    def shards(ns, nm, sec, mst, off, qw, jac, slot, face, rank, live):
        k_size, p_size = ns.shape
        rows = sec.shape[1]
        lines = rows // LANES
        depth = 2 * k_size + EXTRA
        f32, i32, bf16 = jnp.float32, jnp.int32, jnp.bfloat16

        off, jac, slot, face, rank = (x.reshape(lines, LANES) for x in (off, jac, slot, face, rank))

        def packs(deep):
            return [pltpu.VMEM((deep + SUB, LANES), t) for t in (i32, f32, i32, f32)]

        def lanes():
            return [pltpu.VMEM((LANES, LANES), t) for t in (f32, i32, f32)]

        held = pl.pallas_call(
            prep_kernel,
            out_shape=(
                pltpu.VMEM((2 * k_size, rows), bf16),
                pltpu.VMEM((p_size + EXTRA, depth), bf16),
                pltpu.VMEM((2 * k_size, p_size), bf16),
                pltpu.VMEM((lines, LANES), f32),
                pltpu.VMEM((lines, LANES), f32),
                pltpu.VMEM((lines, LANES), i32),
                pltpu.VMEM((lines, LANES), i32),
                pltpu.VMEM((lines, LANES), i32),
                pltpu.VMEM((ALL_ROWS, LANES), f32),
                pltpu.VMEM((ALL_ROWS, LANES), i32),
                pltpu.VMEM((ALL_ROWS, LANES), f32),
                pltpu.VMEM((1, LANES), f32),
            ),
            in_specs=[anywhere] * 11,
            out_specs=(vmem,) * 12,
            scratch_shapes=[
                pltpu.VMEM((1, 1), i32),
                pltpu.VMEM((k_size, p_size), bf16),
                pltpu.VMEM((k_size, p_size), bf16),
                pltpu.VMEM((1, p_size), f32),
                pltpu.VMEM((lines, LANES), f32),
                pltpu.VMEM((lines, LANES), i32),
                pltpu.VMEM((lines, LANES), i32),
                pltpu.VMEM((lines, LANES), f32),
                pltpu.VMEM((lines, LANES), f32),
                packs(SUB),
                lanes(),
                dma((9,)),
                dma,
            ],
            compiler_params=pltpu.CompilerParams(vmem_limit_bytes=VMEM_LIMIT),
        )(
            live.reshape(1, 1),
            *(streamed(x) for x in (ns, nm, qw.reshape(1, p_size), sec, mst, off, jac, slot, face, rank)),
        )

        spill = (2 * SPILL_ROWS, LANES)
        own = (2, OWN_ROWS, LANES)
        pairs = n_dom * n_rep // 2
        results = pl.pallas_call(
            functools.partial(main_kernel, n_dom, n_rep),
            out_shape=(
                pltpu.VMEM((k_size, rows), bf16),
                pltpu.VMEM((OWN_ROWS, LANES), f32),
                pltpu.VMEM((OWN_ROWS, LANES), i32),
                pltpu.VMEM((OWN_ROWS, LANES), f32),
                pltpu.VMEM((1, 1), f32),
            ),
            in_specs=[vmem] * 12,
            out_specs=(vmem,) * 5,
            scratch_shapes=[
                pltpu.VMEM((p_size, rows), bf16),
                pltpu.VMEM((lines, LANES), f32),
                pltpu.VMEM((lines, LANES), f32),
                packs(BATCH * DEPTH),
                lanes(),
                lanes(),
                pltpu.VMEM((OWN_ROWS, LANES), f32),
                pltpu.VMEM((OWN_ROWS, LANES), i32),
                pltpu.VMEM((OWN_ROWS, LANES), f32),
                pltpu.VMEM(spill, f32),
                pltpu.VMEM(spill, i32),
                pltpu.VMEM(own, f32),
                pltpu.VMEM(own, i32),
                pltpu.VMEM((1, LANES), f32),
                pltpu.VMEM((1, LANES), f32),
                pltpu.VMEM((n_rep,) + spill, f32),
                pltpu.VMEM((n_rep,) + spill, i32),
                pltpu.VMEM((n_rep,) + own, f32),
                pltpu.VMEM((n_rep,) + own, i32),
                pltpu.VMEM((1, LANES), f32),
                pltpu.VMEM((pairs, LANES), f32),
            ] + [dma] * 12 + [pltpu.SemaphoreType.REGULAR],
            compiler_params=pltpu.CompilerParams(
                collective_id=0, has_side_effects=True, vmem_limit_bytes=VMEM_LIMIT
            ),
        )(*(kept(x) for x in held))

        force, seg_pen, seg_face, seg_gap, mean = pl.pallas_call(
            finish_kernel,
            out_shape=tuple(jax.ShapeDtypeStruct(x.shape, x.dtype) for x in results),
            in_specs=[vmem] * 5,
            out_specs=(anywhere,) * 5,
            scratch_shapes=[dma((4,)), dma],
            compiler_params=pltpu.CompilerParams(vmem_limit_bytes=VMEM_LIMIT),
        )(*(kept(x) for x in results))
        seg_pen, seg_face, seg_gap = (x.reshape(SEG_DEV) for x in (seg_pen, seg_face, seg_gap))
        return force, seg_pen, seg_face, seg_gap, mean.reshape(())

    rows_spec, wide_spec = P(("dom", "rep")), P(None, ("dom", "rep"))
    return jax.shard_map(
        shards,
        mesh=mesh,
        in_specs=(P(), P(), wide_spec, wide_spec, rows_spec, P()) + (rows_spec,) * 5,
        out_specs=(wide_spec, P("dom"), P("dom"), P("dom"), P()),
        check_vma=False,
    )
```

```python
import functools

import jax
import jax.numpy as jnp
from jax import lax
from jax.experimental import pallas as pl
from jax.experimental.pallas import tpu as pltpu
from jax.sharding import PartitionSpec as P

SEG_DEV = 1024
SPILL = 256
LANES = 128
SUB = 8
WIDTH = 64
PER_ROW = LANES // WIDTH
GROUPS = (SEG_DEV + SPILL) // WIDTH
OWN_GROUPS = SEG_DEV // WIDTH
SPILL_GROUPS = SPILL // WIDTH
OWN_ROWS = SEG_DEV // LANES
SPILL_ROWS = SPILL // LANES
ALL_ROWS = 16
CODE = 32

PENALTY = 400.0
LOWEST_FILL = -1e30
FACE_LIMIT = 1073741824
FACE_MASK = FACE_LIMIT - 1
KEY_LOW = -2147483648
MESH = pl.DeviceIdType.MESH
TILE = 256
DEPTH = 12
BATCH = 4
OWN_BATCHES = OWN_GROUPS // BATCH
UNROLL = 16
CHAINS = 4
FORCE_UNROLL = 8
LOOP_UNROLL = 4
EXTRA = 16
VMEM_LIMIT = 32 << 20


def split3(x):
    a = x.astype(jnp.bfloat16)
    rest = x - a.astype(jnp.float32)
    b = rest.astype(jnp.bfloat16)
    c = (rest - b.astype(jnp.float32)).astype(jnp.bfloat16)
    return a, b, c


def row(ref, at):
    return ref[pl.ds(at, SUB, stride=0), :]


def pull_groups(first, count, depth0, depth, code_ref, sources, packs):
    all_lines = code_ref.shape[0]
    sub = lax.broadcasted_iota(jnp.int32, (SUB, LANES), 0)
    blocks = -(-count * depth // SUB)
    wants = []
    for b in range(blocks):
        line = sub + SUB * b
        want = jnp.full((SUB, LANES), -2, jnp.int32)
        for q in range(count):
            inside = (line >= q * depth) & (line < (q + 1) * depth)
            want = jnp.where(inside, (line + (depth0 - q * depth)) * CODE + (first + q), want)
        wants.append(want)
    fills = (-1, LOWEST_FILL, -1, 0.0)

    def pull(i, carry):
        parts = [list(part) for part in carry]
        code = row(code_ref, i)
        values = [row(ref, i) for ref in sources]
        for b in range(blocks):
            hit = code == wants[b]
            for part, value in zip(parts, values):
                part[b] = jnp.where(hit, value, part[b])
        return tuple(tuple(part) for part in parts)

    start = tuple(
        (jnp.full((SUB, LANES), fill, ref.dtype),) * blocks for fill, ref in zip(fills, sources)
    )
    pulled = lax.fori_loop(0, all_lines, pull, start, unroll=8)
    for ref, parts in zip(packs, pulled):
        for b in range(blocks):
            ref[SUB * b : SUB * (b + 1), :] = parts[b]


def match_group(g, at, depth, packs, unroll):
    sub = lax.broadcasted_iota(jnp.int32, (SUB, LANES), 0)
    tiles = WIDTH // SUB
    marks = [sub + (g * WIDTH + SUB * q) for q in range(tiles)]
    start = (
        (jnp.full((SUB, LANES), LOWEST_FILL, jnp.float32),) * tiles,
        (jnp.full((SUB, LANES), KEY_LOW, jnp.int32),) * tiles,
        (jnp.zeros((SUB, LANES), jnp.float32),) * tiles,
    )

    def one(j, carry):
        pens, keys, gaps = (list(part) for part in carry)
        slot, pen, key, gap = (row(ref, at + j) for ref in packs)
        for q in range(tiles):
            hit = slot == marks[q]
            pens[q] = jnp.maximum(pens[q], jnp.where(hit, pen, LOWEST_FILL))
            keys[q] = jnp.maximum(keys[q], jnp.where(hit, key, KEY_LOW))
            gaps[q] = gaps[q] + jnp.where(hit, gap, 0.0)
        return tuple(pens), tuple(keys), tuple(gaps)

    if unroll == depth:
        for j in range(depth):
            start = one(j, start)
        return start
    return lax.fori_loop(0, depth, one, start, unroll=unroll)


def keep_group(accs, side, parts):
    for ref, part in zip(accs, parts):
        for q in range(WIDTH // SUB):
            at = side * WIDTH + q * SUB
            ref[at : at + SUB, :] = part[q]


def across(accs):
    pens, keys, gaps = (ref[...].T for ref in accs)
    return (
        jnp.max(pens, axis=0, keepdims=True),
        jnp.max(keys, axis=0, keepdims=True),
        jnp.sum(gaps, axis=0, keepdims=True),
    )


def project(wt, x_ref, off_ref, tile):
    cols = pl.ds(tile * TILE, TILE)
    per_tile = TILE // LANES
    offset = jnp.concatenate([row(off_ref, tile * per_tile + i) for i in range(per_tile)], axis=1)
    sub = lax.broadcasted_iota(jnp.int32, (SUB, TILE), 0)
    a, b, c = (part.astype(jnp.float32) for part in split3(offset))
    extra = jnp.where(sub == 0, a, jnp.where(sub == 1, b, jnp.where(sub == 2, c, 0.0)))
    extra = jnp.concatenate([extra, jnp.zeros((EXTRA - SUB, TILE), jnp.float32)], axis=0)
    x = jnp.concatenate([x_ref[:, cols], extra.astype(jnp.bfloat16)], axis=0)
    return jnp.dot(wt, x, preferred_element_type=jnp.float32)


def store_row(ref, tile, value):
    per_tile = TILE // LANES
    for i in range(per_tile):
        ref[pl.ds(tile * per_tile + i, 1), :] = value[:, i * LANES : (i + 1) * LANES]


def reduce_field(field, p_size, tile, pen_ref, gap_ref):
    low = [field[SUB * j : SUB * (j + 1)] for j in range(CHAINS)]
    for j in range(CHAINS, p_size // SUB):
        low[j % CHAINS] = jnp.minimum(low[j % CHAINS], field[SUB * j : SUB * (j + 1)])
    store_row(pen_ref, tile, -jnp.min(functools.reduce(jnp.minimum, low), axis=0, keepdims=True))
    store_row(gap_ref, tile, jnp.sum(field[p_size : p_size + SUB], axis=0, keepdims=True))


def prep_kernel(
    live_h, ns_h, nm_h, qw_h, sec_h, mst_h, off_h, jac_h, slot_h, face_h, rank_h,
    x_ref, wt_ref, nq_ref, off_ref, jl_ref, slot_ref, code_ref, key_ref, over_pen, over_key, over_gap, area_ref,
    live_s, ns_ref, nm_ref, qw_ref, jac_ref, face_ref, rank_ref, pen_ref, gap_ref, packs, accs, s_small, s_big,
):
    lines = slot_ref.shape[0]
    k_size, p_size = ns_ref.shape
    rows = x_ref.shape[1]

    small = [
        pltpu.make_async_copy(source, held, s_small.at[i])
        for i, (source, held) in enumerate((
            (slot_h, slot_ref), (live_h, live_s), (ns_h, ns_ref), (nm_h, nm_ref), (qw_h, qw_ref),
            (face_h, face_ref), (rank_h, rank_ref), (jac_h, jac_ref), (off_h, off_ref),
        ))
    ]
    for copy in small:
        copy.start()
    for base, source in ((0, sec_h), (k_size, mst_h)):
        for at in range(0, k_size, 2 * SUB):
            pltpu.make_async_copy(
                source.at[at : at + 2 * SUB, :], x_ref.at[base + at : base + at + 2 * SUB, :], s_big
            ).start(priority=1)
    for copy in small:
        copy.wait()

    row_id = (
        lax.broadcasted_iota(jnp.int32, (lines, LANES), 0) * LANES
        + lax.broadcasted_iota(jnp.int32, (lines, LANES), 1)
    )
    alive = row_id < live_s[...]
    group = jnp.where(alive, slot_ref[...] // WIDTH, -1)
    before = (
        lax.broadcasted_iota(jnp.int32, (lines, lines), 1)
        < lax.broadcasted_iota(jnp.int32, (lines, lines), 0)
    )
    before = jnp.where(before, 1.0, 0.0).astype(jnp.bfloat16)
    place = jnp.zeros((lines, LANES), jnp.float32)
    for g in range(0, GROUPS, 2):
        mine = [group == g, group == g + 1]
        seen = jnp.concatenate([jnp.where(m, 1.0, 0.0).astype(jnp.bfloat16) for m in mine], axis=1)
        found = jnp.dot(before, seen, preferred_element_type=jnp.float32)
        place = jnp.where(mine[0], found[:, :LANES], jnp.where(mine[1], found[:, LANES:], place))
    code = jnp.where(alive, place.astype(jnp.int32) * CODE + group, -1)
    code_ref[...] = code
    worst = jnp.max(code)

    w = jnp.concatenate([ns_ref[...], -nm_ref[...]], axis=0).astype(jnp.float32)
    qrow = qw_ref[...]
    wt = w.T
    qmat = jnp.broadcast_to(qrow, (LANES, p_size)).T
    v = jnp.sum(wt * qmat, axis=0, keepdims=True)
    qsum = jnp.sum(qmat, axis=0, keepdims=True)
    depth = wt_ref.shape[1]
    pick = lax.broadcasted_iota(jnp.int32, (EXTRA, depth), 0)
    column = lax.broadcasted_iota(jnp.int32, (p_size, depth - 2 * k_size), 1)
    wt_ref[0:p_size, 0 : 2 * k_size] = wt.astype(jnp.bfloat16)
    wt_ref[0:p_size, 2 * k_size :] = jnp.where(column < 3, 1.0, 0.0).astype(jnp.bfloat16)
    lane_row = lax.broadcasted_iota(jnp.int32, (1, LANES), 1)
    tail = jnp.where(lane_row < 3, qsum, 0.0)[:, : depth - 2 * k_size]
    a, b, c = (part.astype(jnp.float32) for part in split3(jnp.concatenate([v, tail], axis=1)))
    stacked = jnp.where(pick == 0, a, jnp.where(pick == 1, b, jnp.where(pick == 2, c, 0.0)))
    wt_ref[p_size:, :] = stacked.astype(jnp.bfloat16)
    scaled = ns_ref[...].astype(jnp.float32) * qrow
    top = scaled.astype(jnp.bfloat16)
    low = (scaled - top.astype(jnp.float32)).astype(jnp.bfloat16)
    nq_ref[...] = jnp.concatenate([top, low], axis=0)

    key_ref[...] = ((rank_ref[...] - 2) << 30) + (FACE_MASK - face_ref[...])
    jl = jnp.where(alive, jac_ref[...], 0.0)
    jl_ref[...] = jl
    area_ref[...] = jnp.sum(jl, axis=0, keepdims=True) * jnp.sum(qrow, axis=1, keepdims=True)
    over_pen[...] = jnp.full(over_pen.shape, LOWEST_FILL, jnp.float32)
    over_key[...] = jnp.full(over_key.shape, KEY_LOW, jnp.int32)
    over_gap[...] = jnp.zeros(over_gap.shape, jnp.float32)

    pltpu.make_async_copy(x_ref, x_ref, s_big).wait()

    @pl.when(worst >= DEPTH * CODE)
    def _():
        weights = wt_ref[...]

        def fill(tile, carry):
            reduce_field(project(weights, x_ref, off_ref, tile), p_size, tile, pen_ref, gap_ref)
            return carry

        lax.fori_loop(0, rows // TILE, fill, 0)
        gap_ref[...] = gap_ref[...] * jl_ref[...]
        face_ref[...] = code_ref[...]

        def one(worst):
            code = face_ref[...]
            g = worst & (CODE - 1)
            low = jnp.maximum((worst // CODE) & -SUB, DEPTH)
            pull_groups(g, 1, low, SUB, face_ref, (slot_ref, pen_ref, key_ref, gap_ref), packs)
            found = match_group(g, 0, SUB, packs, 2)
            odd = jnp.full((SUB, LANES), g & 1, jnp.int32)
            for side in range(PER_ROW):
                keep_group(accs, side, [
                    [jnp.where(odd == side, x, fill) for x in part]
                    for part, fill in zip(found, (LOWEST_FILL, KEY_LOW, 0.0))
                ])
            pen, key, gap = across(accs)
            at = pl.ds(g // PER_ROW, 1)
            over_pen[at, :] = jnp.maximum(over_pen[at, :], pen)
            over_key[at, :] = jnp.maximum(over_key[at, :], key)
            over_gap[at, :] = over_gap[at, :] + gap
            done = ((code & (CODE - 1)) == g) & (code >= low * CODE)
            code = jnp.where(done, -1, code)
            face_ref[...] = code
            return jnp.max(code)

        lax.while_loop(lambda worst: worst >= DEPTH * CODE, one, worst)


def main_kernel(
    n_dom, n_rep,
    x_ref, wt_ref, nq_ref, off_ref, jl_ref, slot_ref, code_ref, key_ref, over_pen, over_key, over_gap, area_ref,
    force_ref, out_pen, out_face, out_gap, out_mean,
    load_ref, pen_ref, gap_ref, packs, even_accs, odd_accs, raw_pen, raw_key, raw_gap,
    sp_sf, sp_si, ow_sf, ow_si, t1_s, t2_s, sp_f, sp_i, ow_f, ow_i, t1_d, t2_d,
    s_spf, r_spf, s_spi, r_spi, s_owf, r_owf, s_owi, r_owi, s_t1, r_t1, s_t2, r_t2, inside,
):
    dom = lax.axis_index("dom")
    rep = lax.axis_index("rep")
    k_size = force_ref.shape[0]
    rows = force_ref.shape[1]
    p_size = load_ref.shape[0]
    per_tile = TILE // LANES
    tiles = rows // TILE
    count = n_dom * n_rep
    me = dom * n_rep + rep

    def dev(d, r):
        return {"dom": lax.rem(d + n_dom, n_dom), "rep": lax.rem(r + n_rep, n_rep)}

    def flat_dev(flat):
        return dev(lax.div(flat, n_rep), lax.rem(flat, n_rep))

    barrier = pltpu.get_barrier_semaphore()

    def signal(sem, first, last):
        def one(flat, carry):
            pl.semaphore_signal(sem, inc=1, device_id=flat_dev(flat), device_id_type=MESH)
            return carry

        lax.fori_loop(first, last, one, 0)

    signal(barrier, me + 1, count)
    signal(barrier, dom * n_rep, me)
    signal(barrier, jnp.maximum(dom - 1, 0) * n_rep, dom * n_rep)

    wt = wt_ref[...]

    def wide_row(ref, tile):
        return jnp.concatenate([row(ref, tile * per_tile + i) for i in range(per_tile)], axis=1)

    last_dom = dom == n_dom - 1

    def enter():
        after = n_rep * jnp.where(last_dom, 0, 1)
        pl.semaphore_wait(barrier, me + (n_rep - 1 - rep) + after)
        signal(inside, 0, me)

    def batch(step, carry):
        @pl.when(last_dom & (step == 1))
        def _():
            enter()

        for i in range(UNROLL):
            tile = step * UNROLL + i
            cols = pl.ds(tile * TILE, TILE)
            field = project(wt, x_ref, off_ref, tile)
            for at in range(0, p_size, 2 * SUB):
                load_ref[at : at + 2 * SUB, cols] = jnp.minimum(field[at : at + 2 * SUB].astype(jnp.bfloat16), 0)
            reduce_field(field, p_size, tile, pen_ref, gap_ref)
        return carry

    lax.fori_loop(0, tiles // UNROLL, batch, 0)
    row_gap = gap_ref[...] * jl_ref[...]
    gap_ref[...] = row_gap
    total_gap = jnp.sum(jnp.sum(row_gap, axis=0, keepdims=True), axis=1, keepdims=True)
    total_area = jnp.sum(area_ref[...], axis=1, keepdims=True)
    lane = lax.broadcasted_iota(jnp.int32, (1, LANES), 1)
    t1_s[...] = jnp.where(lane == 0, total_gap, jnp.where(lane == 1, total_area, 0.0))

    @pl.when(jnp.logical_not(last_dom))
    def _():
        enter()

    mate = rep + 1 - 2 * lax.rem(rep, 2)
    first_copy = pltpu.make_async_remote_copy(
        src_ref=t1_s, dst_ref=t1_d, send_sem=s_t1, recv_sem=r_t1,
        device_id=dev(dom, mate), device_id_type=MESH,
    )
    first_copy.start()

    def pull_batch(first):
        pull_groups(first, BATCH, 0, DEPTH, code_ref, (slot_ref, pen_ref, key_ref, gap_ref), packs)

    def match_pair(first, i, accs, last_accs, over, at):
        g = first + i * PER_ROW
        keep_group(accs, 0, match_group(g, i * PER_ROW * DEPTH, DEPTH, packs, LOOP_UNROLL))
        if last_accs is not None:
            close_pair(last_accs, over, at)
        keep_group(accs, 1, match_group(g + 1, (i * PER_ROW + 1) * DEPTH, DEPTH, packs, DEPTH))

    def close_pair(accs, over, at):
        pen, key, gap = across(accs)
        over, at = pl.ds(over, 1), pl.ds(at, 1)
        raw_pen[at, :] = jnp.maximum(pen, over_pen[over, :])
        raw_key[at, :] = jnp.maximum(key, over_key[over, :])
        raw_gap[at, :] = gap + over_gap[over, :]

    def decode(top, best):
        none = top < LOWEST_FILL * 0.5
        rank = jnp.where(none, -1, (best >> 30) + 2)
        face = jnp.where(none, FACE_LIMIT, FACE_MASK - (best & FACE_MASK))
        return rank, face

    pull_batch(OWN_GROUPS)
    match_pair(OWN_GROUPS, 0, even_accs, None, 0, 0)
    match_pair(OWN_GROUPS, 1, odd_accs, even_accs, OWN_ROWS, 0)
    close_pair(odd_accs, OWN_ROWS + 1, 1)
    part = slice(0, SPILL_ROWS)
    rank, face = decode(raw_pen[part, :], raw_key[part, :])
    sp_sf[0:SPILL_ROWS, :] = raw_pen[part, :]
    sp_sf[SPILL_ROWS:, :] = raw_gap[part, :]
    sp_si[0:SPILL_ROWS, :] = rank
    sp_si[SPILL_ROWS:, :] = face

    def spill_copy(j):
        where = dev(dom + 1, rep + j)
        return (
            pltpu.make_async_remote_copy(
                src_ref=sp_sf, dst_ref=sp_f.at[rep], send_sem=s_spf, recv_sem=r_spf,
                device_id=where, device_id_type=MESH,
            ),
            pltpu.make_async_remote_copy(
                src_ref=sp_si, dst_ref=sp_i.at[rep], send_sem=s_spi, recv_sem=r_spi,
                device_id=where, device_id_type=MESH,
            ),
        )

    for j in range(n_rep):
        for copy in spill_copy(j):
            copy.start()

    first_copy.wait_recv()
    pairs = count // 2
    pair = lax.div(me, 2)
    both = t1_s[...] + t1_d[...]
    t2_s[...] = both
    t2_d[pl.ds(pair, 1), :] = both

    def send_pairs(first, last):
        def one(other, carry):
            pltpu.make_async_remote_copy(
                src_ref=t2_s, dst_ref=t2_d.at[pl.ds(pair, 1), :], send_sem=s_t2, recv_sem=r_t2,
                device_id=flat_dev(other * 2 + lax.rem(rep, 2)), device_id_type=MESH,
            ).start()
            return carry

        lax.fori_loop(first, last, one, 0)

    send_pairs(0, pair)

    def send_up():
        @pl.when(me < count - 1)
        def _():
            pl.semaphore_wait(inside, count - 1 - me)

        send_pairs(pair + 1, pairs)

    quarter = lax.div(me * 4, count)
    turn = OWN_BATCHES - quarter - jnp.where(quarter >= 2, 1, 0)

    def own_scan(i, carry):
        @pl.when(i == turn)
        def _():
            send_up()

        first = i * BATCH
        last = lax.rem(2 * i + OWN_ROWS - 1, OWN_ROWS)
        pull_batch(first)
        match_pair(first, 0, even_accs, odd_accs, last, last)
        match_pair(first, 1, odd_accs, even_accs, 2 * i, 2 * i)
        return carry

    lax.fori_loop(0, OWN_BATCHES, own_scan, 0)
    close_pair(odd_accs, OWN_ROWS - 1, OWN_ROWS - 1)
    rank, face = decode(raw_pen[...], raw_key[...])
    ow_sf[0] = raw_pen[...]
    ow_sf[1] = raw_gap[...]
    ow_si[0] = rank
    ow_si[1] = face

    def own_copy(j):
        where = dev(dom, rep + j)
        return (
            pltpu.make_async_remote_copy(
                src_ref=ow_sf, dst_ref=ow_f.at[rep], send_sem=s_owf, recv_sem=r_owf,
                device_id=where, device_id_type=MESH,
            ),
            pltpu.make_async_remote_copy(
                src_ref=ow_si, dst_ref=ow_i.at[rep], send_sem=s_owi, recv_sem=r_owi,
                device_id=where, device_id_type=MESH,
            ),
        )

    for j in range(1, n_rep):
        for copy in own_copy(j):
            copy.start()
    ow_f[rep] = ow_sf[...]
    ow_i[rep] = ow_si[...]

    @pl.when(turn >= OWN_BATCHES)
    def _():
        send_up()

    nq = nq_ref[...]

    def push(step, carry):
        for i in range(FORCE_UNROLL):
            tile = step * FORCE_UNROLL + i
            cols = pl.ds(tile * TILE, TILE)
            force = jnp.dot(nq, load_ref[:, cols], preferred_element_type=jnp.float32)
            scale = wide_row(jl_ref, tile)[0:1] * -PENALTY
            force_ref[:, cols] = ((force[:k_size] + force[k_size:]) * scale).astype(jnp.bfloat16)
        return carry

    lax.fori_loop(0, tiles // FORCE_UNROLL, push, 0)

    def encode(rank, face):
        return jnp.where(rank < 0, KEY_LOW, ((rank - 2) << 30) + (FACE_MASK - face))

    def settle(ref, sem):
        pltpu.make_async_copy(ref, ref, sem).wait()

    settle(ow_f.at[pl.ds(0, n_rep - 1)], r_owf)
    settle(ow_i.at[pl.ds(0, n_rep - 1)], r_owi)
    pen_o, gap_o = ow_f[0, 0], ow_f[0, 1]
    key_o = encode(ow_i[0, 0], ow_i[0, 1])
    for r in range(1, n_rep):
        pen_o = jnp.maximum(pen_o, ow_f[r, 0])
        gap_o = gap_o + ow_f[r, 1]
        key_o = jnp.maximum(key_o, encode(ow_i[r, 0], ow_i[r, 1]))

    settle(sp_f, s_spf)
    settle(sp_i, s_spi)
    settle(ow_f.at[pl.ds(0, n_rep - 1)], s_owf)
    settle(ow_i.at[pl.ds(0, n_rep - 1)], s_owi)
    first_copy.wait_send()
    settle(t2_d.at[pl.ds(0, pairs - 1), :], s_t2)

    settle(t2_d.at[pl.ds(0, pairs - 1), :], r_t2)
    whole = jnp.sum(t2_d[...], axis=0, keepdims=True)
    out_mean[...] = whole[:, 0:1] / whole[:, 1:2]

    settle(sp_f, r_spf)
    settle(sp_i, r_spi)
    g = SPILL_ROWS
    pen_s, gap_s = sp_f[0, 0:g], sp_f[0, g:]
    key_s = encode(sp_i[0, 0:g], sp_i[0, g:])
    for r in range(1, n_rep):
        pen_s = jnp.maximum(pen_s, sp_f[r, 0:g])
        gap_s = gap_s + sp_f[r, g:]
        key_s = jnp.maximum(key_s, encode(sp_i[r, 0:g], sp_i[r, g:]))

    def finish(at, pen, key, gap):
        none = pen < LOWEST_FILL * 0.5
        out_pen[at, :] = jnp.where(none, 0.0, pen)
        out_face[at, :] = jnp.where(none, -1, FACE_MASK - (key & FACE_MASK))
        out_gap[at, :] = jnp.where(none, 0.0, gap)

    finish(
        slice(0, g), jnp.maximum(pen_o[:g], pen_s), jnp.maximum(key_o[:g], key_s), gap_o[:g] + gap_s
    )
    finish(slice(g, OWN_ROWS), pen_o[g:], key_o[g:], gap_o[g:])


def finish_kernel(force_ref, pen_ref, face_ref, gap_ref, mean_ref, force_h, pen_h, face_h, gap_h, mean_h, sems, s_force):
    copies = [
        pltpu.make_async_copy(held, out, sems.at[i])
        for i, (held, out) in enumerate((
            (pen_ref, pen_h), (face_ref, face_h), (gap_ref, gap_h), (mean_ref, mean_h)
        ))
    ]
    for at in range(0, force_ref.shape[0], SUB):
        part = (slice(at, at + SUB), slice(None))
        pltpu.make_async_copy(force_ref.at[part], force_h.at[part], s_force).start()
    for copy in copies:
        copy.start()
    for copy in copies:
        copy.wait()
    pltpu.make_async_copy(force_ref, force_h, s_force).wait()


def solution(mesh):
    n_dom, n_rep = mesh.shape["dom"], mesh.shape["rep"]
    vmem = pl.BlockSpec(memory_space=pltpu.VMEM)
    anywhere = pl.BlockSpec(memory_space=pl.ANY)
    dma = pltpu.SemaphoreType.DMA

    def kept(x):
        return pltpu.with_memory_space_constraint(x, pltpu.VMEM)

    def streamed(x):
        return pltpu.with_memory_space_constraint(x, pltpu.HBM)

    def shards(ns, nm, sec, mst, off, qw, jac, slot, face, rank, live):
        k_size, p_size = ns.shape
        rows = sec.shape[1]
        lines = rows // LANES
        depth = 2 * k_size + EXTRA
        f32, i32, bf16 = jnp.float32, jnp.int32, jnp.bfloat16

        off, jac, slot, face, rank = (x.reshape(lines, LANES) for x in (off, jac, slot, face, rank))

        def packs(deep):
            return [pltpu.VMEM((deep + SUB, LANES), t) for t in (i32, f32, i32, f32)]

        def lanes():
            return [pltpu.VMEM((LANES, LANES), t) for t in (f32, i32, f32)]

        held = pl.pallas_call(
            prep_kernel,
            out_shape=(
                pltpu.VMEM((2 * k_size, rows), bf16),
                pltpu.VMEM((p_size + EXTRA, depth), bf16),
                pltpu.VMEM((2 * k_size, p_size), bf16),
                pltpu.VMEM((lines, LANES), f32),
                pltpu.VMEM((lines, LANES), f32),
                pltpu.VMEM((lines, LANES), i32),
                pltpu.VMEM((lines, LANES), i32),
                pltpu.VMEM((lines, LANES), i32),
                pltpu.VMEM((ALL_ROWS, LANES), f32),
                pltpu.VMEM((ALL_ROWS, LANES), i32),
                pltpu.VMEM((ALL_ROWS, LANES), f32),
                pltpu.VMEM((1, LANES), f32),
            ),
            in_specs=[anywhere] * 11,
            out_specs=(vmem,) * 12,
            scratch_shapes=[
                pltpu.VMEM((1, 1), i32),
                pltpu.VMEM((k_size, p_size), bf16),
                pltpu.VMEM((k_size, p_size), bf16),
                pltpu.VMEM((1, p_size), f32),
                pltpu.VMEM((lines, LANES), f32),
                pltpu.VMEM((lines, LANES), i32),
                pltpu.VMEM((lines, LANES), i32),
                pltpu.VMEM((lines, LANES), f32),
                pltpu.VMEM((lines, LANES), f32),
                packs(SUB),
                lanes(),
                dma((9,)),
                dma,
            ],
            compiler_params=pltpu.CompilerParams(vmem_limit_bytes=VMEM_LIMIT),
        )(
            live.reshape(1, 1),
            *(streamed(x) for x in (ns, nm, qw.reshape(1, p_size), sec, mst, off, jac, slot, face, rank)),
        )

        spill = (2 * SPILL_ROWS, LANES)
        own = (2, OWN_ROWS, LANES)
        pairs = n_dom * n_rep // 2
        results = pl.pallas_call(
            functools.partial(main_kernel, n_dom, n_rep),
            out_shape=(
                pltpu.VMEM((k_size, rows), bf16),
                pltpu.VMEM((OWN_ROWS, LANES), f32),
                pltpu.VMEM((OWN_ROWS, LANES), i32),
                pltpu.VMEM((OWN_ROWS, LANES), f32),
                pltpu.VMEM((1, 1), f32),
            ),
            in_specs=[vmem] * 12,
            out_specs=(vmem,) * 5,
            scratch_shapes=[
                pltpu.VMEM((p_size, rows), bf16),
                pltpu.VMEM((lines, LANES), f32),
                pltpu.VMEM((lines, LANES), f32),
                packs(BATCH * DEPTH),
                lanes(),
                lanes(),
                pltpu.VMEM((OWN_ROWS, LANES), f32),
                pltpu.VMEM((OWN_ROWS, LANES), i32),
                pltpu.VMEM((OWN_ROWS, LANES), f32),
                pltpu.VMEM(spill, f32),
                pltpu.VMEM(spill, i32),
                pltpu.VMEM(own, f32),
                pltpu.VMEM(own, i32),
                pltpu.VMEM((1, LANES), f32),
                pltpu.VMEM((1, LANES), f32),
                pltpu.VMEM((n_rep,) + spill, f32),
                pltpu.VMEM((n_rep,) + spill, i32),
                pltpu.VMEM((n_rep,) + own, f32),
                pltpu.VMEM((n_rep,) + own, i32),
                pltpu.VMEM((1, LANES), f32),
                pltpu.VMEM((pairs, LANES), f32),
            ] + [dma] * 12 + [pltpu.SemaphoreType.REGULAR],
            compiler_params=pltpu.CompilerParams(
                collective_id=0, has_side_effects=True, vmem_limit_bytes=VMEM_LIMIT
            ),
        )(*(kept(x) for x in held))

        force, seg_pen, seg_face, seg_gap, mean = pl.pallas_call(
            finish_kernel,
            out_shape=tuple(jax.ShapeDtypeStruct(x.shape, x.dtype) for x in results),
            in_specs=[vmem] * 5,
            out_specs=(anywhere,) * 5,
            scratch_shapes=[dma((4,)), dma],
            compiler_params=pltpu.CompilerParams(vmem_limit_bytes=VMEM_LIMIT),
        )(*(kept(x) for x in results))
        seg_pen, seg_face, seg_gap = (x.reshape(SEG_DEV) for x in (seg_pen, seg_face, seg_gap))
        return force, seg_pen, seg_face, seg_gap, mean.reshape(())

    rows_spec, wide_spec = P(("dom", "rep")), P(None, ("dom", "rep"))
    return jax.shard_map(
        shards,
        mesh=mesh,
        in_specs=(P(), P(), wide_spec, wide_spec, rows_spec, P()) + (rows_spec,) * 5,
        out_specs=(wide_spec, P("dom"), P("dom"), P("dom"), P()),
        check_vma=False,
    )
```

```python
import functools

import jax
import jax.numpy as jnp
from jax import lax
from jax.experimental import pallas as pl
from jax.experimental.pallas import tpu as pltpu
from jax.sharding import PartitionSpec as P

SEG_DEV = 1024
SPILL = 256
LANES = 128
SUB = 8
WIDTH = 64
PER_ROW = LANES // WIDTH
GROUPS = (SEG_DEV + SPILL) // WIDTH
OWN_GROUPS = SEG_DEV // WIDTH
SPILL_GROUPS = SPILL // WIDTH
OWN_ROWS = SEG_DEV // LANES
SPILL_ROWS = SPILL // LANES
ALL_ROWS = 16
CODE = 32

PENALTY = 400.0
LOWEST_FILL = -1e30
FACE_LIMIT = 1073741824
FACE_MASK = FACE_LIMIT - 1
KEY_LOW = -2147483648
MESH = pl.DeviceIdType.MESH
TILE = 256
DEPTH = 12
BATCH = 4
OWN_BATCHES = OWN_GROUPS // BATCH
PHASES = (4, 28)
CHAINS = 4
FORCE_UNROLL = 8
LOOP_UNROLL = 4
EXTRA = 16
VMEM_LIMIT = 32 << 20


def split3(x):
    a = x.astype(jnp.bfloat16)
    rest = x - a.astype(jnp.float32)
    b = rest.astype(jnp.bfloat16)
    c = (rest - b.astype(jnp.float32)).astype(jnp.bfloat16)
    return a, b, c


def row(ref, at):
    return ref[pl.ds(at, SUB, stride=0), :]


def pull_groups(first, count, depth0, depth, code_ref, sources, packs):
    all_lines = code_ref.shape[0]
    sub = lax.broadcasted_iota(jnp.int32, (SUB, LANES), 0)
    blocks = -(-count * depth // SUB)
    wants = []
    for b in range(blocks):
        line = sub + SUB * b
        want = jnp.full((SUB, LANES), -2, jnp.int32)
        for q in range(count):
            inside = (line >= q * depth) & (line < (q + 1) * depth)
            want = jnp.where(inside, (line + (depth0 - q * depth)) * CODE + (first + q), want)
        wants.append(want)
    fills = (-1, LOWEST_FILL, -1, 0.0)

    def pull(i, carry):
        parts = [list(part) for part in carry]
        code = row(code_ref, i)
        values = [row(ref, i) for ref in sources]
        for b in range(blocks):
            hit = code == wants[b]
            for part, value in zip(parts, values):
                part[b] = jnp.where(hit, value, part[b])
        return tuple(tuple(part) for part in parts)

    start = tuple(
        (jnp.full((SUB, LANES), fill, ref.dtype),) * blocks for fill, ref in zip(fills, sources)
    )
    pulled = lax.fori_loop(0, all_lines, pull, start, unroll=8)
    for ref, parts in zip(packs, pulled):
        for b in range(blocks):
            ref[SUB * b : SUB * (b + 1), :] = parts[b]


def match_group(g, at, depth, packs, unroll):
    sub = lax.broadcasted_iota(jnp.int32, (SUB, LANES), 0)
    tiles = WIDTH // SUB
    marks = [sub + (g * WIDTH + SUB * q) for q in range(tiles)]
    start = (
        (jnp.full((SUB, LANES), LOWEST_FILL, jnp.float32),) * tiles,
        (jnp.full((SUB, LANES), KEY_LOW, jnp.int32),) * tiles,
        (jnp.zeros((SUB, LANES), jnp.float32),) * tiles,
    )

    def one(j, carry):
        pens, keys, gaps = (list(part) for part in carry)
        slot, pen, key, gap = (row(ref, at + j) for ref in packs)
        for q in range(tiles):
            hit = slot == marks[q]
            pens[q] = jnp.maximum(pens[q], jnp.where(hit, pen, LOWEST_FILL))
            keys[q] = jnp.maximum(keys[q], jnp.where(hit, key, KEY_LOW))
            gaps[q] = gaps[q] + jnp.where(hit, gap, 0.0)
        return tuple(pens), tuple(keys), tuple(gaps)

    if unroll == depth:
        for j in range(depth):
            start = one(j, start)
        return start
    return lax.fori_loop(0, depth, one, start, unroll=unroll)


def keep_group(accs, side, parts):
    for ref, part in zip(accs, parts):
        for q in range(WIDTH // SUB):
            at = side * WIDTH + q * SUB
            ref[at : at + SUB, :] = part[q]


def across(accs):
    pens, keys, gaps = (ref[...].T for ref in accs)
    return (
        jnp.max(pens, axis=0, keepdims=True),
        jnp.max(keys, axis=0, keepdims=True),
        jnp.sum(gaps, axis=0, keepdims=True),
    )


def project(wt, x_ref, off_ref, tile):
    cols = pl.ds(tile * TILE, TILE)
    per_tile = TILE // LANES
    offset = jnp.concatenate([row(off_ref, tile * per_tile + i) for i in range(per_tile)], axis=1)
    sub = lax.broadcasted_iota(jnp.int32, (SUB, TILE), 0)
    a, b, c = (part.astype(jnp.float32) for part in split3(offset))
    extra = jnp.where(sub == 0, a, jnp.where(sub == 1, b, jnp.where(sub == 2, c, 0.0)))
    extra = jnp.concatenate([extra, jnp.zeros((EXTRA - SUB, TILE), jnp.float32)], axis=0)
    x = jnp.concatenate([x_ref[:, cols], extra.astype(jnp.bfloat16)], axis=0)
    return jnp.dot(wt, x, preferred_element_type=jnp.float32)


def store_row(ref, tile, value):
    per_tile = TILE // LANES
    for i in range(per_tile):
        ref[pl.ds(tile * per_tile + i, 1), :] = value[:, i * LANES : (i + 1) * LANES]


def reduce_field(field, p_size, tile, pen_ref, gap_ref):
    low = [field[SUB * j : SUB * (j + 1)] for j in range(CHAINS)]
    for j in range(CHAINS, p_size // SUB):
        low[j % CHAINS] = jnp.minimum(low[j % CHAINS], field[SUB * j : SUB * (j + 1)])
    store_row(pen_ref, tile, -jnp.min(functools.reduce(jnp.minimum, low), axis=0, keepdims=True))
    store_row(gap_ref, tile, jnp.sum(field[p_size : p_size + SUB], axis=0, keepdims=True))


def prep_kernel(
    live_h, ns_h, nm_h, qw_h, sec_h, mst_h, off_h, jac_h, slot_h, face_h, rank_h,
    load_ref, nq_ref, pen_ref, gap_ref, jl_ref, slot_ref, code_ref, key_ref, over_pen, over_key, over_gap, pair_ref,
    x_ref, wt_ref, off_ref, live_s, ns_ref, nm_ref, qw_ref, jac_ref, face_ref, rank_ref, packs, accs, s_small, s_big,
):
    lines = slot_ref.shape[0]
    k_size, p_size = ns_ref.shape
    rows = x_ref.shape[1]

    small = [
        pltpu.make_async_copy(source, held, s_small.at[i])
        for i, (source, held) in enumerate((
            (slot_h, slot_ref), (live_h, live_s), (ns_h, ns_ref), (nm_h, nm_ref), (qw_h, qw_ref),
            (face_h, face_ref), (rank_h, rank_ref), (jac_h, jac_ref), (off_h, off_ref),
        ))
    ]
    for copy in small:
        copy.start()
    starts = [sum(PHASES[:i]) * TILE for i in range(len(PHASES))]
    for i, tiles in enumerate(PHASES):
        for half in range(2):
            width = tiles * TILE // 2
            cols = pl.ds(starts[i] + half * width, width)
            for base, source in ((0, sec_h), (k_size, mst_h)):
                pltpu.make_async_copy(
                    source.at[:, cols], x_ref.at[base : base + k_size, cols], s_big.at[i]
                ).start(priority=1)
    for copy in small:
        copy.wait()

    w = jnp.concatenate([ns_ref[...], -nm_ref[...]], axis=0).astype(jnp.float32)
    qrow = qw_ref[...]
    wt = w.T
    qmat = jnp.broadcast_to(qrow, (LANES, p_size)).T
    v = jnp.sum(wt * qmat, axis=0, keepdims=True)
    qsum = jnp.sum(qmat, axis=0, keepdims=True)
    depth = wt_ref.shape[1]
    pick = lax.broadcasted_iota(jnp.int32, (EXTRA, depth), 0)
    column = lax.broadcasted_iota(jnp.int32, (p_size, depth - 2 * k_size), 1)
    wt_ref[0:p_size, 0 : 2 * k_size] = wt.astype(jnp.bfloat16)
    wt_ref[0:p_size, 2 * k_size :] = jnp.where(column < 3, 1.0, 0.0).astype(jnp.bfloat16)
    lane_row = lax.broadcasted_iota(jnp.int32, (1, LANES), 1)
    tail = jnp.where(lane_row < 3, qsum, 0.0)[:, : depth - 2 * k_size]
    a, b, c = (part.astype(jnp.float32) for part in split3(jnp.concatenate([v, tail], axis=1)))
    stacked = jnp.where(pick == 0, a, jnp.where(pick == 1, b, jnp.where(pick == 2, c, 0.0)))
    wt_ref[p_size:, :] = stacked.astype(jnp.bfloat16)
    scaled = ns_ref[...].astype(jnp.float32) * qrow
    top = scaled.astype(jnp.bfloat16)
    low = (scaled - top.astype(jnp.float32)).astype(jnp.bfloat16)
    nq_ref[...] = jnp.concatenate([top, low], axis=0)

    weights = wt_ref[...]

    def dense(phase):
        done = x_ref.at[:, pl.ds(starts[phase], PHASES[phase] * TILE)]
        pltpu.make_async_copy(done, done, s_big.at[phase]).wait()
        for i in range(PHASES[phase]):
            tile = starts[phase] // TILE + i
            cols = pl.ds(tile * TILE, TILE)
            field = project(weights, x_ref, off_ref, tile)
            for at in range(0, p_size, 2 * SUB):
                load_ref[at : at + 2 * SUB, cols] = jnp.minimum(field[at : at + 2 * SUB].astype(jnp.bfloat16), 0)
            reduce_field(field, p_size, tile, pen_ref, gap_ref)

    dense(0)
    row_id = (
        lax.broadcasted_iota(jnp.int32, (lines, LANES), 0) * LANES
        + lax.broadcasted_iota(jnp.int32, (lines, LANES), 1)
    )
    alive = row_id < live_s[...]
    group = jnp.where(alive, slot_ref[...] // WIDTH, -1)
    before = (
        lax.broadcasted_iota(jnp.int32, (lines, lines), 1)
        < lax.broadcasted_iota(jnp.int32, (lines, lines), 0)
    )
    before = jnp.where(before, 1.0, 0.0).astype(jnp.bfloat16)
    place = jnp.zeros((lines, LANES), jnp.float32)
    for g in range(0, GROUPS, 2):
        mine = [group == g, group == g + 1]
        seen = jnp.concatenate([jnp.where(m, 1.0, 0.0).astype(jnp.bfloat16) for m in mine], axis=1)
        found = jnp.dot(before, seen, preferred_element_type=jnp.float32)
        place = jnp.where(mine[0], found[:, :LANES], jnp.where(mine[1], found[:, LANES:], place))
    code = jnp.where(alive, place.astype(jnp.int32) * CODE + group, -1)
    code_ref[...] = code
    worst = jnp.max(code)

    key_ref[...] = ((rank_ref[...] - 2) << 30) + (FACE_MASK - face_ref[...])
    jl = jnp.where(alive, jac_ref[...], 0.0)
    jl_ref[...] = jl
    over_pen[...] = jnp.full(over_pen.shape, LOWEST_FILL, jnp.float32)
    over_key[...] = jnp.full(over_key.shape, KEY_LOW, jnp.int32)
    over_gap[...] = jnp.zeros(over_gap.shape, jnp.float32)

    for phase in range(1, len(PHASES)):
        dense(phase)
    row_gap = gap_ref[...] * jl
    gap_ref[...] = row_gap
    total_gap = jnp.sum(jnp.sum(row_gap, axis=0, keepdims=True), axis=1, keepdims=True)
    total_area = jnp.sum(jnp.sum(jl, axis=0, keepdims=True), axis=1, keepdims=True)
    total_area = total_area * jnp.sum(qrow, axis=1, keepdims=True)
    pair_ref[...] = jnp.where(lane_row == 0, total_gap, jnp.where(lane_row == 1, total_area, 0.0))

    @pl.when(worst >= DEPTH * CODE)
    def _():
        face_ref[...] = code_ref[...]

        def one(worst):
            code = face_ref[...]
            g = worst & (CODE - 1)
            low = jnp.maximum((worst // CODE) & -SUB, DEPTH)
            pull_groups(g, 1, low, SUB, face_ref, (slot_ref, pen_ref, key_ref, gap_ref), packs)
            found = match_group(g, 0, SUB, packs, 2)
            odd = jnp.full((SUB, LANES), g & 1, jnp.int32)
            for side in range(PER_ROW):
                keep_group(accs, side, [
                    [jnp.where(odd == side, x, fill) for x in part]
                    for part, fill in zip(found, (LOWEST_FILL, KEY_LOW, 0.0))
                ])
            pen, key, gap = across(accs)
            at = pl.ds(g // PER_ROW, 1)
            over_pen[at, :] = jnp.maximum(over_pen[at, :], pen)
            over_key[at, :] = jnp.maximum(over_key[at, :], key)
            over_gap[at, :] = over_gap[at, :] + gap
            done = ((code & (CODE - 1)) == g) & (code >= low * CODE)
            code = jnp.where(done, -1, code)
            face_ref[...] = code
            return jnp.max(code)

        lax.while_loop(lambda worst: worst >= DEPTH * CODE, one, worst)


def main_kernel(
    n_dom, n_rep,
    load_ref, nq_ref, pen_ref, gap_ref, jl_ref, slot_ref, code_ref, key_ref, over_pen, over_key, over_gap, pair_ref,
    force_ref, out_pen, out_face, out_gap, out_mean,
    packs, even_accs, odd_accs, raw_pen, raw_key, raw_gap,
    sp_sf, sp_si, ow_sf, ow_si, t2_s, sp_f, sp_i, ow_f, ow_i, t1_d, t2_d,
    s_spf, r_spf, s_spi, r_spi, s_owf, r_owf, s_owi, r_owi, s_t1, r_t1, s_t2, r_t2, inside,
):
    dom = lax.axis_index("dom")
    rep = lax.axis_index("rep")
    k_size = force_ref.shape[0]
    rows = force_ref.shape[1]
    per_tile = TILE // LANES
    tiles = rows // TILE
    count = n_dom * n_rep
    me = dom * n_rep + rep

    def dev(d, r):
        return {"dom": lax.rem(d + n_dom, n_dom), "rep": lax.rem(r + n_rep, n_rep)}

    def flat_dev(flat):
        return dev(lax.div(flat, n_rep), lax.rem(flat, n_rep))

    barrier = pltpu.get_barrier_semaphore()

    def signal(sem, first, last):
        def one(flat, carry):
            pl.semaphore_signal(sem, inc=1, device_id=flat_dev(flat), device_id_type=MESH)
            return carry

        lax.fori_loop(first, last, one, 0)

    signal(barrier, me + 1, count)
    signal(barrier, dom * n_rep, me)
    signal(barrier, jnp.maximum(dom - 1, 0) * n_rep, dom * n_rep)

    def wide_row(ref, tile):
        return jnp.concatenate([row(ref, tile * per_tile + i) for i in range(per_tile)], axis=1)

    last_dom = dom == n_dom - 1
    mate = rep + 1 - 2 * lax.rem(rep, 2)
    first_copy = pltpu.make_async_remote_copy(
        src_ref=pair_ref, dst_ref=t1_d, send_sem=s_t1, recv_sem=r_t1,
        device_id=dev(dom, mate), device_id_type=MESH,
    )

    def enter():
        after = n_rep * jnp.where(last_dom, 0, 1)
        pl.semaphore_wait(barrier, me + (n_rep - 1 - rep) + after)
        signal(inside, 0, me)
        first_copy.start()

    def pull_batch(first):
        pull_groups(first, BATCH, 0, DEPTH, code_ref, (slot_ref, pen_ref, key_ref, gap_ref), packs)

    def match_pair(first, i, accs, last_accs, over, at):
        g = first + i * PER_ROW
        keep_group(accs, 0, match_group(g, i * PER_ROW * DEPTH, DEPTH, packs, LOOP_UNROLL))
        if last_accs is not None:
            close_pair(last_accs, over, at)
        keep_group(accs, 1, match_group(g + 1, (i * PER_ROW + 1) * DEPTH, DEPTH, packs, DEPTH))

    def close_pair(accs, over, at):
        pen, key, gap = across(accs)
        over, at = pl.ds(over, 1), pl.ds(at, 1)
        raw_pen[at, :] = jnp.maximum(pen, over_pen[over, :])
        raw_key[at, :] = jnp.maximum(key, over_key[over, :])
        raw_gap[at, :] = gap + over_gap[over, :]

    def decode(top, best):
        none = top < LOWEST_FILL * 0.5
        rank = jnp.where(none, -1, (best >> 30) + 2)
        face = jnp.where(none, FACE_LIMIT, FACE_MASK - (best & FACE_MASK))
        return rank, face

    pull_batch(OWN_GROUPS)

    @pl.when(last_dom)
    def _():
        enter()

    match_pair(OWN_GROUPS, 0, even_accs, None, 0, 0)
    match_pair(OWN_GROUPS, 1, odd_accs, even_accs, OWN_ROWS, 0)
    close_pair(odd_accs, OWN_ROWS + 1, 1)
    part = slice(0, SPILL_ROWS)
    rank, face = decode(raw_pen[part, :], raw_key[part, :])
    sp_sf[0:SPILL_ROWS, :] = raw_pen[part, :]
    sp_sf[SPILL_ROWS:, :] = raw_gap[part, :]
    sp_si[0:SPILL_ROWS, :] = rank
    sp_si[SPILL_ROWS:, :] = face

    @pl.when(jnp.logical_not(last_dom))
    def _():
        enter()

    def spill_copy(j):
        where = dev(dom + 1, rep + j)
        return (
            pltpu.make_async_remote_copy(
                src_ref=sp_sf, dst_ref=sp_f.at[rep], send_sem=s_spf, recv_sem=r_spf,
                device_id=where, device_id_type=MESH,
            ),
            pltpu.make_async_remote_copy(
                src_ref=sp_si, dst_ref=sp_i.at[rep], send_sem=s_spi, recv_sem=r_spi,
                device_id=where, device_id_type=MESH,
            ),
        )

    for j in range(n_rep):
        for copy in spill_copy(j):
            copy.start()

    first_copy.wait_recv()
    pairs = count // 2
    pair = lax.div(me, 2)
    both = pair_ref[...] + t1_d[...]
    t2_s[...] = both
    t2_d[pl.ds(pair, 1), :] = both

    def send_pairs(first, last):
        def one(other, carry):
            pltpu.make_async_remote_copy(
                src_ref=t2_s, dst_ref=t2_d.at[pl.ds(pair, 1), :], send_sem=s_t2, recv_sem=r_t2,
                device_id=flat_dev(other * 2 + lax.rem(rep, 2)), device_id_type=MESH,
            ).start()
            return carry

        lax.fori_loop(first, last, one, 0)

    send_pairs(0, pair)

    def send_up():
        @pl.when(me < count - 1)
        def _():
            pl.semaphore_wait(inside, count - 1 - me)

        send_pairs(pair + 1, pairs)

    quarter = lax.div(me * 4, count)
    turn = OWN_BATCHES - quarter - jnp.where(quarter >= 2, 1, 0)

    def own_scan(i, carry):
        @pl.when(i == turn)
        def _():
            send_up()

        first = i * BATCH
        last = lax.rem(2 * i + OWN_ROWS - 1, OWN_ROWS)
        pull_batch(first)
        match_pair(first, 0, even_accs, odd_accs, last, last)
        match_pair(first, 1, odd_accs, even_accs, 2 * i, 2 * i)
        return carry

    lax.fori_loop(0, OWN_BATCHES, own_scan, 0)
    close_pair(odd_accs, OWN_ROWS - 1, OWN_ROWS - 1)
    rank, face = decode(raw_pen[...], raw_key[...])
    ow_sf[0] = raw_pen[...]
    ow_sf[1] = raw_gap[...]
    ow_si[0] = rank
    ow_si[1] = face

    def own_copy(j):
        where = dev(dom, rep + j)
        return (
            pltpu.make_async_remote_copy(
                src_ref=ow_sf, dst_ref=ow_f.at[rep], send_sem=s_owf, recv_sem=r_owf,
                device_id=where, device_id_type=MESH,
            ),
            pltpu.make_async_remote_copy(
                src_ref=ow_si, dst_ref=ow_i.at[rep], send_sem=s_owi, recv_sem=r_owi,
                device_id=where, device_id_type=MESH,
            ),
        )

    for j in range(1, n_rep):
        for copy in own_copy(j):
            copy.start()
    ow_f[rep] = ow_sf[...]
    ow_i[rep] = ow_si[...]

    @pl.when(turn >= OWN_BATCHES)
    def _():
        send_up()

    nq = nq_ref[...]

    def push(step, carry):
        for i in range(FORCE_UNROLL):
            tile = step * FORCE_UNROLL + i
            cols = pl.ds(tile * TILE, TILE)
            force = jnp.dot(nq, load_ref[:, cols], preferred_element_type=jnp.float32)
            scale = wide_row(jl_ref, tile)[0:1] * -PENALTY
            force_ref[:, cols] = ((force[:k_size] + force[k_size:]) * scale).astype(jnp.bfloat16)
        return carry

    lax.fori_loop(0, tiles // FORCE_UNROLL, push, 0)

    def encode(rank, face):
        return jnp.where(rank < 0, KEY_LOW, ((rank - 2) << 30) + (FACE_MASK - face))

    def settle(ref, sem):
        pltpu.make_async_copy(ref, ref, sem).wait()

    settle(ow_f.at[pl.ds(0, n_rep - 1)], r_owf)
    settle(ow_i.at[pl.ds(0, n_rep - 1)], r_owi)
    pen_o, gap_o = ow_f[0, 0], ow_f[0, 1]
    key_o = encode(ow_i[0, 0], ow_i[0, 1])
    for r in range(1, n_rep):
        pen_o = jnp.maximum(pen_o, ow_f[r, 0])
        gap_o = gap_o + ow_f[r, 1]
        key_o = jnp.maximum(key_o, encode(ow_i[r, 0], ow_i[r, 1]))

    settle(sp_f, s_spf)
    settle(sp_i, s_spi)
    settle(ow_f.at[pl.ds(0, n_rep - 1)], s_owf)
    settle(ow_i.at[pl.ds(0, n_rep - 1)], s_owi)
    first_copy.wait_send()
    settle(t2_d.at[pl.ds(0, pairs - 1), :], s_t2)

    settle(t2_d.at[pl.ds(0, pairs - 1), :], r_t2)
    whole = jnp.sum(t2_d[...], axis=0, keepdims=True)
    out_mean[...] = whole[:, 0:1] / whole[:, 1:2]

    settle(sp_f, r_spf)
    settle(sp_i, r_spi)
    g = SPILL_ROWS
    pen_s, gap_s = sp_f[0, 0:g], sp_f[0, g:]
    key_s = encode(sp_i[0, 0:g], sp_i[0, g:])
    for r in range(1, n_rep):
        pen_s = jnp.maximum(pen_s, sp_f[r, 0:g])
        gap_s = gap_s + sp_f[r, g:]
        key_s = jnp.maximum(key_s, encode(sp_i[r, 0:g], sp_i[r, g:]))

    def finish(at, pen, key, gap):
        none = pen < LOWEST_FILL * 0.5
        out_pen[at, :] = jnp.where(none, 0.0, pen)
        out_face[at, :] = jnp.where(none, -1, FACE_MASK - (key & FACE_MASK))
        out_gap[at, :] = jnp.where(none, 0.0, gap)

    finish(
        slice(0, g), jnp.maximum(pen_o[:g], pen_s), jnp.maximum(key_o[:g], key_s), gap_o[:g] + gap_s
    )
    finish(slice(g, OWN_ROWS), pen_o[g:], key_o[g:], gap_o[g:])


def finish_kernel(force_ref, pen_ref, face_ref, gap_ref, mean_ref, force_h, pen_h, face_h, gap_h, mean_h, sems, s_force):
    copies = [
        pltpu.make_async_copy(held, out, sems.at[i])
        for i, (held, out) in enumerate((
            (pen_ref, pen_h), (face_ref, face_h), (gap_ref, gap_h), (mean_ref, mean_h)
        ))
    ]
    for at in range(0, force_ref.shape[0], SUB):
        part = (slice(at, at + SUB), slice(None))
        pltpu.make_async_copy(force_ref.at[part], force_h.at[part], s_force).start()
    for copy in copies:
        copy.start()
    for copy in copies:
        copy.wait()
    pltpu.make_async_copy(force_ref, force_h, s_force).wait()


def solution(mesh):
    n_dom, n_rep = mesh.shape["dom"], mesh.shape["rep"]
    vmem = pl.BlockSpec(memory_space=pltpu.VMEM)
    anywhere = pl.BlockSpec(memory_space=pl.ANY)
    dma = pltpu.SemaphoreType.DMA

    def kept(x):
        return pltpu.with_memory_space_constraint(x, pltpu.VMEM)

    def streamed(x):
        return pltpu.with_memory_space_constraint(x, pltpu.HBM)

    def shards(ns, nm, sec, mst, off, qw, jac, slot, face, rank, live):
        k_size, p_size = ns.shape
        rows = sec.shape[1]
        lines = rows // LANES
        depth = 2 * k_size + EXTRA
        f32, i32, bf16 = jnp.float32, jnp.int32, jnp.bfloat16

        off, jac, slot, face, rank = (x.reshape(lines, LANES) for x in (off, jac, slot, face, rank))

        def packs(deep):
            return [pltpu.VMEM((deep + SUB, LANES), t) for t in (i32, f32, i32, f32)]

        def lanes():
            return [pltpu.VMEM((LANES, LANES), t) for t in (f32, i32, f32)]

        held = pl.pallas_call(
            prep_kernel,
            out_shape=(
                pltpu.VMEM((p_size, rows), bf16),
                pltpu.VMEM((2 * k_size, p_size), bf16),
                pltpu.VMEM((lines, LANES), f32),
                pltpu.VMEM((lines, LANES), f32),
                pltpu.VMEM((lines, LANES), f32),
                pltpu.VMEM((lines, LANES), i32),
                pltpu.VMEM((lines, LANES), i32),
                pltpu.VMEM((lines, LANES), i32),
                pltpu.VMEM((ALL_ROWS, LANES), f32),
                pltpu.VMEM((ALL_ROWS, LANES), i32),
                pltpu.VMEM((ALL_ROWS, LANES), f32),
                pltpu.VMEM((1, LANES), f32),
            ),
            in_specs=[anywhere] * 11,
            out_specs=(vmem,) * 12,
            scratch_shapes=[
                pltpu.VMEM((2 * k_size, rows), bf16),
                pltpu.VMEM((p_size + EXTRA, depth), bf16),
                pltpu.VMEM((lines, LANES), f32),
                pltpu.VMEM((1, 1), i32),
                pltpu.VMEM((k_size, p_size), bf16),
                pltpu.VMEM((k_size, p_size), bf16),
                pltpu.VMEM((1, p_size), f32),
                pltpu.VMEM((lines, LANES), f32),
                pltpu.VMEM((lines, LANES), i32),
                pltpu.VMEM((lines, LANES), i32),
                packs(SUB),
                lanes(),
                dma((9,)),
                dma((len(PHASES),)),
            ],
            compiler_params=pltpu.CompilerParams(vmem_limit_bytes=VMEM_LIMIT),
        )(
            live.reshape(1, 1),
            *(streamed(x) for x in (ns, nm, qw.reshape(1, p_size), sec, mst, off, jac, slot, face, rank)),
        )

        spill = (2 * SPILL_ROWS, LANES)
        own = (2, OWN_ROWS, LANES)
        pairs = n_dom * n_rep // 2
        results = pl.pallas_call(
            functools.partial(main_kernel, n_dom, n_rep),
            out_shape=(
                pltpu.VMEM((k_size, rows), bf16),
                pltpu.VMEM((OWN_ROWS, LANES), f32),
                pltpu.VMEM((OWN_ROWS, LANES), i32),
                pltpu.VMEM((OWN_ROWS, LANES), f32),
                pltpu.VMEM((1, 1), f32),
            ),
            in_specs=[vmem] * 12,
            out_specs=(vmem,) * 5,
            scratch_shapes=[
                packs(BATCH * DEPTH),
                lanes(),
                lanes(),
                pltpu.VMEM((OWN_ROWS, LANES), f32),
                pltpu.VMEM((OWN_ROWS, LANES), i32),
                pltpu.VMEM((OWN_ROWS, LANES), f32),
                pltpu.VMEM(spill, f32),
                pltpu.VMEM(spill, i32),
                pltpu.VMEM(own, f32),
                pltpu.VMEM(own, i32),
                pltpu.VMEM((1, LANES), f32),
                pltpu.VMEM((n_rep,) + spill, f32),
                pltpu.VMEM((n_rep,) + spill, i32),
                pltpu.VMEM((n_rep,) + own, f32),
                pltpu.VMEM((n_rep,) + own, i32),
                pltpu.VMEM((1, LANES), f32),
                pltpu.VMEM((pairs, LANES), f32),
            ] + [dma] * 12 + [pltpu.SemaphoreType.REGULAR],
            compiler_params=pltpu.CompilerParams(
                collective_id=0, has_side_effects=True, vmem_limit_bytes=VMEM_LIMIT
            ),
        )(*(kept(x) for x in held))

        force, seg_pen, seg_face, seg_gap, mean = pl.pallas_call(
            finish_kernel,
            out_shape=tuple(jax.ShapeDtypeStruct(x.shape, x.dtype) for x in results),
            in_specs=[vmem] * 5,
            out_specs=(anywhere,) * 5,
            scratch_shapes=[dma((4,)), dma],
            compiler_params=pltpu.CompilerParams(vmem_limit_bytes=VMEM_LIMIT),
        )(*(kept(x) for x in results))
        seg_pen, seg_face, seg_gap = (x.reshape(SEG_DEV) for x in (seg_pen, seg_face, seg_gap))
        return force, seg_pen, seg_face, seg_gap, mean.reshape(())

    rows_spec, wide_spec = P(("dom", "rep")), P(None, ("dom", "rep"))
    return jax.shard_map(
        shards,
        mesh=mesh,
        in_specs=(P(), P(), wide_spec, wide_spec, rows_spec, P()) + (rows_spec,) * 5,
        out_specs=(wide_spec, P("dom"), P("dom"), P("dom"), P()),
        check_vma=False,
    )
```

```python
import functools

import jax
import jax.numpy as jnp
from jax import lax
from jax.experimental import pallas as pl
from jax.experimental.pallas import tpu as pltpu
from jax.sharding import PartitionSpec as P

SEG_DEV = 1024
SPILL = 256
LANES = 128
SUB = 8
WIDTH = 64
PER_ROW = LANES // WIDTH
GROUPS = (SEG_DEV + SPILL) // WIDTH
OWN_GROUPS = SEG_DEV // WIDTH
SPILL_GROUPS = SPILL // WIDTH
OWN_ROWS = SEG_DEV // LANES
SPILL_ROWS = SPILL // LANES
ALL_ROWS = 16
CODE = 32

PENALTY = 400.0
LOWEST_FILL = -1e30
FACE_LIMIT = 1073741824
FACE_MASK = FACE_LIMIT - 1
KEY_LOW = -2147483648
LOGICAL = pl.DeviceIdType.LOGICAL
TILE = 256
DEPTH = 12
BATCH = 4
OWN_BATCHES = OWN_GROUPS // BATCH
PHASES = (4, 28)
CHAINS = 4
FORCE_UNROLL = 8
LOOP_UNROLL = 4
EXTRA = 16
VMEM_LIMIT = 32 << 20


def split3(x):
    a = x.astype(jnp.bfloat16)
    rest = x - a.astype(jnp.float32)
    b = rest.astype(jnp.bfloat16)
    c = (rest - b.astype(jnp.float32)).astype(jnp.bfloat16)
    return a, b, c


def row(ref, at):
    return ref[pl.ds(at, SUB, stride=0), :]


def pull_groups(first, count, depth0, depth, code_ref, sources, packs):
    all_lines = code_ref.shape[0]
    sub = lax.broadcasted_iota(jnp.int32, (SUB, LANES), 0)
    blocks = -(-count * depth // SUB)
    wants = []
    for b in range(blocks):
        line = sub + SUB * b
        want = jnp.full((SUB, LANES), -2, jnp.int32)
        for q in range(count):
            inside = (line >= q * depth) & (line < (q + 1) * depth)
            want = jnp.where(inside, (line + (depth0 - q * depth)) * CODE + (first + q), want)
        wants.append(want)
    fills = (-1, LOWEST_FILL, -1, 0.0)

    def pull(i, carry):
        parts = [list(part) for part in carry]
        code = row(code_ref, i)
        values = [row(ref, i) for ref in sources]
        for b in range(blocks):
            hit = code == wants[b]
            for part, value in zip(parts, values):
                part[b] = jnp.where(hit, value, part[b])
        return tuple(tuple(part) for part in parts)

    start = tuple(
        (jnp.full((SUB, LANES), fill, ref.dtype),) * blocks for fill, ref in zip(fills, sources)
    )
    pulled = lax.fori_loop(0, all_lines, pull, start, unroll=8)
    for ref, parts in zip(packs, pulled):
        for b in range(blocks):
            ref[SUB * b : SUB * (b + 1), :] = parts[b]


def match_group(g, at, depth, packs, unroll):
    sub = lax.broadcasted_iota(jnp.int32, (SUB, LANES), 0)
    tiles = WIDTH // SUB
    marks = [sub + (g * WIDTH + SUB * q) for q in range(tiles)]
    start = (
        (jnp.full((SUB, LANES), LOWEST_FILL, jnp.float32),) * tiles,
        (jnp.full((SUB, LANES), KEY_LOW, jnp.int32),) * tiles,
        (jnp.zeros((SUB, LANES), jnp.float32),) * tiles,
    )

    def one(j, carry):
        pens, keys, gaps = (list(part) for part in carry)
        slot, pen, key, gap = (row(ref, at + j) for ref in packs)
        for q in range(tiles):
            hit = slot == marks[q]
            pens[q] = jnp.maximum(pens[q], jnp.where(hit, pen, LOWEST_FILL))
            keys[q] = jnp.maximum(keys[q], jnp.where(hit, key, KEY_LOW))
            gaps[q] = gaps[q] + jnp.where(hit, gap, 0.0)
        return tuple(pens), tuple(keys), tuple(gaps)

    if unroll == depth:
        for j in range(depth):
            start = one(j, start)
        return start
    return lax.fori_loop(0, depth, one, start, unroll=unroll)


def keep_group(accs, side, parts):
    for ref, part in zip(accs, parts):
        for q in range(WIDTH // SUB):
            at = side * WIDTH + q * SUB
            ref[at : at + SUB, :] = part[q]


def across(accs):
    pens, keys, gaps = (ref[...].T for ref in accs)
    return (
        jnp.max(pens, axis=0, keepdims=True),
        jnp.max(keys, axis=0, keepdims=True),
        jnp.sum(gaps, axis=0, keepdims=True),
    )


def project(wt, x_ref, off_ref, tile):
    cols = pl.ds(tile * TILE, TILE)
    per_tile = TILE // LANES
    offset = jnp.concatenate([row(off_ref, tile * per_tile + i) for i in range(per_tile)], axis=1)
    sub = lax.broadcasted_iota(jnp.int32, (SUB, TILE), 0)
    a, b, c = (part.astype(jnp.float32) for part in split3(offset))
    extra = jnp.where(sub == 0, a, jnp.where(sub == 1, b, jnp.where(sub == 2, c, 0.0)))
    extra = jnp.concatenate([extra, jnp.zeros((EXTRA - SUB, TILE), jnp.float32)], axis=0)
    x = jnp.concatenate([x_ref[:, cols], extra.astype(jnp.bfloat16)], axis=0)
    return jnp.dot(wt, x, preferred_element_type=jnp.float32)


def store_row(ref, tile, value):
    per_tile = TILE // LANES
    for i in range(per_tile):
        ref[pl.ds(tile * per_tile + i, 1), :] = value[:, i * LANES : (i + 1) * LANES]


def reduce_field(field, p_size, tile, pen_ref, gap_ref):
    low = [field[SUB * j : SUB * (j + 1)] for j in range(CHAINS)]
    for j in range(CHAINS, p_size // SUB):
        low[j % CHAINS] = jnp.minimum(low[j % CHAINS], field[SUB * j : SUB * (j + 1)])
    store_row(pen_ref, tile, -jnp.min(functools.reduce(jnp.minimum, low), axis=0, keepdims=True))
    store_row(gap_ref, tile, jnp.sum(field[p_size : p_size + SUB], axis=0, keepdims=True))


def prep_kernel(
    live_h, ns_h, nm_h, qw_h, sec_h, mst_h, off_h, jac_h, slot_h, face_h, rank_h,
    load_ref, nq_ref, pen_ref, gap_ref, jl_ref, slot_ref, code_ref, key_ref, over_pen, over_key, over_gap, pair_ref,
    x_ref, wt_ref, off_ref, live_s, ns_ref, nm_ref, qw_ref, jac_ref, face_ref, rank_ref, packs, accs, s_small, s_big,
):
    lines = slot_ref.shape[0]
    k_size, p_size = ns_ref.shape
    rows = x_ref.shape[1]

    small = [
        pltpu.make_async_copy(source, held, s_small.at[i])
        for i, (source, held) in enumerate((
            (slot_h, slot_ref), (live_h, live_s), (ns_h, ns_ref), (nm_h, nm_ref), (qw_h, qw_ref),
            (face_h, face_ref), (rank_h, rank_ref), (jac_h, jac_ref), (off_h, off_ref),
        ))
    ]
    for copy in small:
        copy.start()
    starts = [sum(PHASES[:i]) * TILE for i in range(len(PHASES))]
    for i, tiles in enumerate(PHASES):
        for half in range(2):
            width = tiles * TILE // 2
            cols = pl.ds(starts[i] + half * width, width)
            for base, source in ((0, sec_h), (k_size, mst_h)):
                pltpu.make_async_copy(
                    source.at[:, cols], x_ref.at[base : base + k_size, cols], s_big.at[i]
                ).start(priority=1)
    for copy in small:
        copy.wait()

    w = jnp.concatenate([ns_ref[...], -nm_ref[...]], axis=0).astype(jnp.float32)
    qrow = qw_ref[...]
    wt = w.T
    qmat = jnp.broadcast_to(qrow, (LANES, p_size)).T
    v = jnp.sum(wt * qmat, axis=0, keepdims=True)
    qsum = jnp.sum(qmat, axis=0, keepdims=True)
    depth = wt_ref.shape[1]
    pick = lax.broadcasted_iota(jnp.int32, (EXTRA, depth), 0)
    column = lax.broadcasted_iota(jnp.int32, (p_size, depth - 2 * k_size), 1)
    wt_ref[0:p_size, 0 : 2 * k_size] = wt.astype(jnp.bfloat16)
    wt_ref[0:p_size, 2 * k_size :] = jnp.where(column < 3, 1.0, 0.0).astype(jnp.bfloat16)
    lane_row = lax.broadcasted_iota(jnp.int32, (1, LANES), 1)
    tail = jnp.where(lane_row < 3, qsum, 0.0)[:, : depth - 2 * k_size]
    a, b, c = (part.astype(jnp.float32) for part in split3(jnp.concatenate([v, tail], axis=1)))
    stacked = jnp.where(pick == 0, a, jnp.where(pick == 1, b, jnp.where(pick == 2, c, 0.0)))
    wt_ref[p_size:, :] = stacked.astype(jnp.bfloat16)
    scaled = ns_ref[...].astype(jnp.float32) * qrow
    top = scaled.astype(jnp.bfloat16)
    low = (scaled - top.astype(jnp.float32)).astype(jnp.bfloat16)
    nq_ref[...] = jnp.concatenate([top, low], axis=0)

    weights = wt_ref[...]

    def dense(phase):
        done = x_ref.at[:, pl.ds(starts[phase], PHASES[phase] * TILE)]
        pltpu.make_async_copy(done, done, s_big.at[phase]).wait()
        for i in range(PHASES[phase]):
            tile = starts[phase] // TILE + i
            cols = pl.ds(tile * TILE, TILE)
            field = project(weights, x_ref, off_ref, tile)
            for at in range(0, p_size, 2 * SUB):
                load_ref[at : at + 2 * SUB, cols] = jnp.minimum(field[at : at + 2 * SUB].astype(jnp.bfloat16), 0)
            reduce_field(field, p_size, tile, pen_ref, gap_ref)

    dense(0)
    row_id = (
        lax.broadcasted_iota(jnp.int32, (lines, LANES), 0) * LANES
        + lax.broadcasted_iota(jnp.int32, (lines, LANES), 1)
    )
    alive = row_id < live_s[...]
    group = jnp.where(alive, slot_ref[...] // WIDTH, -1)
    before = (
        lax.broadcasted_iota(jnp.int32, (lines, lines), 1)
        < lax.broadcasted_iota(jnp.int32, (lines, lines), 0)
    )
    before = jnp.where(before, 1.0, 0.0).astype(jnp.bfloat16)
    place = jnp.zeros((lines, LANES), jnp.float32)
    for g in range(0, GROUPS, 2):
        mine = [group == g, group == g + 1]
        seen = jnp.concatenate([jnp.where(m, 1.0, 0.0).astype(jnp.bfloat16) for m in mine], axis=1)
        found = jnp.dot(before, seen, preferred_element_type=jnp.float32)
        place = jnp.where(mine[0], found[:, :LANES], jnp.where(mine[1], found[:, LANES:], place))
    code = jnp.where(alive, place.astype(jnp.int32) * CODE + group, -1)
    code_ref[...] = code
    worst = jnp.max(code)

    key_ref[...] = ((rank_ref[...] - 2) << 30) + (FACE_MASK - face_ref[...])
    jl = jnp.where(alive, jac_ref[...], 0.0)
    jl_ref[...] = jl
    over_pen[...] = jnp.full(over_pen.shape, LOWEST_FILL, jnp.float32)
    over_key[...] = jnp.full(over_key.shape, KEY_LOW, jnp.int32)
    over_gap[...] = jnp.zeros(over_gap.shape, jnp.float32)

    for phase in range(1, len(PHASES)):
        dense(phase)
    row_gap = gap_ref[...] * jl
    gap_ref[...] = row_gap
    total_gap = jnp.sum(jnp.sum(row_gap, axis=0, keepdims=True), axis=1, keepdims=True)
    total_area = jnp.sum(jnp.sum(jl, axis=0, keepdims=True), axis=1, keepdims=True)
    total_area = total_area * jnp.sum(qrow, axis=1, keepdims=True)
    pair_ref[...] = jnp.where(lane_row == 0, total_gap, jnp.where(lane_row == 1, total_area, 0.0))

    @pl.when(worst >= DEPTH * CODE)
    def _():
        face_ref[...] = code_ref[...]

        def one(worst):
            code = face_ref[...]
            g = worst & (CODE - 1)
            low = jnp.maximum((worst // CODE) & -SUB, DEPTH)
            pull_groups(g, 1, low, SUB, face_ref, (slot_ref, pen_ref, key_ref, gap_ref), packs)
            found = match_group(g, 0, SUB, packs, 2)
            odd = jnp.full((SUB, LANES), g & 1, jnp.int32)
            for side in range(PER_ROW):
                keep_group(accs, side, [
                    [jnp.where(odd == side, x, fill) for x in part]
                    for part, fill in zip(found, (LOWEST_FILL, KEY_LOW, 0.0))
                ])
            pen, key, gap = across(accs)
            at = pl.ds(g // PER_ROW, 1)
            over_pen[at, :] = jnp.maximum(over_pen[at, :], pen)
            over_key[at, :] = jnp.maximum(over_key[at, :], key)
            over_gap[at, :] = over_gap[at, :] + gap
            done = ((code & (CODE - 1)) == g) & (code >= low * CODE)
            code = jnp.where(done, -1, code)
            face_ref[...] = code
            return jnp.max(code)

        lax.while_loop(lambda worst: worst >= DEPTH * CODE, one, worst)


def main_kernel(
    n_dom, n_rep,
    load_ref, nq_ref, pen_ref, gap_ref, jl_ref, slot_ref, code_ref, key_ref, over_pen, over_key, over_gap, pair_ref,
    force_ref, out_pen, out_face, out_gap, out_mean,
    packs, even_accs, odd_accs, raw_pen, raw_key, raw_gap,
    sp_sf, sp_si, ow_sf, ow_si, t2_s, sp_f, sp_i, ow_f, ow_i, t1_d, t2_d,
    s_spf, r_spf, s_spi, r_spi, s_owf, r_owf, s_owi, r_owi, s_t1, r_t1, s_t2, r_t2, inside, follows,
):
    dom = lax.axis_index("dom")
    rep = lax.axis_index("rep")
    k_size = force_ref.shape[0]
    rows = force_ref.shape[1]
    per_tile = TILE // LANES
    tiles = rows // TILE
    count = n_dom * n_rep
    me = dom * n_rep + rep

    def flat(d, r):
        return lax.rem(d + n_dom, n_dom) * n_rep + lax.rem(r + n_rep, n_rep)

    barrier = pltpu.get_barrier_semaphore()

    def signal(sem, first, last):
        def one(other, carry):
            pl.semaphore_signal(sem, inc=1, device_id=other, device_id_type=LOGICAL)
            return carry

        lax.fori_loop(first, last, one, 0)

    odd = lax.rem(rep, 2)
    mate = rep + 1 - 2 * odd
    signal(barrier, me + 1, count)
    signal(barrier, me - odd, me)

    def wide_row(ref, tile):
        return jnp.concatenate([row(ref, tile * per_tile + i) for i in range(per_tile)], axis=1)

    last_dom = dom == n_dom - 1
    first_copy = pltpu.make_async_remote_copy(
        src_ref=pair_ref, dst_ref=t1_d, send_sem=s_t1, recv_sem=r_t1,
        device_id=flat(dom, mate), device_id_type=LOGICAL,
    )
    pl.semaphore_wait(barrier, me + 1 - odd)
    first_copy.start()
    signal(follows, jnp.maximum(dom - 1, 0) * n_rep, dom * n_rep)

    def pull_batch(first):
        pull_groups(first, BATCH, 0, DEPTH, code_ref, (slot_ref, pen_ref, key_ref, gap_ref), packs)

    def match_pair(first, i, accs, last_accs, over, at):
        g = first + i * PER_ROW
        keep_group(accs, 0, match_group(g, i * PER_ROW * DEPTH, DEPTH, packs, LOOP_UNROLL))
        if last_accs is not None:
            close_pair(last_accs, over, at)
        keep_group(accs, 1, match_group(g + 1, (i * PER_ROW + 1) * DEPTH, DEPTH, packs, DEPTH))

    def close_pair(accs, over, at):
        pen, key, gap = across(accs)
        over, at = pl.ds(over, 1), pl.ds(at, 1)
        raw_pen[at, :] = jnp.maximum(pen, over_pen[over, :])
        raw_key[at, :] = jnp.maximum(key, over_key[over, :])
        raw_gap[at, :] = gap + over_gap[over, :]

    def decode(top, best):
        none = top < LOWEST_FILL * 0.5
        rank = jnp.where(none, -1, (best >> 30) + 2)
        face = jnp.where(none, FACE_LIMIT, FACE_MASK - (best & FACE_MASK))
        return rank, face

    pull_batch(OWN_GROUPS)

    match_pair(OWN_GROUPS, 0, even_accs, None, 0, 0)
    match_pair(OWN_GROUPS, 1, odd_accs, even_accs, OWN_ROWS, 0)
    close_pair(odd_accs, OWN_ROWS + 1, 1)
    part = slice(0, SPILL_ROWS)
    rank, face = decode(raw_pen[part, :], raw_key[part, :])
    sp_sf[0:SPILL_ROWS, :] = raw_pen[part, :]
    sp_sf[SPILL_ROWS:, :] = raw_gap[part, :]
    sp_si[0:SPILL_ROWS, :] = rank
    sp_si[SPILL_ROWS:, :] = face

    @pl.when(jnp.logical_not(last_dom))
    def _():
        pl.semaphore_wait(follows, n_rep)

    def spill_copy(j):
        where = flat(dom + 1, rep + j)
        return (
            pltpu.make_async_remote_copy(
                src_ref=sp_sf, dst_ref=sp_f.at[rep], send_sem=s_spf, recv_sem=r_spf,
                device_id=where, device_id_type=LOGICAL,
            ),
            pltpu.make_async_remote_copy(
                src_ref=sp_si, dst_ref=sp_i.at[rep], send_sem=s_spi, recv_sem=r_spi,
                device_id=where, device_id_type=LOGICAL,
            ),
        )

    for j in range(n_rep):
        for copy in spill_copy(j):
            copy.start()

    signal(inside, 0, me)
    first_copy.wait_recv()
    pairs = count // 2
    pair = lax.div(me, 2)
    both = pair_ref[...] + t1_d[...]
    t2_s[...] = both
    t2_d[pl.ds(pair, 1), :] = both

    def send_pairs(first, last):
        def one(other, carry):
            pltpu.make_async_remote_copy(
                src_ref=t2_s, dst_ref=t2_d.at[pl.ds(pair, 1), :], send_sem=s_t2, recv_sem=r_t2,
                device_id=other * 2 + odd, device_id_type=LOGICAL,
            ).start()
            return carry

        lax.fori_loop(first, last, one, 0)

    send_pairs(0, pair)

    def send_up():
        @pl.when(me < count - 1)
        def _():
            pl.semaphore_wait(inside, count - 1 - me)

        send_pairs(pair + 1, pairs)

    quarter = lax.div(me * 4, count)
    turn = OWN_BATCHES - jnp.maximum(quarter * 2 - 3, 0)

    def own_scan(i, carry):
        @pl.when(i == turn)
        def _():
            send_up()

        first = i * BATCH
        last = lax.rem(2 * i + OWN_ROWS - 1, OWN_ROWS)
        pull_batch(first)
        match_pair(first, 0, even_accs, odd_accs, last, last)
        match_pair(first, 1, odd_accs, even_accs, 2 * i, 2 * i)
        return carry

    lax.fori_loop(0, OWN_BATCHES, own_scan, 0)
    close_pair(odd_accs, OWN_ROWS - 1, OWN_ROWS - 1)
    @pl.when(turn >= OWN_BATCHES)
    def _():
        send_up()

    rank, face = decode(raw_pen[...], raw_key[...])
    ow_sf[0] = raw_pen[...]
    ow_sf[1] = raw_gap[...]
    ow_si[0] = rank
    ow_si[1] = face

    def own_copy(j):
        where = flat(dom, rep + j)
        return (
            pltpu.make_async_remote_copy(
                src_ref=ow_sf, dst_ref=ow_f.at[rep], send_sem=s_owf, recv_sem=r_owf,
                device_id=where, device_id_type=LOGICAL,
            ),
            pltpu.make_async_remote_copy(
                src_ref=ow_si, dst_ref=ow_i.at[rep], send_sem=s_owi, recv_sem=r_owi,
                device_id=where, device_id_type=LOGICAL,
            ),
        )

    for j in range(1, n_rep):
        for copy in own_copy(j):
            copy.start()
    ow_f[rep] = ow_sf[...]
    ow_i[rep] = ow_si[...]

    nq = nq_ref[...]

    def push(step, carry):
        for i in range(FORCE_UNROLL):
            tile = step * FORCE_UNROLL + i
            cols = pl.ds(tile * TILE, TILE)
            force = jnp.dot(nq, load_ref[:, cols], preferred_element_type=jnp.float32)
            scale = wide_row(jl_ref, tile)[0:1] * -PENALTY
            force_ref[:, cols] = ((force[:k_size] + force[k_size:]) * scale).astype(jnp.bfloat16)
        return carry

    lax.fori_loop(0, tiles // FORCE_UNROLL, push, 0)

    def encode(rank, face):
        return jnp.where(rank < 0, KEY_LOW, ((rank - 2) << 30) + (FACE_MASK - face))

    def settle(ref, sem):
        pltpu.make_async_copy(ref, ref, sem).wait()

    settle(ow_f.at[pl.ds(0, n_rep - 1)], r_owf)
    settle(ow_i.at[pl.ds(0, n_rep - 1)], r_owi)
    pen_o, gap_o = ow_f[0, 0], ow_f[0, 1]
    key_o = encode(ow_i[0, 0], ow_i[0, 1])
    for r in range(1, n_rep):
        pen_o = jnp.maximum(pen_o, ow_f[r, 0])
        gap_o = gap_o + ow_f[r, 1]
        key_o = jnp.maximum(key_o, encode(ow_i[r, 0], ow_i[r, 1]))

    settle(sp_f, s_spf)
    settle(sp_i, s_spi)
    settle(ow_f.at[pl.ds(0, n_rep - 1)], s_owf)
    settle(ow_i.at[pl.ds(0, n_rep - 1)], s_owi)
    first_copy.wait_send()
    settle(t2_d.at[pl.ds(0, pairs - 1), :], s_t2)

    settle(t2_d.at[pl.ds(0, pairs - 1), :], r_t2)
    whole = jnp.sum(t2_d[...], axis=0, keepdims=True)
    out_mean[...] = whole[:, 0:1] / whole[:, 1:2]

    settle(sp_f, r_spf)
    settle(sp_i, r_spi)
    g = SPILL_ROWS
    pen_s, gap_s = sp_f[0, 0:g], sp_f[0, g:]
    key_s = encode(sp_i[0, 0:g], sp_i[0, g:])
    for r in range(1, n_rep):
        pen_s = jnp.maximum(pen_s, sp_f[r, 0:g])
        gap_s = gap_s + sp_f[r, g:]
        key_s = jnp.maximum(key_s, encode(sp_i[r, 0:g], sp_i[r, g:]))

    def finish(at, pen, key, gap):
        none = pen < LOWEST_FILL * 0.5
        out_pen[at, :] = jnp.where(none, 0.0, pen)
        out_face[at, :] = jnp.where(none, -1, FACE_MASK - (key & FACE_MASK))
        out_gap[at, :] = jnp.where(none, 0.0, gap)

    finish(
        slice(0, g), jnp.maximum(pen_o[:g], pen_s), jnp.maximum(key_o[:g], key_s), gap_o[:g] + gap_s
    )
    finish(slice(g, OWN_ROWS), pen_o[g:], key_o[g:], gap_o[g:])


def finish_kernel(force_ref, pen_ref, face_ref, gap_ref, mean_ref, force_h, pen_h, face_h, gap_h, mean_h, sems, s_force):
    copies = [
        pltpu.make_async_copy(held, out, sems.at[i])
        for i, (held, out) in enumerate((
            (pen_ref, pen_h), (face_ref, face_h), (gap_ref, gap_h), (mean_ref, mean_h)
        ))
    ]
    for at in range(0, force_ref.shape[0], SUB):
        part = (slice(at, at + SUB), slice(None))
        pltpu.make_async_copy(force_ref.at[part], force_h.at[part], s_force).start()
    for copy in copies:
        copy.start()
    for copy in copies:
        copy.wait()
    pltpu.make_async_copy(force_ref, force_h, s_force).wait()


def solution(mesh):
    n_dom, n_rep = mesh.shape["dom"], mesh.shape["rep"]
    vmem = pl.BlockSpec(memory_space=pltpu.VMEM)
    anywhere = pl.BlockSpec(memory_space=pl.ANY)
    dma = pltpu.SemaphoreType.DMA

    def kept(x):
        return pltpu.with_memory_space_constraint(x, pltpu.VMEM)

    def streamed(x):
        return pltpu.with_memory_space_constraint(x, pltpu.HBM)

    def shards(ns, nm, sec, mst, off, qw, jac, slot, face, rank, live):
        k_size, p_size = ns.shape
        rows = sec.shape[1]
        lines = rows // LANES
        depth = 2 * k_size + EXTRA
        f32, i32, bf16 = jnp.float32, jnp.int32, jnp.bfloat16

        off, jac, slot, face, rank = (x.reshape(lines, LANES) for x in (off, jac, slot, face, rank))

        def packs(deep):
            return [pltpu.VMEM((deep + SUB, LANES), t) for t in (i32, f32, i32, f32)]

        def lanes():
            return [pltpu.VMEM((LANES, LANES), t) for t in (f32, i32, f32)]

        held = pl.pallas_call(
            prep_kernel,
            out_shape=(
                pltpu.VMEM((p_size, rows), bf16),
                pltpu.VMEM((2 * k_size, p_size), bf16),
                pltpu.VMEM((lines, LANES), f32),
                pltpu.VMEM((lines, LANES), f32),
                pltpu.VMEM((lines, LANES), f32),
                pltpu.VMEM((lines, LANES), i32),
                pltpu.VMEM((lines, LANES), i32),
                pltpu.VMEM((lines, LANES), i32),
                pltpu.VMEM((ALL_ROWS, LANES), f32),
                pltpu.VMEM((ALL_ROWS, LANES), i32),
                pltpu.VMEM((ALL_ROWS, LANES), f32),
                pltpu.VMEM((1, LANES), f32),
            ),
            in_specs=[anywhere] * 11,
            out_specs=(vmem,) * 12,
            scratch_shapes=[
                pltpu.VMEM((2 * k_size, rows), bf16),
                pltpu.VMEM((p_size + EXTRA, depth), bf16),
                pltpu.VMEM((lines, LANES), f32),
                pltpu.VMEM((1, 1), i32),
                pltpu.VMEM((k_size, p_size), bf16),
                pltpu.VMEM((k_size, p_size), bf16),
                pltpu.VMEM((1, p_size), f32),
                pltpu.VMEM((lines, LANES), f32),
                pltpu.VMEM((lines, LANES), i32),
                pltpu.VMEM((lines, LANES), i32),
                packs(SUB),
                lanes(),
                dma((9,)),
                dma((len(PHASES),)),
            ],
            compiler_params=pltpu.CompilerParams(vmem_limit_bytes=VMEM_LIMIT),
        )(
            live.reshape(1, 1),
            *(streamed(x) for x in (ns, nm, qw.reshape(1, p_size), sec, mst, off, jac, slot, face, rank)),
        )

        spill = (2 * SPILL_ROWS, LANES)
        own = (2, OWN_ROWS, LANES)
        pairs = n_dom * n_rep // 2
        results = pl.pallas_call(
            functools.partial(main_kernel, n_dom, n_rep),
            out_shape=(
                pltpu.VMEM((k_size, rows), bf16),
                pltpu.VMEM((OWN_ROWS, LANES), f32),
                pltpu.VMEM((OWN_ROWS, LANES), i32),
                pltpu.VMEM((OWN_ROWS, LANES), f32),
                pltpu.VMEM((1, 1), f32),
            ),
            in_specs=[vmem] * 12,
            out_specs=(vmem,) * 5,
            scratch_shapes=[
                packs(BATCH * DEPTH),
                lanes(),
                lanes(),
                pltpu.VMEM((OWN_ROWS, LANES), f32),
                pltpu.VMEM((OWN_ROWS, LANES), i32),
                pltpu.VMEM((OWN_ROWS, LANES), f32),
                pltpu.VMEM(spill, f32),
                pltpu.VMEM(spill, i32),
                pltpu.VMEM(own, f32),
                pltpu.VMEM(own, i32),
                pltpu.VMEM((1, LANES), f32),
                pltpu.VMEM((n_rep,) + spill, f32),
                pltpu.VMEM((n_rep,) + spill, i32),
                pltpu.VMEM((n_rep,) + own, f32),
                pltpu.VMEM((n_rep,) + own, i32),
                pltpu.VMEM((1, LANES), f32),
                pltpu.VMEM((pairs, LANES), f32),
            ] + [dma] * 12 + [pltpu.SemaphoreType.REGULAR] * 2,
            compiler_params=pltpu.CompilerParams(
                collective_id=0, has_side_effects=True, vmem_limit_bytes=VMEM_LIMIT
            ),
        )(*(kept(x) for x in held))

        force, seg_pen, seg_face, seg_gap, mean = pl.pallas_call(
            finish_kernel,
            out_shape=tuple(jax.ShapeDtypeStruct(x.shape, x.dtype) for x in results),
            in_specs=[vmem] * 5,
            out_specs=(anywhere,) * 5,
            scratch_shapes=[dma((4,)), dma],
            compiler_params=pltpu.CompilerParams(vmem_limit_bytes=VMEM_LIMIT),
        )(*(kept(x) for x in results))
        seg_pen, seg_face, seg_gap = (x.reshape(SEG_DEV) for x in (seg_pen, seg_face, seg_gap))
        return force, seg_pen, seg_face, seg_gap, mean.reshape(())

    rows_spec, wide_spec = P(("dom", "rep")), P(None, ("dom", "rep"))
    return jax.shard_map(
        shards,
        mesh=mesh,
        in_specs=(P(), P(), wide_spec, wide_spec, rows_spec, P()) + (rows_spec,) * 5,
        out_specs=(wide_spec, P("dom"), P("dom"), P("dom"), P()),
        check_vma=False,
    )
```

```python
import functools

import jax
import jax.numpy as jnp
from jax import lax
from jax.experimental import pallas as pl
from jax.experimental.pallas import tpu as pltpu
from jax.sharding import PartitionSpec as P

SEG_DEV = 1024
SPILL = 256
LANES = 128
SUB = 8
WIDTH = 64
PER_ROW = LANES // WIDTH
GROUPS = (SEG_DEV + SPILL) // WIDTH
OWN_GROUPS = SEG_DEV // WIDTH
SPILL_GROUPS = SPILL // WIDTH
OWN_ROWS = SEG_DEV // LANES
SPILL_ROWS = SPILL // LANES
ALL_ROWS = 16
CODE = 32

PENALTY = 400.0
LOWEST_FILL = -1e30
FACE_LIMIT = 1073741824
FACE_MASK = FACE_LIMIT - 1
KEY_LOW = -2147483648
LOGICAL = pl.DeviceIdType.LOGICAL
TILE = 256
DEPTH = 12
BATCH = 4
OWN_BATCHES = OWN_GROUPS // BATCH
PHASES = (4, 28)
CHAINS = 4
FORCE_UNROLL = 8
LOOP_UNROLL = 4
EXTRA = 16
VMEM_LIMIT = 32 << 20


def split3(x):
    a = x.astype(jnp.bfloat16)
    rest = x - a.astype(jnp.float32)
    b = rest.astype(jnp.bfloat16)
    c = (rest - b.astype(jnp.float32)).astype(jnp.bfloat16)
    return a, b, c


def row(ref, at):
    return ref[pl.ds(at, SUB, stride=0), :]


def pull_groups(first, count, depth0, depth, code_ref, sources, packs):
    all_lines = code_ref.shape[0]
    sub = lax.broadcasted_iota(jnp.int32, (SUB, LANES), 0)
    blocks = -(-count * depth // SUB)
    wants = []
    for b in range(blocks):
        line = sub + SUB * b
        want = jnp.full((SUB, LANES), -2, jnp.int32)
        for q in range(count):
            inside = (line >= q * depth) & (line < (q + 1) * depth)
            want = jnp.where(inside, (line + (depth0 - q * depth)) * CODE + (first + q), want)
        wants.append(want)
    fills = (-1, LOWEST_FILL, -1, 0.0)

    def pull(i, carry):
        parts = [list(part) for part in carry]
        code = row(code_ref, i)
        values = [row(ref, i) for ref in sources]
        for b in range(blocks):
            hit = code == wants[b]
            for part, value in zip(parts, values):
                part[b] = jnp.where(hit, value, part[b])
        return tuple(tuple(part) for part in parts)

    start = tuple(
        (jnp.full((SUB, LANES), fill, ref.dtype),) * blocks for fill, ref in zip(fills, sources)
    )
    pulled = lax.fori_loop(0, all_lines, pull, start, unroll=8)
    for ref, parts in zip(packs, pulled):
        for b in range(blocks):
            ref[SUB * b : SUB * (b + 1), :] = parts[b]


def match_group(g, at, depth, packs, unroll):
    sub = lax.broadcasted_iota(jnp.int32, (SUB, LANES), 0)
    tiles = WIDTH // SUB
    marks = [sub + (g * WIDTH + SUB * q) for q in range(tiles)]
    start = (
        (jnp.full((SUB, LANES), LOWEST_FILL, jnp.float32),) * tiles,
        (jnp.full((SUB, LANES), KEY_LOW, jnp.int32),) * tiles,
        (jnp.zeros((SUB, LANES), jnp.float32),) * tiles,
    )

    def one(j, carry):
        pens, keys, gaps = (list(part) for part in carry)
        slot, pen, key, gap = (row(ref, at + j) for ref in packs)
        for q in range(tiles):
            hit = slot == marks[q]
            pens[q] = jnp.maximum(pens[q], jnp.where(hit, pen, LOWEST_FILL))
            keys[q] = jnp.maximum(keys[q], jnp.where(hit, key, KEY_LOW))
            gaps[q] = gaps[q] + jnp.where(hit, gap, 0.0)
        return tuple(pens), tuple(keys), tuple(gaps)

    if unroll == depth:
        for j in range(depth):
            start = one(j, start)
        return start
    return lax.fori_loop(0, depth, one, start, unroll=unroll)


def keep_group(accs, side, parts):
    for ref, part in zip(accs, parts):
        for q in range(WIDTH // SUB):
            at = side * WIDTH + q * SUB
            ref[at : at + SUB, :] = part[q]


def across(accs):
    pens, keys, gaps = (ref[...].T for ref in accs)
    return (
        jnp.max(pens, axis=0, keepdims=True),
        jnp.max(keys, axis=0, keepdims=True),
        jnp.sum(gaps, axis=0, keepdims=True),
    )


def project(wt, x_ref, off_ref, tile):
    cols = pl.ds(tile * TILE, TILE)
    per_tile = TILE // LANES
    offset = jnp.concatenate([row(off_ref, tile * per_tile + i) for i in range(per_tile)], axis=1)
    sub = lax.broadcasted_iota(jnp.int32, (SUB, TILE), 0)
    a, b, c = (part.astype(jnp.float32) for part in split3(offset))
    extra = jnp.where(sub == 0, a, jnp.where(sub == 1, b, jnp.where(sub == 2, c, 0.0)))
    extra = jnp.concatenate([extra, jnp.zeros((EXTRA - SUB, TILE), jnp.float32)], axis=0)
    x = jnp.concatenate([x_ref[:, cols], extra.astype(jnp.bfloat16)], axis=0)
    return jnp.dot(wt, x, preferred_element_type=jnp.float32)


def store_row(ref, tile, value):
    per_tile = TILE // LANES
    for i in range(per_tile):
        ref[pl.ds(tile * per_tile + i, 1), :] = value[:, i * LANES : (i + 1) * LANES]


def reduce_field(field, p_size, tile, pen_ref, gap_ref):
    low = [field[SUB * j : SUB * (j + 1)] for j in range(CHAINS)]
    for j in range(CHAINS, p_size // SUB):
        low[j % CHAINS] = jnp.minimum(low[j % CHAINS], field[SUB * j : SUB * (j + 1)])
    store_row(pen_ref, tile, -jnp.min(functools.reduce(jnp.minimum, low), axis=0, keepdims=True))
    store_row(gap_ref, tile, jnp.sum(field[p_size : p_size + SUB], axis=0, keepdims=True))


def prep_kernel(
    live_h, ns_h, nm_h, qw_h, sec_h, mst_h, off_h, jac_h, slot_h, face_h, rank_h,
    load_ref, nq_ref, pen_ref, gap_ref, jl_ref, slot_ref, code_ref, key_ref, over_pen, over_key, over_gap, pair_ref,
    x_ref, wt_ref, off_ref, live_s, ns_ref, nm_ref, qw_ref, jac_ref, face_ref, rank_ref, packs, accs, s_small, s_big,
):
    lines = slot_ref.shape[0]
    k_size, p_size = ns_ref.shape
    rows = x_ref.shape[1]

    small = [
        pltpu.make_async_copy(source, held, s_small.at[i])
        for i, (source, held) in enumerate((
            (slot_h, slot_ref), (live_h, live_s), (ns_h, ns_ref), (nm_h, nm_ref), (qw_h, qw_ref),
            (face_h, face_ref), (rank_h, rank_ref), (jac_h, jac_ref), (off_h, off_ref),
        ))
    ]
    for copy in small:
        copy.start()
    starts = [sum(PHASES[:i]) * TILE for i in range(len(PHASES))]
    for i, tiles in enumerate(PHASES):
        for half in range(2):
            width = tiles * TILE // 2
            cols = pl.ds(starts[i] + half * width, width)
            for base, source in ((0, sec_h), (k_size, mst_h)):
                pltpu.make_async_copy(
                    source.at[:, cols], x_ref.at[base : base + k_size, cols], s_big.at[i]
                ).start(priority=1)
    for copy in small:
        copy.wait()

    w = jnp.concatenate([ns_ref[...], -nm_ref[...]], axis=0).astype(jnp.float32)
    qrow = qw_ref[...]
    wt = w.T
    qmat = jnp.broadcast_to(qrow, (LANES, p_size)).T
    v = jnp.sum(wt * qmat, axis=0, keepdims=True)
    qsum = jnp.sum(qmat, axis=0, keepdims=True)
    depth = wt_ref.shape[1]
    pick = lax.broadcasted_iota(jnp.int32, (EXTRA, depth), 0)
    column = lax.broadcasted_iota(jnp.int32, (p_size, depth - 2 * k_size), 1)
    wt_ref[0:p_size, 0 : 2 * k_size] = wt.astype(jnp.bfloat16)
    wt_ref[0:p_size, 2 * k_size :] = jnp.where(column < 3, 1.0, 0.0).astype(jnp.bfloat16)
    lane_row = lax.broadcasted_iota(jnp.int32, (1, LANES), 1)
    tail = jnp.where(lane_row < 3, qsum, 0.0)[:, : depth - 2 * k_size]
    a, b, c = (part.astype(jnp.float32) for part in split3(jnp.concatenate([v, tail], axis=1)))
    stacked = jnp.where(pick == 0, a, jnp.where(pick == 1, b, jnp.where(pick == 2, c, 0.0)))
    wt_ref[p_size:, :] = stacked.astype(jnp.bfloat16)
    scaled = ns_ref[...].astype(jnp.float32) * qrow
    top = scaled.astype(jnp.bfloat16)
    low = (scaled - top.astype(jnp.float32)).astype(jnp.bfloat16)
    nq_ref[...] = jnp.concatenate([top, low], axis=0)

    weights = wt_ref[...]

    def dense(phase):
        done = x_ref.at[:, pl.ds(starts[phase], PHASES[phase] * TILE)]
        pltpu.make_async_copy(done, done, s_big.at[phase]).wait()
        for i in range(PHASES[phase]):
            tile = starts[phase] // TILE + i
            cols = pl.ds(tile * TILE, TILE)
            field = project(weights, x_ref, off_ref, tile)
            for at in range(0, p_size, 2 * SUB):
                load_ref[at : at + 2 * SUB, cols] = jnp.minimum(field[at : at + 2 * SUB].astype(jnp.bfloat16), 0)
            reduce_field(field, p_size, tile, pen_ref, gap_ref)

    dense(0)
    row_id = (
        lax.broadcasted_iota(jnp.int32, (lines, LANES), 0) * LANES
        + lax.broadcasted_iota(jnp.int32, (lines, LANES), 1)
    )
    alive = row_id < live_s[...]
    group = jnp.where(alive, slot_ref[...] // WIDTH, -1)
    before = (
        lax.broadcasted_iota(jnp.int32, (lines, lines), 1)
        < lax.broadcasted_iota(jnp.int32, (lines, lines), 0)
    )
    before = jnp.where(before, 1.0, 0.0).astype(jnp.bfloat16)
    place = jnp.zeros((lines, LANES), jnp.float32)
    for g in range(0, GROUPS, 2):
        mine = [group == g, group == g + 1]
        seen = jnp.concatenate([jnp.where(m, 1.0, 0.0).astype(jnp.bfloat16) for m in mine], axis=1)
        found = jnp.dot(before, seen, preferred_element_type=jnp.float32)
        place = jnp.where(mine[0], found[:, :LANES], jnp.where(mine[1], found[:, LANES:], place))
    code = jnp.where(alive, place.astype(jnp.int32) * CODE + group, -1)
    code_ref[...] = code
    worst = jnp.max(code)

    key_ref[...] = ((rank_ref[...] - 2) << 30) + (FACE_MASK - face_ref[...])
    jl = jnp.where(alive, jac_ref[...], 0.0)
    jl_ref[...] = jl
    over_pen[...] = jnp.full(over_pen.shape, LOWEST_FILL, jnp.float32)
    over_key[...] = jnp.full(over_key.shape, KEY_LOW, jnp.int32)
    over_gap[...] = jnp.zeros(over_gap.shape, jnp.float32)

    for phase in range(1, len(PHASES)):
        dense(phase)
    row_gap = gap_ref[...] * jl
    gap_ref[...] = row_gap
    total_gap = jnp.sum(jnp.sum(row_gap, axis=0, keepdims=True), axis=1, keepdims=True)
    total_area = jnp.sum(jnp.sum(jl, axis=0, keepdims=True), axis=1, keepdims=True)
    total_area = total_area * jnp.sum(qrow, axis=1, keepdims=True)
    pair_ref[...] = jnp.where(lane_row == 0, total_gap, jnp.where(lane_row == 1, total_area, 0.0))

    @pl.when(worst >= DEPTH * CODE)
    def _():
        face_ref[...] = code_ref[...]

        def one(worst):
            code = face_ref[...]
            g = worst & (CODE - 1)
            low = jnp.maximum((worst // CODE) & -SUB, DEPTH)
            pull_groups(g, 1, low, SUB, face_ref, (slot_ref, pen_ref, key_ref, gap_ref), packs)
            found = match_group(g, 0, SUB, packs, 2)
            odd = jnp.full((SUB, LANES), g & 1, jnp.int32)
            for side in range(PER_ROW):
                keep_group(accs, side, [
                    [jnp.where(odd == side, x, fill) for x in part]
                    for part, fill in zip(found, (LOWEST_FILL, KEY_LOW, 0.0))
                ])
            pen, key, gap = across(accs)
            at = pl.ds(g // PER_ROW, 1)
            over_pen[at, :] = jnp.maximum(over_pen[at, :], pen)
            over_key[at, :] = jnp.maximum(over_key[at, :], key)
            over_gap[at, :] = over_gap[at, :] + gap
            done = ((code & (CODE - 1)) == g) & (code >= low * CODE)
            code = jnp.where(done, -1, code)
            face_ref[...] = code
            return jnp.max(code)

        lax.while_loop(lambda worst: worst >= DEPTH * CODE, one, worst)


def main_kernel(
    n_dom, n_rep,
    load_ref, nq_ref, pen_ref, gap_ref, jl_ref, slot_ref, code_ref, key_ref, over_pen, over_key, over_gap, pair_ref,
    force_ref, out_pen, out_face, out_gap, out_mean,
    packs, even_accs, odd_accs, raw_pen, raw_key, raw_gap,
    sp_sf, sp_si, ow_sf, ow_si, t2_s, sp_f, sp_i, ow_f, ow_i, t1_d, t2_d,
    s_spf, r_spf, s_spi, r_spi, s_owf, r_owf, s_owi, r_owi, s_t1, r_t1, s_t2, r_t2, inside, follows, peers,
):
    dom = lax.axis_index("dom")
    rep = lax.axis_index("rep")
    k_size = force_ref.shape[0]
    rows = force_ref.shape[1]
    per_tile = TILE // LANES
    tiles = rows // TILE
    count = n_dom * n_rep
    me = dom * n_rep + rep

    def flat(d, r):
        return lax.rem(d + n_dom, n_dom) * n_rep + lax.rem(r + n_rep, n_rep)

    barrier = pltpu.get_barrier_semaphore()

    def signal(sem, first, last, step=1, at=0):
        def one(i, carry):
            pl.semaphore_signal(sem, inc=1, device_id=i * step + at, device_id_type=LOGICAL)
            return carry

        lax.fori_loop(first, last, one, 0)

    odd = lax.rem(rep, 2)
    mate = rep + 1 - 2 * odd
    signal(barrier, me + 1, count)
    signal(barrier, me - odd, me)

    def wide_row(ref, tile):
        return jnp.concatenate([row(ref, tile * per_tile + i) for i in range(per_tile)], axis=1)

    last_dom = dom == n_dom - 1
    first_copy = pltpu.make_async_remote_copy(
        src_ref=pair_ref, dst_ref=t1_d, send_sem=s_t1, recv_sem=r_t1,
        device_id=flat(dom, mate), device_id_type=LOGICAL,
    )
    pl.semaphore_wait(barrier, me + 1 - odd)
    first_copy.start()
    pairs = count // 2
    pair = lax.div(me, 2)
    signal(inside, 0, pair, 2, odd)
    signal(follows, jnp.maximum(dom - 1, 0) * n_rep, dom * n_rep)
    signal(peers, dom * n_rep, me)

    def pull_batch(first):
        pull_groups(first, BATCH, 0, DEPTH, code_ref, (slot_ref, pen_ref, key_ref, gap_ref), packs)

    def match_pair(first, i, accs, last_accs, over, at):
        g = first + i * PER_ROW
        keep_group(accs, 0, match_group(g, i * PER_ROW * DEPTH, DEPTH, packs, LOOP_UNROLL))
        if last_accs is not None:
            close_pair(last_accs, over, at)
        keep_group(accs, 1, match_group(g + 1, (i * PER_ROW + 1) * DEPTH, DEPTH, packs, DEPTH))

    def close_pair(accs, over, at):
        pen, key, gap = across(accs)
        over, at = pl.ds(over, 1), pl.ds(at, 1)
        raw_pen[at, :] = jnp.maximum(pen, over_pen[over, :])
        raw_key[at, :] = jnp.maximum(key, over_key[over, :])
        raw_gap[at, :] = gap + over_gap[over, :]

    def decode(top, best):
        none = top < LOWEST_FILL * 0.5
        rank = jnp.where(none, -1, (best >> 30) + 2)
        face = jnp.where(none, FACE_LIMIT, FACE_MASK - (best & FACE_MASK))
        return rank, face

    pull_batch(OWN_GROUPS)

    match_pair(OWN_GROUPS, 0, even_accs, None, 0, 0)
    match_pair(OWN_GROUPS, 1, odd_accs, even_accs, OWN_ROWS, 0)
    close_pair(odd_accs, OWN_ROWS + 1, 1)
    part = slice(0, SPILL_ROWS)
    rank, face = decode(raw_pen[part, :], raw_key[part, :])
    sp_sf[0:SPILL_ROWS, :] = raw_pen[part, :]
    sp_sf[SPILL_ROWS:, :] = raw_gap[part, :]
    sp_si[0:SPILL_ROWS, :] = rank
    sp_si[SPILL_ROWS:, :] = face

    @pl.when(jnp.logical_not(last_dom))
    def _():
        pl.semaphore_wait(follows, n_rep)

    def spill_copy(j):
        where = flat(dom + 1, rep + j)
        return (
            pltpu.make_async_remote_copy(
                src_ref=sp_sf, dst_ref=sp_f.at[rep], send_sem=s_spf, recv_sem=r_spf,
                device_id=where, device_id_type=LOGICAL,
            ),
            pltpu.make_async_remote_copy(
                src_ref=sp_si, dst_ref=sp_i.at[rep], send_sem=s_spi, recv_sem=r_spi,
                device_id=where, device_id_type=LOGICAL,
            ),
        )

    for j in range(n_rep):
        for copy in spill_copy(j):
            copy.start()

    first_copy.wait_recv()
    both = pair_ref[...] + t1_d[...]
    t2_s[...] = both
    t2_d[pl.ds(pair, 1), :] = both

    def send_pairs(first, last):
        def one(other, carry):
            pltpu.make_async_remote_copy(
                src_ref=t2_s, dst_ref=t2_d.at[pl.ds(pair, 1), :], send_sem=s_t2, recv_sem=r_t2,
                device_id=other * 2 + odd, device_id_type=LOGICAL,
            ).start()
            return carry

        lax.fori_loop(first, last, one, 0)

    send_pairs(0, pair)

    def send_up():
        @pl.when(pair < pairs - 1)
        def _():
            pl.semaphore_wait(inside, pairs - 1 - pair)

        send_pairs(pair + 1, pairs)

    quarter = lax.div(me * 4, count)
    turn = OWN_BATCHES - jnp.maximum(quarter * 2 - 3, 0)

    def own_scan(i, carry):
        @pl.when(i == turn)
        def _():
            send_up()

        first = i * BATCH
        last = lax.rem(2 * i + OWN_ROWS - 1, OWN_ROWS)
        pull_batch(first)
        match_pair(first, 0, even_accs, odd_accs, last, last)
        match_pair(first, 1, odd_accs, even_accs, 2 * i, 2 * i)
        return carry

    lax.fori_loop(0, OWN_BATCHES, own_scan, 0)
    close_pair(odd_accs, OWN_ROWS - 1, OWN_ROWS - 1)
    rank, face = decode(raw_pen[...], raw_key[...])
    ow_sf[0] = raw_pen[...]
    ow_sf[1] = raw_gap[...]
    ow_si[0] = rank
    ow_si[1] = face

    @pl.when(rep < n_rep - 1)
    def _():
        pl.semaphore_wait(peers, n_rep - 1 - rep)

    def own_copy(j):
        where = flat(dom, rep + j)
        return (
            pltpu.make_async_remote_copy(
                src_ref=ow_sf, dst_ref=ow_f.at[rep], send_sem=s_owf, recv_sem=r_owf,
                device_id=where, device_id_type=LOGICAL,
            ),
            pltpu.make_async_remote_copy(
                src_ref=ow_si, dst_ref=ow_i.at[rep], send_sem=s_owi, recv_sem=r_owi,
                device_id=where, device_id_type=LOGICAL,
            ),
        )

    for j in range(1, n_rep):
        for copy in own_copy(j):
            copy.start()
    ow_f[rep] = ow_sf[...]
    ow_i[rep] = ow_si[...]

    @pl.when(turn >= OWN_BATCHES)
    def _():
        send_up()

    nq = nq_ref[...]

    def push(step, carry):
        for i in range(FORCE_UNROLL):
            tile = step * FORCE_UNROLL + i
            cols = pl.ds(tile * TILE, TILE)
            force = jnp.dot(nq, load_ref[:, cols], preferred_element_type=jnp.float32)
            scale = wide_row(jl_ref, tile)[0:1] * -PENALTY
            force_ref[:, cols] = ((force[:k_size] + force[k_size:]) * scale).astype(jnp.bfloat16)
        return carry

    lax.fori_loop(0, tiles // FORCE_UNROLL, push, 0)

    def encode(rank, face):
        return jnp.where(rank < 0, KEY_LOW, ((rank - 2) << 30) + (FACE_MASK - face))

    def settle(ref, sem):
        pltpu.make_async_copy(ref, ref, sem).wait()

    settle(ow_f.at[pl.ds(0, n_rep - 1)], r_owf)
    settle(ow_i.at[pl.ds(0, n_rep - 1)], r_owi)
    pen_o, gap_o = ow_f[0, 0], ow_f[0, 1]
    key_o = encode(ow_i[0, 0], ow_i[0, 1])
    for r in range(1, n_rep):
        pen_o = jnp.maximum(pen_o, ow_f[r, 0])
        gap_o = gap_o + ow_f[r, 1]
        key_o = jnp.maximum(key_o, encode(ow_i[r, 0], ow_i[r, 1]))

    settle(sp_f, s_spf)
    settle(sp_i, s_spi)
    settle(ow_f.at[pl.ds(0, n_rep - 1)], s_owf)
    settle(ow_i.at[pl.ds(0, n_rep - 1)], s_owi)
    first_copy.wait_send()
    settle(t2_d.at[pl.ds(0, pairs - 1), :], s_t2)

    settle(t2_d.at[pl.ds(0, pairs - 1), :], r_t2)
    whole = jnp.sum(t2_d[...], axis=0, keepdims=True)
    out_mean[...] = whole[:, 0:1] / whole[:, 1:2]

    settle(sp_f, r_spf)
    settle(sp_i, r_spi)
    g = SPILL_ROWS
    pen_s, gap_s = sp_f[0, 0:g], sp_f[0, g:]
    key_s = encode(sp_i[0, 0:g], sp_i[0, g:])
    for r in range(1, n_rep):
        pen_s = jnp.maximum(pen_s, sp_f[r, 0:g])
        gap_s = gap_s + sp_f[r, g:]
        key_s = jnp.maximum(key_s, encode(sp_i[r, 0:g], sp_i[r, g:]))

    def finish(at, pen, key, gap):
        none = pen < LOWEST_FILL * 0.5
        out_pen[at, :] = jnp.where(none, 0.0, pen)
        out_face[at, :] = jnp.where(none, -1, FACE_MASK - (key & FACE_MASK))
        out_gap[at, :] = jnp.where(none, 0.0, gap)

    finish(
        slice(0, g), jnp.maximum(pen_o[:g], pen_s), jnp.maximum(key_o[:g], key_s), gap_o[:g] + gap_s
    )
    finish(slice(g, OWN_ROWS), pen_o[g:], key_o[g:], gap_o[g:])


def finish_kernel(force_ref, pen_ref, face_ref, gap_ref, mean_ref, force_h, pen_h, face_h, gap_h, mean_h, sems, s_force):
    copies = [
        pltpu.make_async_copy(held, out, sems.at[i])
        for i, (held, out) in enumerate((
            (pen_ref, pen_h), (face_ref, face_h), (gap_ref, gap_h), (mean_ref, mean_h)
        ))
    ]
    for at in range(0, force_ref.shape[0], SUB):
        part = (slice(at, at + SUB), slice(None))
        pltpu.make_async_copy(force_ref.at[part], force_h.at[part], s_force).start()
    for copy in copies:
        copy.start()
    for copy in copies:
        copy.wait()
    pltpu.make_async_copy(force_ref, force_h, s_force).wait()


def solution(mesh):
    n_dom, n_rep = mesh.shape["dom"], mesh.shape["rep"]
    vmem = pl.BlockSpec(memory_space=pltpu.VMEM)
    anywhere = pl.BlockSpec(memory_space=pl.ANY)
    dma = pltpu.SemaphoreType.DMA

    def kept(x):
        return pltpu.with_memory_space_constraint(x, pltpu.VMEM)

    def streamed(x):
        return pltpu.with_memory_space_constraint(x, pltpu.HBM)

    def shards(ns, nm, sec, mst, off, qw, jac, slot, face, rank, live):
        k_size, p_size = ns.shape
        rows = sec.shape[1]
        lines = rows // LANES
        depth = 2 * k_size + EXTRA
        f32, i32, bf16 = jnp.float32, jnp.int32, jnp.bfloat16

        off, jac, slot, face, rank = (x.reshape(lines, LANES) for x in (off, jac, slot, face, rank))

        def packs(deep):
            return [pltpu.VMEM((deep + SUB, LANES), t) for t in (i32, f32, i32, f32)]

        def lanes():
            return [pltpu.VMEM((LANES, LANES), t) for t in (f32, i32, f32)]

        held = pl.pallas_call(
            prep_kernel,
            out_shape=(
                pltpu.VMEM((p_size, rows), bf16),
                pltpu.VMEM((2 * k_size, p_size), bf16),
                pltpu.VMEM((lines, LANES), f32),
                pltpu.VMEM((lines, LANES), f32),
                pltpu.VMEM((lines, LANES), f32),
                pltpu.VMEM((lines, LANES), i32),
                pltpu.VMEM((lines, LANES), i32),
                pltpu.VMEM((lines, LANES), i32),
                pltpu.VMEM((ALL_ROWS, LANES), f32),
                pltpu.VMEM((ALL_ROWS, LANES), i32),
                pltpu.VMEM((ALL_ROWS, LANES), f32),
                pltpu.VMEM((1, LANES), f32),
            ),
            in_specs=[anywhere] * 11,
            out_specs=(vmem,) * 12,
            scratch_shapes=[
                pltpu.VMEM((2 * k_size, rows), bf16),
                pltpu.VMEM((p_size + EXTRA, depth), bf16),
                pltpu.VMEM((lines, LANES), f32),
                pltpu.VMEM((1, 1), i32),
                pltpu.VMEM((k_size, p_size), bf16),
                pltpu.VMEM((k_size, p_size), bf16),
                pltpu.VMEM((1, p_size), f32),
                pltpu.VMEM((lines, LANES), f32),
                pltpu.VMEM((lines, LANES), i32),
                pltpu.VMEM((lines, LANES), i32),
                packs(SUB),
                lanes(),
                dma((9,)),
                dma((len(PHASES),)),
            ],
            compiler_params=pltpu.CompilerParams(vmem_limit_bytes=VMEM_LIMIT),
        )(
            live.reshape(1, 1),
            *(streamed(x) for x in (ns, nm, qw.reshape(1, p_size), sec, mst, off, jac, slot, face, rank)),
        )

        spill = (2 * SPILL_ROWS, LANES)
        own = (2, OWN_ROWS, LANES)
        pairs = n_dom * n_rep // 2
        results = pl.pallas_call(
            functools.partial(main_kernel, n_dom, n_rep),
            out_shape=(
                pltpu.VMEM((k_size, rows), bf16),
                pltpu.VMEM((OWN_ROWS, LANES), f32),
                pltpu.VMEM((OWN_ROWS, LANES), i32),
                pltpu.VMEM((OWN_ROWS, LANES), f32),
                pltpu.VMEM((1, 1), f32),
            ),
            in_specs=[vmem] * 12,
            out_specs=(vmem,) * 5,
            scratch_shapes=[
                packs(BATCH * DEPTH),
                lanes(),
                lanes(),
                pltpu.VMEM((OWN_ROWS, LANES), f32),
                pltpu.VMEM((OWN_ROWS, LANES), i32),
                pltpu.VMEM((OWN_ROWS, LANES), f32),
                pltpu.VMEM(spill, f32),
                pltpu.VMEM(spill, i32),
                pltpu.VMEM(own, f32),
                pltpu.VMEM(own, i32),
                pltpu.VMEM((1, LANES), f32),
                pltpu.VMEM((n_rep,) + spill, f32),
                pltpu.VMEM((n_rep,) + spill, i32),
                pltpu.VMEM((n_rep,) + own, f32),
                pltpu.VMEM((n_rep,) + own, i32),
                pltpu.VMEM((1, LANES), f32),
                pltpu.VMEM((pairs, LANES), f32),
            ] + [dma] * 12 + [pltpu.SemaphoreType.REGULAR] * 3,
            compiler_params=pltpu.CompilerParams(
                collective_id=0, has_side_effects=True, vmem_limit_bytes=VMEM_LIMIT
            ),
        )(*(kept(x) for x in held))

        force, seg_pen, seg_face, seg_gap, mean = pl.pallas_call(
            finish_kernel,
            out_shape=tuple(jax.ShapeDtypeStruct(x.shape, x.dtype) for x in results),
            in_specs=[vmem] * 5,
            out_specs=(anywhere,) * 5,
            scratch_shapes=[dma((4,)), dma],
            compiler_params=pltpu.CompilerParams(vmem_limit_bytes=VMEM_LIMIT),
        )(*(kept(x) for x in results))
        seg_pen, seg_face, seg_gap = (x.reshape(SEG_DEV) for x in (seg_pen, seg_face, seg_gap))
        return force, seg_pen, seg_face, seg_gap, mean.reshape(())

    rows_spec, wide_spec = P(("dom", "rep")), P(None, ("dom", "rep"))
    return jax.shard_map(
        shards,
        mesh=mesh,
        in_specs=(P(), P(), wide_spec, wide_spec, rows_spec, P()) + (rows_spec,) * 5,
        out_specs=(wide_spec, P("dom"), P("dom"), P("dom"), P()),
        check_vma=False,
    )
```

```python
import functools

import jax
import jax.numpy as jnp
from jax import lax
from jax.experimental import pallas as pl
from jax.experimental.pallas import tpu as pltpu
from jax.sharding import PartitionSpec as P

SEG_DEV = 1024
SPILL = 256
LANES = 128
SUB = 8
WIDTH = 64
PER_ROW = LANES // WIDTH
GROUPS = (SEG_DEV + SPILL) // WIDTH
OWN_GROUPS = SEG_DEV // WIDTH
SPILL_GROUPS = SPILL // WIDTH
OWN_ROWS = SEG_DEV // LANES
SPILL_ROWS = SPILL // LANES
ALL_ROWS = 16
CODE = 32

PENALTY = 400.0
LOWEST_FILL = -1e30
FACE_LIMIT = 1073741824
FACE_MASK = FACE_LIMIT - 1
KEY_LOW = -2147483648
LOGICAL = pl.DeviceIdType.LOGICAL
TILE = 256
DEPTH = 12
BATCH = 4
OWN_BATCHES = OWN_GROUPS // BATCH
UNROLL = 16
CHAINS = 4
FORCE_UNROLL = 8
LOOP_UNROLL = 4
EXTRA = 16
VMEM_LIMIT = 32 << 20


def split3(x):
    a = x.astype(jnp.bfloat16)
    rest = x - a.astype(jnp.float32)
    b = rest.astype(jnp.bfloat16)
    c = (rest - b.astype(jnp.float32)).astype(jnp.bfloat16)
    return a, b, c


def row(ref, at):
    return ref[pl.ds(at, SUB, stride=0), :]


def pull_groups(first, count, depth0, depth, code_ref, sources, packs):
    all_lines = code_ref.shape[0]
    sub = lax.broadcasted_iota(jnp.int32, (SUB, LANES), 0)
    blocks = -(-count * depth // SUB)
    wants = []
    for b in range(blocks):
        line = sub + SUB * b
        want = jnp.full((SUB, LANES), -2, jnp.int32)
        for q in range(count):
            inside = (line >= q * depth) & (line < (q + 1) * depth)
            want = jnp.where(inside, (line + (depth0 - q * depth)) * CODE + (first + q), want)
        wants.append(want)
    fills = (-1, LOWEST_FILL, -1, 0.0)

    def pull(i, carry):
        parts = [list(part) for part in carry]
        code = row(code_ref, i)
        values = [row(ref, i) for ref in sources]
        for b in range(blocks):
            hit = code == wants[b]
            for part, value in zip(parts, values):
                part[b] = jnp.where(hit, value, part[b])
        return tuple(tuple(part) for part in parts)

    start = tuple(
        (jnp.full((SUB, LANES), fill, ref.dtype),) * blocks for fill, ref in zip(fills, sources)
    )
    pulled = lax.fori_loop(0, all_lines, pull, start, unroll=8)
    for ref, parts in zip(packs, pulled):
        for b in range(blocks):
            ref[SUB * b : SUB * (b + 1), :] = parts[b]


def match_group(g, at, depth, packs, unroll):
    sub = lax.broadcasted_iota(jnp.int32, (SUB, LANES), 0)
    tiles = WIDTH // SUB
    marks = [sub + (g * WIDTH + SUB * q) for q in range(tiles)]
    start = (
        (jnp.full((SUB, LANES), LOWEST_FILL, jnp.float32),) * tiles,
        (jnp.full((SUB, LANES), KEY_LOW, jnp.int32),) * tiles,
        (jnp.zeros((SUB, LANES), jnp.float32),) * tiles,
    )

    def one(j, carry):
        pens, keys, gaps = (list(part) for part in carry)
        slot, pen, key, gap = (row(ref, at + j) for ref in packs)
        for q in range(tiles):
            hit = slot == marks[q]
            pens[q] = jnp.maximum(pens[q], jnp.where(hit, pen, LOWEST_FILL))
            keys[q] = jnp.maximum(keys[q], jnp.where(hit, key, KEY_LOW))
            gaps[q] = gaps[q] + jnp.where(hit, gap, 0.0)
        return tuple(pens), tuple(keys), tuple(gaps)

    if unroll == depth:
        for j in range(depth):
            start = one(j, start)
        return start
    return lax.fori_loop(0, depth, one, start, unroll=unroll)


def keep_group(accs, side, parts):
    for ref, part in zip(accs, parts):
        for q in range(WIDTH // SUB):
            at = side * WIDTH + q * SUB
            ref[at : at + SUB, :] = part[q]


def across(accs):
    pens, keys, gaps = (ref[...].T for ref in accs)
    return (
        jnp.max(pens, axis=0, keepdims=True),
        jnp.max(keys, axis=0, keepdims=True),
        jnp.sum(gaps, axis=0, keepdims=True),
    )


def project(wt, x_ref, off_ref, tile):
    cols = pl.ds(tile * TILE, TILE)
    per_tile = TILE // LANES
    offset = jnp.concatenate([row(off_ref, tile * per_tile + i) for i in range(per_tile)], axis=1)
    sub = lax.broadcasted_iota(jnp.int32, (SUB, TILE), 0)
    a, b, c = (part.astype(jnp.float32) for part in split3(offset))
    extra = jnp.where(sub == 0, a, jnp.where(sub == 1, b, jnp.where(sub == 2, c, 0.0)))
    extra = jnp.concatenate([extra, jnp.zeros((EXTRA - SUB, TILE), jnp.float32)], axis=0)
    x = jnp.concatenate([x_ref[:, cols], extra.astype(jnp.bfloat16)], axis=0)
    return jnp.dot(wt, x, preferred_element_type=jnp.float32)


def store_row(ref, tile, value):
    per_tile = TILE // LANES
    for i in range(per_tile):
        ref[pl.ds(tile * per_tile + i, 1), :] = value[:, i * LANES : (i + 1) * LANES]


def reduce_field(field, p_size, tile, pen_ref, gap_ref):
    low = [field[SUB * j : SUB * (j + 1)] for j in range(CHAINS)]
    for j in range(CHAINS, p_size // SUB):
        low[j % CHAINS] = jnp.minimum(low[j % CHAINS], field[SUB * j : SUB * (j + 1)])
    store_row(pen_ref, tile, -jnp.min(functools.reduce(jnp.minimum, low), axis=0, keepdims=True))
    store_row(gap_ref, tile, jnp.sum(field[p_size : p_size + SUB], axis=0, keepdims=True))


def prep_kernel(
    live_h, ns_h, nm_h, qw_h, sec_h, mst_h, off_h, jac_h, slot_h, face_h, rank_h,
    x_ref, wt_ref, nq_ref, off_ref, jl_ref, slot_ref, code_ref, key_ref, over_pen, over_key, over_gap, area_ref,
    live_s, ns_ref, nm_ref, qw_ref, jac_ref, face_ref, rank_ref, pen_ref, gap_ref, packs, accs, s_small, s_big,
):
    lines = slot_ref.shape[0]
    k_size, p_size = ns_ref.shape
    rows = x_ref.shape[1]

    small = [
        pltpu.make_async_copy(source, held, s_small.at[i])
        for i, (source, held) in enumerate((
            (slot_h, slot_ref), (live_h, live_s), (ns_h, ns_ref), (nm_h, nm_ref), (qw_h, qw_ref),
            (face_h, face_ref), (rank_h, rank_ref), (jac_h, jac_ref), (off_h, off_ref),
        ))
    ]
    for copy in small:
        copy.start()
    for base, source in ((0, sec_h), (k_size, mst_h)):
        for at in range(0, k_size, 2 * SUB):
            pltpu.make_async_copy(
                source.at[at : at + 2 * SUB, :], x_ref.at[base + at : base + at + 2 * SUB, :], s_big
            ).start(priority=1)
    for copy in small:
        copy.wait()

    row_id = (
        lax.broadcasted_iota(jnp.int32, (lines, LANES), 0) * LANES
        + lax.broadcasted_iota(jnp.int32, (lines, LANES), 1)
    )
    alive = row_id < live_s[...]
    group = jnp.where(alive, slot_ref[...] // WIDTH, -1)
    before = (
        lax.broadcasted_iota(jnp.int32, (lines, lines), 1)
        < lax.broadcasted_iota(jnp.int32, (lines, lines), 0)
    )
    before = jnp.where(before, 1.0, 0.0).astype(jnp.bfloat16)
    place = jnp.zeros((lines, LANES), jnp.float32)
    for g in range(0, GROUPS, 2):
        mine = [group == g, group == g + 1]
        seen = jnp.concatenate([jnp.where(m, 1.0, 0.0).astype(jnp.bfloat16) for m in mine], axis=1)
        found = jnp.dot(before, seen, preferred_element_type=jnp.float32)
        place = jnp.where(mine[0], found[:, :LANES], jnp.where(mine[1], found[:, LANES:], place))
    code = jnp.where(alive, place.astype(jnp.int32) * CODE + group, -1)
    code_ref[...] = code
    worst = jnp.max(code)

    w = jnp.concatenate([ns_ref[...], -nm_ref[...]], axis=0).astype(jnp.float32)
    qrow = qw_ref[...]
    wt = w.T
    qmat = jnp.broadcast_to(qrow, (LANES, p_size)).T
    v = jnp.sum(wt * qmat, axis=0, keepdims=True)
    qsum = jnp.sum(qmat, axis=0, keepdims=True)
    depth = wt_ref.shape[1]
    pick = lax.broadcasted_iota(jnp.int32, (EXTRA, depth), 0)
    column = lax.broadcasted_iota(jnp.int32, (p_size, depth - 2 * k_size), 1)
    wt_ref[0:p_size, 0 : 2 * k_size] = wt.astype(jnp.bfloat16)
    wt_ref[0:p_size, 2 * k_size :] = jnp.where(column < 3, 1.0, 0.0).astype(jnp.bfloat16)
    lane_row = lax.broadcasted_iota(jnp.int32, (1, LANES), 1)
    tail = jnp.where(lane_row < 3, qsum, 0.0)[:, : depth - 2 * k_size]
    a, b, c = (part.astype(jnp.float32) for part in split3(jnp.concatenate([v, tail], axis=1)))
    stacked = jnp.where(pick == 0, a, jnp.where(pick == 1, b, jnp.where(pick == 2, c, 0.0)))
    wt_ref[p_size:, :] = stacked.astype(jnp.bfloat16)
    scaled = ns_ref[...].astype(jnp.float32) * qrow
    top = scaled.astype(jnp.bfloat16)
    low = (scaled - top.astype(jnp.float32)).astype(jnp.bfloat16)
    nq_ref[...] = jnp.concatenate([top, low], axis=0)

    key_ref[...] = ((rank_ref[...] - 2) << 30) + (FACE_MASK - face_ref[...])
    jl = jnp.where(alive, jac_ref[...], 0.0)
    jl_ref[...] = jl
    area_ref[...] = jnp.sum(jl, axis=0, keepdims=True) * jnp.sum(qrow, axis=1, keepdims=True)
    over_pen[...] = jnp.full(over_pen.shape, LOWEST_FILL, jnp.float32)
    over_key[...] = jnp.full(over_key.shape, KEY_LOW, jnp.int32)
    over_gap[...] = jnp.zeros(over_gap.shape, jnp.float32)

    pltpu.make_async_copy(x_ref, x_ref, s_big).wait()

    @pl.when(worst >= DEPTH * CODE)
    def _():
        weights = wt_ref[...]
        work = face_ref
        line_id = lax.broadcasted_iota(jnp.int32, (lines, LANES), 0)
        work[...] = jnp.where(code >= DEPTH * CODE, line_id * CODE + (code & (CODE - 1)), -1)

        def one(mark):
            line, g = mark // CODE, mark & (CODE - 1)
            tile = line // (TILE // LANES)
            reduce_field(project(weights, x_ref, off_ref, tile), p_size, tile, pen_ref, gap_ref)
            here = row(work, line) == mark
            values = (
                row(slot_ref, line), row(pen_ref, line), row(key_ref, line), row(gap_ref, line) * row(jl_ref, line)
            )
            for ref, value in zip(packs, values):
                ref[0:SUB, :] = jnp.where(here, value, -1) if ref is packs[0] else value
            found = match_group(g, 0, 1, packs, 1)
            odd = jnp.full((SUB, LANES), g & 1, jnp.int32)
            for side in range(PER_ROW):
                keep_group(accs, side, [
                    [jnp.where(odd == side, x, fill) for x in part]
                    for part, fill in zip(found, (LOWEST_FILL, KEY_LOW, 0.0))
                ])
            pen, key, gap = across(accs)
            at = pl.ds(g // PER_ROW, 1)
            over_pen[at, :] = jnp.maximum(over_pen[at, :], pen)
            over_key[at, :] = jnp.maximum(over_key[at, :], key)
            over_gap[at, :] = over_gap[at, :] + gap
            left = jnp.where(work[...] == mark, -1, work[...])
            work[...] = left
            return jnp.max(left)

        lax.while_loop(lambda mark: mark >= 0, one, jnp.max(work[...]))


def main_kernel(
    n_dom, n_rep,
    x_ref, wt_ref, nq_ref, off_ref, jl_ref, slot_ref, code_ref, key_ref, over_pen, over_key, over_gap, area_ref,
    force_ref, out_pen, out_face, out_gap, out_mean,
    load_ref, pen_ref, gap_ref, packs, even_accs, odd_accs, raw_pen, raw_key, raw_gap,
    sp_sf, sp_si, ow_sf, ow_si, t1_s, t2_s, sp_f, sp_i, ow_f, ow_i, t1_d, t2_d,
    s_spf, r_spf, s_spi, r_spi, s_owf, r_owf, s_owi, r_owi, s_t1, r_t1, s_t2, r_t2, inside,
):
    dom = lax.axis_index("dom")
    rep = lax.axis_index("rep")
    k_size = force_ref.shape[0]
    rows = force_ref.shape[1]
    p_size = load_ref.shape[0]
    per_tile = TILE // LANES
    tiles = rows // TILE
    count = n_dom * n_rep
    me = dom * n_rep + rep

    def flat(d, r):
        return lax.rem(d + n_dom, n_dom) * n_rep + lax.rem(r + n_rep, n_rep)

    barrier = pltpu.get_barrier_semaphore()

    def signal(sem, first, last, step=1, at=0):
        def one(i, carry):
            pl.semaphore_signal(sem, inc=1, device_id=i * step + at, device_id_type=LOGICAL)
            return carry

        lax.fori_loop(first, last, one, 0)

    signal(barrier, me + 1, count)
    signal(barrier, dom * n_rep, me)
    signal(barrier, jnp.maximum(dom - 1, 0) * n_rep, dom * n_rep)

    wt = wt_ref[...]

    def wide_row(ref, tile):
        return jnp.concatenate([row(ref, tile * per_tile + i) for i in range(per_tile)], axis=1)

    last_dom = dom == n_dom - 1
    pairs = count // 2
    pair = lax.div(me, 2)
    odd = lax.rem(rep, 2)
    mate = rep + 1 - 2 * odd

    def enter():
        after = n_rep * jnp.where(last_dom, 0, 1)
        pl.semaphore_wait(barrier, me + (n_rep - 1 - rep) + after)
        signal(inside, 0, pair, 2, odd)

    def batch(step, carry):
        @pl.when(last_dom & (step == 1))
        def _():
            enter()

        for i in range(UNROLL):
            tile = step * UNROLL + i
            cols = pl.ds(tile * TILE, TILE)
            field = project(wt, x_ref, off_ref, tile)
            for at in range(0, p_size, 2 * SUB):
                load_ref[at : at + 2 * SUB, cols] = jnp.minimum(field[at : at + 2 * SUB].astype(jnp.bfloat16), 0)
            reduce_field(field, p_size, tile, pen_ref, gap_ref)
        return carry

    lax.fori_loop(0, tiles // UNROLL, batch, 0)
    row_gap = gap_ref[...] * jl_ref[...]
    gap_ref[...] = row_gap
    total_gap = jnp.sum(jnp.sum(row_gap, axis=0, keepdims=True), axis=1, keepdims=True)
    total_area = jnp.sum(area_ref[...], axis=1, keepdims=True)
    lane = lax.broadcasted_iota(jnp.int32, (1, LANES), 1)
    t1_s[...] = jnp.where(lane == 0, total_gap, jnp.where(lane == 1, total_area, 0.0))

    @pl.when(jnp.logical_not(last_dom))
    def _():
        enter()

    first_copy = pltpu.make_async_remote_copy(
        src_ref=t1_s, dst_ref=t1_d, send_sem=s_t1, recv_sem=r_t1,
        device_id=flat(dom, mate), device_id_type=LOGICAL,
    )
    first_copy.start()

    def pull_batch(first):
        pull_groups(first, BATCH, 0, DEPTH, code_ref, (slot_ref, pen_ref, key_ref, gap_ref), packs)

    def match_pair(first, i, accs, last_accs, over, at):
        g = first + i * PER_ROW
        keep_group(accs, 0, match_group(g, i * PER_ROW * DEPTH, DEPTH, packs, LOOP_UNROLL))
        if last_accs is not None:
            close_pair(last_accs, over, at)
        keep_group(accs, 1, match_group(g + 1, (i * PER_ROW + 1) * DEPTH, DEPTH, packs, DEPTH))

    def close_pair(accs, over, at):
        pen, key, gap = across(accs)
        over, at = pl.ds(over, 1), pl.ds(at, 1)
        raw_pen[at, :] = jnp.maximum(pen, over_pen[over, :])
        raw_key[at, :] = jnp.maximum(key, over_key[over, :])
        raw_gap[at, :] = gap + over_gap[over, :]

    def decode(top, best):
        none = top < LOWEST_FILL * 0.5
        rank = jnp.where(none, -1, (best >> 30) + 2)
        face = jnp.where(none, FACE_LIMIT, FACE_MASK - (best & FACE_MASK))
        return rank, face

    pull_batch(OWN_GROUPS)
    match_pair(OWN_GROUPS, 0, even_accs, None, 0, 0)
    match_pair(OWN_GROUPS, 1, odd_accs, even_accs, OWN_ROWS, 0)
    close_pair(odd_accs, OWN_ROWS + 1, 1)
    part = slice(0, SPILL_ROWS)
    rank, face = decode(raw_pen[part, :], raw_key[part, :])
    sp_sf[0:SPILL_ROWS, :] = raw_pen[part, :]
    sp_sf[SPILL_ROWS:, :] = raw_gap[part, :]
    sp_si[0:SPILL_ROWS, :] = rank
    sp_si[SPILL_ROWS:, :] = face

    def spill_copy(j):
        where = flat(dom + 1, rep + j)
        return (
            pltpu.make_async_remote_copy(
                src_ref=sp_sf, dst_ref=sp_f.at[rep], send_sem=s_spf, recv_sem=r_spf,
                device_id=where, device_id_type=LOGICAL,
            ),
            pltpu.make_async_remote_copy(
                src_ref=sp_si, dst_ref=sp_i.at[rep], send_sem=s_spi, recv_sem=r_spi,
                device_id=where, device_id_type=LOGICAL,
            ),
        )

    for j in range(n_rep):
        for copy in spill_copy(j):
            copy.start()

    first_copy.wait_recv()
    both = t1_s[...] + t1_d[...]
    t2_s[...] = both
    t2_d[pl.ds(pair, 1), :] = both

    def send_pairs(first, last):
        def one(other, carry):
            pltpu.make_async_remote_copy(
                src_ref=t2_s, dst_ref=t2_d.at[pl.ds(pair, 1), :], send_sem=s_t2, recv_sem=r_t2,
                device_id=other * 2 + odd, device_id_type=LOGICAL,
            ).start()
            return carry

        lax.fori_loop(first, last, one, 0)

    send_pairs(0, pair)

    def send_up():
        @pl.when(pair < pairs - 1)
        def _():
            pl.semaphore_wait(inside, pairs - 1 - pair)

        send_pairs(pair + 1, pairs)

    quarter = lax.div(me * 4, count)
    turn = OWN_BATCHES - quarter - jnp.where(quarter >= 2, 1, 0)

    def own_scan(i, carry):
        @pl.when(i == turn)
        def _():
            send_up()

        first = i * BATCH
        last = lax.rem(2 * i + OWN_ROWS - 1, OWN_ROWS)
        pull_batch(first)
        match_pair(first, 0, even_accs, odd_accs, last, last)
        match_pair(first, 1, odd_accs, even_accs, 2 * i, 2 * i)
        return carry

    lax.fori_loop(0, OWN_BATCHES, own_scan, 0)
    close_pair(odd_accs, OWN_ROWS - 1, OWN_ROWS - 1)
    rank, face = decode(raw_pen[...], raw_key[...])
    ow_sf[0] = raw_pen[...]
    ow_sf[1] = raw_gap[...]
    ow_si[0] = rank
    ow_si[1] = face

    def own_copy(j):
        where = flat(dom, rep + j)
        return (
            pltpu.make_async_remote_copy(
                src_ref=ow_sf, dst_ref=ow_f.at[rep], send_sem=s_owf, recv_sem=r_owf,
                device_id=where, device_id_type=LOGICAL,
            ),
            pltpu.make_async_remote_copy(
                src_ref=ow_si, dst_ref=ow_i.at[rep], send_sem=s_owi, recv_sem=r_owi,
                device_id=where, device_id_type=LOGICAL,
            ),
        )

    for j in range(1, n_rep):
        for copy in own_copy(j):
            copy.start()
    ow_f[rep] = ow_sf[...]
    ow_i[rep] = ow_si[...]

    @pl.when(turn >= OWN_BATCHES)
    def _():
        send_up()

    nq = nq_ref[...]

    def push(step, carry):
        for i in range(FORCE_UNROLL):
            tile = step * FORCE_UNROLL + i
            cols = pl.ds(tile * TILE, TILE)
            force = jnp.dot(nq, load_ref[:, cols], preferred_element_type=jnp.float32)
            scale = wide_row(jl_ref, tile)[0:1] * -PENALTY
            force_ref[:, cols] = ((force[:k_size] + force[k_size:]) * scale).astype(jnp.bfloat16)
        return carry

    lax.fori_loop(0, tiles // FORCE_UNROLL, push, 0)

    def encode(rank, face):
        return jnp.where(rank < 0, KEY_LOW, ((rank - 2) << 30) + (FACE_MASK - face))

    def settle(ref, sem):
        pltpu.make_async_copy(ref, ref, sem).wait()

    settle(ow_f.at[pl.ds(0, n_rep - 1)], r_owf)
    settle(ow_i.at[pl.ds(0, n_rep - 1)], r_owi)
    pen_o, gap_o = ow_f[0, 0], ow_f[0, 1]
    key_o = encode(ow_i[0, 0], ow_i[0, 1])
    for r in range(1, n_rep):
        pen_o = jnp.maximum(pen_o, ow_f[r, 0])
        gap_o = gap_o + ow_f[r, 1]
        key_o = jnp.maximum(key_o, encode(ow_i[r, 0], ow_i[r, 1]))

    settle(sp_f, s_spf)
    settle(sp_i, s_spi)
    settle(ow_f.at[pl.ds(0, n_rep - 1)], s_owf)
    settle(ow_i.at[pl.ds(0, n_rep - 1)], s_owi)
    first_copy.wait_send()
    settle(t2_d.at[pl.ds(0, pairs - 1), :], s_t2)

    settle(t2_d.at[pl.ds(0, pairs - 1), :], r_t2)
    settle(sp_f, r_spf)
    settle(sp_i, r_spi)
    whole = jnp.sum(t2_d[...], axis=0, keepdims=True)
    out_mean[...] = whole[:, 0:1] / whole[:, 1:2]

    g = SPILL_ROWS
    pen_s, gap_s = sp_f[0, 0:g], sp_f[0, g:]
    key_s = encode(sp_i[0, 0:g], sp_i[0, g:])
    for r in range(1, n_rep):
        pen_s = jnp.maximum(pen_s, sp_f[r, 0:g])
        gap_s = gap_s + sp_f[r, g:]
        key_s = jnp.maximum(key_s, encode(sp_i[r, 0:g], sp_i[r, g:]))

    def finish(at, pen, key, gap):
        none = pen < LOWEST_FILL * 0.5
        out_pen[at, :] = jnp.where(none, 0.0, pen)
        out_face[at, :] = jnp.where(none, -1, FACE_MASK - (key & FACE_MASK))
        out_gap[at, :] = jnp.where(none, 0.0, gap)

    finish(
        slice(0, g), jnp.maximum(pen_o[:g], pen_s), jnp.maximum(key_o[:g], key_s), gap_o[:g] + gap_s
    )
    finish(slice(g, OWN_ROWS), pen_o[g:], key_o[g:], gap_o[g:])


def finish_kernel(force_ref, pen_ref, face_ref, gap_ref, mean_ref, force_h, pen_h, face_h, gap_h, mean_h, sems, s_force):
    copies = [
        pltpu.make_async_copy(held, out, sems.at[i])
        for i, (held, out) in enumerate((
            (pen_ref, pen_h), (face_ref, face_h), (gap_ref, gap_h), (mean_ref, mean_h)
        ))
    ]
    for at in range(0, force_ref.shape[0], SUB):
        part = (slice(at, at + SUB), slice(None))
        pltpu.make_async_copy(force_ref.at[part], force_h.at[part], s_force).start()
    for copy in copies:
        copy.start()
    for copy in copies:
        copy.wait()
    pltpu.make_async_copy(force_ref, force_h, s_force).wait()


def solution(mesh):
    n_dom, n_rep = mesh.shape["dom"], mesh.shape["rep"]
    vmem = pl.BlockSpec(memory_space=pltpu.VMEM)
    anywhere = pl.BlockSpec(memory_space=pl.ANY)
    dma = pltpu.SemaphoreType.DMA

    def kept(x):
        return pltpu.with_memory_space_constraint(x, pltpu.VMEM)

    def streamed(x):
        return pltpu.with_memory_space_constraint(x, pltpu.HBM)

    def shards(ns, nm, sec, mst, off, qw, jac, slot, face, rank, live):
        k_size, p_size = ns.shape
        rows = sec.shape[1]
        lines = rows // LANES
        depth = 2 * k_size + EXTRA
        f32, i32, bf16 = jnp.float32, jnp.int32, jnp.bfloat16

        off, jac, slot, face, rank = (x.reshape(lines, LANES) for x in (off, jac, slot, face, rank))

        def packs(deep):
            return [pltpu.VMEM((deep + SUB, LANES), t) for t in (i32, f32, i32, f32)]

        def lanes():
            return [pltpu.VMEM((LANES, LANES), t) for t in (f32, i32, f32)]

        held = pl.pallas_call(
            prep_kernel,
            out_shape=(
                pltpu.VMEM((2 * k_size, rows), bf16),
                pltpu.VMEM((p_size + EXTRA, depth), bf16),
                pltpu.VMEM((2 * k_size, p_size), bf16),
                pltpu.VMEM((lines, LANES), f32),
                pltpu.VMEM((lines, LANES), f32),
                pltpu.VMEM((lines, LANES), i32),
                pltpu.VMEM((lines, LANES), i32),
                pltpu.VMEM((lines, LANES), i32),
                pltpu.VMEM((ALL_ROWS, LANES), f32),
                pltpu.VMEM((ALL_ROWS, LANES), i32),
                pltpu.VMEM((ALL_ROWS, LANES), f32),
                pltpu.VMEM((1, LANES), f32),
            ),
            in_specs=[anywhere] * 11,
            out_specs=(vmem,) * 12,
            scratch_shapes=[
                pltpu.VMEM((1, 1), i32),
                pltpu.VMEM((k_size, p_size), bf16),
                pltpu.VMEM((k_size, p_size), bf16),
                pltpu.VMEM((1, p_size), f32),
                pltpu.VMEM((lines, LANES), f32),
                pltpu.VMEM((lines, LANES), i32),
                pltpu.VMEM((lines, LANES), i32),
                pltpu.VMEM((lines, LANES), f32),
                pltpu.VMEM((lines, LANES), f32),
                packs(SUB),
                lanes(),
                dma((9,)),
                dma,
            ],
            compiler_params=pltpu.CompilerParams(vmem_limit_bytes=VMEM_LIMIT),
        )(
            live.reshape(1, 1),
            *(streamed(x) for x in (ns, nm, qw.reshape(1, p_size), sec, mst, off, jac, slot, face, rank)),
        )

        spill = (2 * SPILL_ROWS, LANES)
        own = (2, OWN_ROWS, LANES)
        pairs = n_dom * n_rep // 2
        results = pl.pallas_call(
            functools.partial(main_kernel, n_dom, n_rep),
            out_shape=(
                pltpu.VMEM((k_size, rows), bf16),
                pltpu.VMEM((OWN_ROWS, LANES), f32),
                pltpu.VMEM((OWN_ROWS, LANES), i32),
                pltpu.VMEM((OWN_ROWS, LANES), f32),
                pltpu.VMEM((1, 1), f32),
            ),
            in_specs=[vmem] * 12,
            out_specs=(vmem,) * 5,
            scratch_shapes=[
                pltpu.VMEM((p_size, rows), bf16),
                pltpu.VMEM((lines, LANES), f32),
                pltpu.VMEM((lines, LANES), f32),
                packs(BATCH * DEPTH),
                lanes(),
                lanes(),
                pltpu.VMEM((OWN_ROWS, LANES), f32),
                pltpu.VMEM((OWN_ROWS, LANES), i32),
                pltpu.VMEM((OWN_ROWS, LANES), f32),
                pltpu.VMEM(spill, f32),
                pltpu.VMEM(spill, i32),
                pltpu.VMEM(own, f32),
                pltpu.VMEM(own, i32),
                pltpu.VMEM((1, LANES), f32),
                pltpu.VMEM((1, LANES), f32),
                pltpu.VMEM((n_rep,) + spill, f32),
                pltpu.VMEM((n_rep,) + spill, i32),
                pltpu.VMEM((n_rep,) + own, f32),
                pltpu.VMEM((n_rep,) + own, i32),
                pltpu.VMEM((1, LANES), f32),
                pltpu.VMEM((pairs, LANES), f32),
            ] + [dma] * 12 + [pltpu.SemaphoreType.REGULAR],
            compiler_params=pltpu.CompilerParams(
                collective_id=0, has_side_effects=True, vmem_limit_bytes=VMEM_LIMIT
            ),
        )(*(kept(x) for x in held))

        force, seg_pen, seg_face, seg_gap, mean = pl.pallas_call(
            finish_kernel,
            out_shape=tuple(jax.ShapeDtypeStruct(x.shape, x.dtype) for x in results),
            in_specs=[vmem] * 5,
            out_specs=(anywhere,) * 5,
            scratch_shapes=[dma((4,)), dma],
            compiler_params=pltpu.CompilerParams(vmem_limit_bytes=VMEM_LIMIT),
        )(*(kept(x) for x in results))
        seg_pen, seg_face, seg_gap = (x.reshape(SEG_DEV) for x in (seg_pen, seg_face, seg_gap))
        return force, seg_pen, seg_face, seg_gap, mean.reshape(())

    rows_spec, wide_spec = P(("dom", "rep")), P(None, ("dom", "rep"))
    return jax.shard_map(
        shards,
        mesh=mesh,
        in_specs=(P(), P(), wide_spec, wide_spec, rows_spec, P()) + (rows_spec,) * 5,
        out_specs=(wide_spec, P("dom"), P("dom"), P("dom"), P()),
        check_vma=False,
    )
```

```python
import functools

import jax
import jax.numpy as jnp
from jax import lax
from jax.experimental import pallas as pl
from jax.experimental.pallas import tpu as pltpu
from jax.sharding import PartitionSpec as P

SEG_DEV = 1024
SPILL = 256
LANES = 128
SUB = 8
WIDTH = 64
PER_ROW = LANES // WIDTH
GROUPS = (SEG_DEV + SPILL) // WIDTH
OWN_GROUPS = SEG_DEV // WIDTH
SPILL_GROUPS = SPILL // WIDTH
OWN_ROWS = SEG_DEV // LANES
SPILL_ROWS = SPILL // LANES
ALL_ROWS = 16
CODE = 32

PENALTY = 400.0
LOWEST_FILL = -1e30
FACE_LIMIT = 1073741824
FACE_MASK = FACE_LIMIT - 1
KEY_LOW = -2147483648
LOGICAL = pl.DeviceIdType.LOGICAL
TILE = 256
DEPTH = 12
BATCH = 4
OWN_BATCHES = OWN_GROUPS // BATCH
UNROLL = 32
CHAINS = 4
FORCE_UNROLL = 8
LOOP_UNROLL = 4
EXTRA = 16
VMEM_LIMIT = 32 << 20


def split3(x):
    a = x.astype(jnp.bfloat16)
    rest = x - a.astype(jnp.float32)
    b = rest.astype(jnp.bfloat16)
    c = (rest - b.astype(jnp.float32)).astype(jnp.bfloat16)
    return a, b, c


def row(ref, at):
    return ref[pl.ds(at, SUB, stride=0), :]


def pull_groups(first, count, depth0, depth, code_ref, sources, packs):
    all_lines = code_ref.shape[0]
    sub = lax.broadcasted_iota(jnp.int32, (SUB, LANES), 0)
    blocks = -(-count * depth // SUB)
    wants = []
    for b in range(blocks):
        line = sub + SUB * b
        want = jnp.full((SUB, LANES), -2, jnp.int32)
        for q in range(count):
            inside = (line >= q * depth) & (line < (q + 1) * depth)
            want = jnp.where(inside, (line + (depth0 - q * depth)) * CODE + (first + q), want)
        wants.append(want)
    fills = (-1, LOWEST_FILL, -1, 0.0)

    def pull(i, carry):
        parts = [list(part) for part in carry]
        code = row(code_ref, i)
        values = [row(ref, i) for ref in sources]
        for b in range(blocks):
            hit = code == wants[b]
            for part, value in zip(parts, values):
                part[b] = jnp.where(hit, value, part[b])
        return tuple(tuple(part) for part in parts)

    start = tuple(
        (jnp.full((SUB, LANES), fill, ref.dtype),) * blocks for fill, ref in zip(fills, sources)
    )
    pulled = lax.fori_loop(0, all_lines, pull, start, unroll=8)
    for ref, parts in zip(packs, pulled):
        for b in range(blocks):
            ref[SUB * b : SUB * (b + 1), :] = parts[b]


def match_group(g, at, depth, packs, unroll):
    sub = lax.broadcasted_iota(jnp.int32, (SUB, LANES), 0)
    tiles = WIDTH // SUB
    marks = [sub + (g * WIDTH + SUB * q) for q in range(tiles)]
    start = (
        (jnp.full((SUB, LANES), LOWEST_FILL, jnp.float32),) * tiles,
        (jnp.full((SUB, LANES), KEY_LOW, jnp.int32),) * tiles,
        (jnp.zeros((SUB, LANES), jnp.float32),) * tiles,
    )

    def one(j, carry):
        pens, keys, gaps = (list(part) for part in carry)
        slot, pen, key, gap = (row(ref, at + j) for ref in packs)
        for q in range(tiles):
            hit = slot == marks[q]
            pens[q] = jnp.maximum(pens[q], jnp.where(hit, pen, LOWEST_FILL))
            keys[q] = jnp.maximum(keys[q], jnp.where(hit, key, KEY_LOW))
            gaps[q] = gaps[q] + jnp.where(hit, gap, 0.0)
        return tuple(pens), tuple(keys), tuple(gaps)

    if unroll == depth:
        for j in range(depth):
            start = one(j, start)
        return start
    return lax.fori_loop(0, depth, one, start, unroll=unroll)


def keep_group(accs, side, parts):
    for ref, part in zip(accs, parts):
        for q in range(WIDTH // SUB):
            at = side * WIDTH + q * SUB
            ref[at : at + SUB, :] = part[q]


def across(accs):
    pens, keys, gaps = (ref[...].T for ref in accs)
    return (
        jnp.max(pens, axis=0, keepdims=True),
        jnp.max(keys, axis=0, keepdims=True),
        jnp.sum(gaps, axis=0, keepdims=True),
    )


def project(wt, x_ref, off_ref, tile):
    cols = pl.ds(tile * TILE, TILE)
    per_tile = TILE // LANES
    offset = jnp.concatenate([row(off_ref, tile * per_tile + i) for i in range(per_tile)], axis=1)
    sub = lax.broadcasted_iota(jnp.int32, (SUB, TILE), 0)
    a, b, c = (part.astype(jnp.float32) for part in split3(offset))
    extra = jnp.where(sub == 0, a, jnp.where(sub == 1, b, jnp.where(sub == 2, c, 0.0)))
    extra = jnp.concatenate([extra, jnp.zeros((EXTRA - SUB, TILE), jnp.float32)], axis=0)
    x = jnp.concatenate([x_ref[:, cols], extra.astype(jnp.bfloat16)], axis=0)
    return jnp.dot(wt, x, preferred_element_type=jnp.float32)


def store_row(ref, tile, value):
    per_tile = TILE // LANES
    for i in range(per_tile):
        ref[pl.ds(tile * per_tile + i, 1), :] = value[:, i * LANES : (i + 1) * LANES]


def reduce_field(field, p_size, tile, pen_ref, gap_ref):
    low = [field[SUB * j : SUB * (j + 1)] for j in range(CHAINS)]
    for j in range(CHAINS, p_size // SUB):
        low[j % CHAINS] = jnp.minimum(low[j % CHAINS], field[SUB * j : SUB * (j + 1)])
    store_row(pen_ref, tile, -jnp.min(functools.reduce(jnp.minimum, low), axis=0, keepdims=True))
    store_row(gap_ref, tile, jnp.sum(field[p_size : p_size + SUB], axis=0, keepdims=True))


def prep_kernel(
    live_h, ns_h, nm_h, qw_h, sec_h, mst_h, off_h, jac_h, slot_h, face_h, rank_h,
    x_ref, wt_ref, nq_ref, off_ref, jl_ref, slot_ref, code_ref, key_ref, over_pen, over_key, over_gap, area_ref,
    live_s, ns_ref, nm_ref, qw_ref, jac_ref, face_ref, rank_ref, pen_ref, gap_ref, packs, accs, s_small, s_big,
):
    lines = slot_ref.shape[0]
    k_size, p_size = ns_ref.shape
    rows = x_ref.shape[1]

    small = [
        pltpu.make_async_copy(source, held, s_small.at[i])
        for i, (source, held) in enumerate((
            (slot_h, slot_ref), (live_h, live_s), (ns_h, ns_ref), (nm_h, nm_ref), (qw_h, qw_ref),
            (face_h, face_ref), (rank_h, rank_ref), (jac_h, jac_ref), (off_h, off_ref),
        ))
    ]
    for copy in small:
        copy.start()
    for base, source in ((0, sec_h), (k_size, mst_h)):
        for at in range(0, k_size, 2 * SUB):
            pltpu.make_async_copy(
                source.at[at : at + 2 * SUB, :], x_ref.at[base + at : base + at + 2 * SUB, :], s_big
            ).start(priority=1)
    for copy in small:
        copy.wait()

    row_id = (
        lax.broadcasted_iota(jnp.int32, (lines, LANES), 0) * LANES
        + lax.broadcasted_iota(jnp.int32, (lines, LANES), 1)
    )
    alive = row_id < live_s[...]
    group = jnp.where(alive, slot_ref[...] // WIDTH, -1)
    before = (
        lax.broadcasted_iota(jnp.int32, (lines, lines), 1)
        < lax.broadcasted_iota(jnp.int32, (lines, lines), 0)
    )
    before = jnp.where(before, 1.0, 0.0).astype(jnp.bfloat16)
    place = jnp.zeros((lines, LANES), jnp.float32)
    for g in range(0, GROUPS, 2):
        mine = [group == g, group == g + 1]
        seen = jnp.concatenate([jnp.where(m, 1.0, 0.0).astype(jnp.bfloat16) for m in mine], axis=1)
        found = jnp.dot(before, seen, preferred_element_type=jnp.float32)
        place = jnp.where(mine[0], found[:, :LANES], jnp.where(mine[1], found[:, LANES:], place))
    code = jnp.where(alive, place.astype(jnp.int32) * CODE + group, -1)
    code_ref[...] = code
    worst = jnp.max(code)

    w = jnp.concatenate([ns_ref[...], -nm_ref[...]], axis=0).astype(jnp.float32)
    qrow = qw_ref[...]
    wt = w.T
    qmat = jnp.broadcast_to(qrow, (LANES, p_size)).T
    v = jnp.sum(wt * qmat, axis=0, keepdims=True)
    qsum = jnp.sum(qmat, axis=0, keepdims=True)
    depth = wt_ref.shape[1]
    pick = lax.broadcasted_iota(jnp.int32, (EXTRA, depth), 0)
    column = lax.broadcasted_iota(jnp.int32, (p_size, depth - 2 * k_size), 1)
    wt_ref[0:p_size, 0 : 2 * k_size] = wt.astype(jnp.bfloat16)
    wt_ref[0:p_size, 2 * k_size :] = jnp.where(column < 3, 1.0, 0.0).astype(jnp.bfloat16)
    lane_row = lax.broadcasted_iota(jnp.int32, (1, LANES), 1)
    tail = jnp.where(lane_row < 3, qsum, 0.0)[:, : depth - 2 * k_size]
    a, b, c = (part.astype(jnp.float32) for part in split3(jnp.concatenate([v, tail], axis=1)))
    stacked = jnp.where(pick == 0, a, jnp.where(pick == 1, b, jnp.where(pick == 2, c, 0.0)))
    wt_ref[p_size:, :] = stacked.astype(jnp.bfloat16)
    scaled = ns_ref[...].astype(jnp.float32) * qrow
    top = scaled.astype(jnp.bfloat16)
    low = (scaled - top.astype(jnp.float32)).astype(jnp.bfloat16)
    nq_ref[...] = jnp.concatenate([top, low], axis=0)

    key_ref[...] = ((rank_ref[...] - 2) << 30) + (FACE_MASK - face_ref[...])
    jl = jnp.where(alive, jac_ref[...], 0.0)
    jl_ref[...] = jl
    area_ref[...] = jnp.sum(jl, axis=0, keepdims=True) * jnp.sum(qrow, axis=1, keepdims=True)
    over_pen[...] = jnp.full(over_pen.shape, LOWEST_FILL, jnp.float32)
    over_key[...] = jnp.full(over_key.shape, KEY_LOW, jnp.int32)
    over_gap[...] = jnp.zeros(over_gap.shape, jnp.float32)

    pltpu.make_async_copy(x_ref, x_ref, s_big).wait()

    @pl.when(worst >= DEPTH * CODE)
    def _():
        weights = wt_ref[...]
        work = face_ref
        line_id = lax.broadcasted_iota(jnp.int32, (lines, LANES), 0)
        work[...] = jnp.where(code >= DEPTH * CODE, line_id * CODE + (code & (CODE - 1)), -1)

        def one(mark):
            line, g = mark // CODE, mark & (CODE - 1)
            tile = line // (TILE // LANES)
            reduce_field(project(weights, x_ref, off_ref, tile), p_size, tile, pen_ref, gap_ref)
            here = row(work, line) == mark
            values = (
                row(slot_ref, line), row(pen_ref, line), row(key_ref, line), row(gap_ref, line) * row(jl_ref, line)
            )
            for ref, value in zip(packs, values):
                ref[0:SUB, :] = jnp.where(here, value, -1) if ref is packs[0] else value
            found = match_group(g, 0, 1, packs, 1)
            odd = jnp.full((SUB, LANES), g & 1, jnp.int32)
            for side in range(PER_ROW):
                keep_group(accs, side, [
                    [jnp.where(odd == side, x, fill) for x in part]
                    for part, fill in zip(found, (LOWEST_FILL, KEY_LOW, 0.0))
                ])
            pen, key, gap = across(accs)
            at = pl.ds(g // PER_ROW, 1)
            over_pen[at, :] = jnp.maximum(over_pen[at, :], pen)
            over_key[at, :] = jnp.maximum(over_key[at, :], key)
            over_gap[at, :] = over_gap[at, :] + gap
            left = jnp.where(work[...] == mark, -1, work[...])
            work[...] = left
            return jnp.max(left)

        lax.while_loop(lambda mark: mark >= 0, one, jnp.max(work[...]))


def main_kernel(
    n_dom, n_rep,
    x_ref, wt_ref, nq_ref, off_ref, jl_ref, slot_ref, code_ref, key_ref, over_pen, over_key, over_gap, area_ref,
    force_ref, out_pen, out_face, out_gap, out_mean,
    load_ref, pen_ref, gap_ref, packs, even_accs, odd_accs, raw_pen, raw_key, raw_gap,
    sp_sf, sp_si, ow_sf, ow_si, t1_s, t2_s, sp_f, sp_i, ow_f, ow_i, t1_d, t2_d,
    s_spf, r_spf, s_spi, r_spi, s_owf, r_owf, s_owi, r_owi, s_t1, r_t1, s_t2, r_t2, inside,
):
    dom = lax.axis_index("dom")
    rep = lax.axis_index("rep")
    k_size = force_ref.shape[0]
    rows = force_ref.shape[1]
    p_size = load_ref.shape[0]
    per_tile = TILE // LANES
    tiles = rows // TILE
    count = n_dom * n_rep
    me = dom * n_rep + rep

    def flat(d, r):
        return lax.rem(d + n_dom, n_dom) * n_rep + lax.rem(r + n_rep, n_rep)

    barrier = pltpu.get_barrier_semaphore()

    def signal(sem, first, last, step=1, at=0):
        def one(i, carry):
            pl.semaphore_signal(sem, inc=1, device_id=i * step + at, device_id_type=LOGICAL)
            return carry

        lax.fori_loop(first, last, one, 0)

    signal(barrier, me + 1, count)
    signal(barrier, dom * n_rep, me)
    signal(barrier, jnp.maximum(dom - 1, 0) * n_rep, dom * n_rep)

    wt = wt_ref[...]

    def wide_row(ref, tile):
        return jnp.concatenate([row(ref, tile * per_tile + i) for i in range(per_tile)], axis=1)

    pairs = count // 2
    pair = lax.div(me, 2)
    odd = lax.rem(rep, 2)
    mate = rep + 1 - 2 * odd

    def batch(step, carry):
        for i in range(UNROLL):
            tile = step * UNROLL + i
            cols = pl.ds(tile * TILE, TILE)
            field = project(wt, x_ref, off_ref, tile)
            for at in range(0, p_size, 2 * SUB):
                load_ref[at : at + 2 * SUB, cols] = jnp.minimum(field[at : at + 2 * SUB].astype(jnp.bfloat16), 0)
            reduce_field(field, p_size, tile, pen_ref, gap_ref)
        return carry

    lax.fori_loop(0, tiles // UNROLL, batch, 0)
    row_gap = gap_ref[...] * jl_ref[...]
    gap_ref[...] = row_gap
    total_gap = jnp.sum(jnp.sum(row_gap, axis=0, keepdims=True), axis=1, keepdims=True)
    total_area = jnp.sum(area_ref[...], axis=1, keepdims=True)
    lane = lax.broadcasted_iota(jnp.int32, (1, LANES), 1)
    t1_s[...] = jnp.where(lane == 0, total_gap, jnp.where(lane == 1, total_area, 0.0))

    after = n_rep * jnp.where(dom == n_dom - 1, 0, 1)
    pl.semaphore_wait(barrier, me + (n_rep - 1 - rep) + after)
    first_copy = pltpu.make_async_remote_copy(
        src_ref=t1_s, dst_ref=t1_d, send_sem=s_t1, recv_sem=r_t1,
        device_id=flat(dom, mate), device_id_type=LOGICAL,
    )
    first_copy.start()
    signal(inside, 0, pair, 2, odd)

    def pull_batch(first):
        pull_groups(first, BATCH, 0, DEPTH, code_ref, (slot_ref, pen_ref, key_ref, gap_ref), packs)

    def match_pair(first, i, accs, last_accs, over, at):
        g = first + i * PER_ROW
        keep_group(accs, 0, match_group(g, i * PER_ROW * DEPTH, DEPTH, packs, LOOP_UNROLL))
        if last_accs is not None:
            close_pair(last_accs, over, at)
        keep_group(accs, 1, match_group(g + 1, (i * PER_ROW + 1) * DEPTH, DEPTH, packs, DEPTH))

    def close_pair(accs, over, at):
        pen, key, gap = across(accs)
        over, at = pl.ds(over, 1), pl.ds(at, 1)
        raw_pen[at, :] = jnp.maximum(pen, over_pen[over, :])
        raw_key[at, :] = jnp.maximum(key, over_key[over, :])
        raw_gap[at, :] = gap + over_gap[over, :]

    def decode(top, best):
        none = top < LOWEST_FILL * 0.5
        rank = jnp.where(none, -1, (best >> 30) + 2)
        face = jnp.where(none, FACE_LIMIT, FACE_MASK - (best & FACE_MASK))
        return rank, face

    pull_batch(OWN_GROUPS)
    match_pair(OWN_GROUPS, 0, even_accs, None, 0, 0)
    match_pair(OWN_GROUPS, 1, odd_accs, even_accs, OWN_ROWS, 0)
    close_pair(odd_accs, OWN_ROWS + 1, 1)
    part = slice(0, SPILL_ROWS)
    rank, face = decode(raw_pen[part, :], raw_key[part, :])
    sp_sf[0:SPILL_ROWS, :] = raw_pen[part, :]
    sp_sf[SPILL_ROWS:, :] = raw_gap[part, :]
    sp_si[0:SPILL_ROWS, :] = rank
    sp_si[SPILL_ROWS:, :] = face

    def spill_copy(j):
        where = flat(dom + 1, rep + j)
        return (
            pltpu.make_async_remote_copy(
                src_ref=sp_sf, dst_ref=sp_f.at[rep], send_sem=s_spf, recv_sem=r_spf,
                device_id=where, device_id_type=LOGICAL,
            ),
            pltpu.make_async_remote_copy(
                src_ref=sp_si, dst_ref=sp_i.at[rep], send_sem=s_spi, recv_sem=r_spi,
                device_id=where, device_id_type=LOGICAL,
            ),
        )

    for j in range(n_rep):
        for copy in spill_copy(j):
            copy.start()

    first_copy.wait_recv()
    both = t1_s[...] + t1_d[...]
    t2_s[...] = both
    t2_d[pl.ds(pair, 1), :] = both

    def send_pairs(first, last):
        def one(other, carry):
            pltpu.make_async_remote_copy(
                src_ref=t2_s, dst_ref=t2_d.at[pl.ds(pair, 1), :], send_sem=s_t2, recv_sem=r_t2,
                device_id=other * 2 + odd, device_id_type=LOGICAL,
            ).start()
            return carry

        lax.fori_loop(first, last, one, 0)

    send_pairs(0, pair)

    def send_up():
        @pl.when(pair < pairs - 1)
        def _():
            pl.semaphore_wait(inside, pairs - 1 - pair)

        send_pairs(pair + 1, pairs)

    quarter = lax.div(me * 4, count)
    turn = OWN_BATCHES - quarter - jnp.where(quarter >= 2, 1, 0)

    def own_scan(i, carry):
        @pl.when(i == turn)
        def _():
            send_up()

        first = i * BATCH
        last = lax.rem(2 * i + OWN_ROWS - 1, OWN_ROWS)
        pull_batch(first)
        match_pair(first, 0, even_accs, odd_accs, last, last)
        match_pair(first, 1, odd_accs, even_accs, 2 * i, 2 * i)
        return carry

    lax.fori_loop(0, OWN_BATCHES, own_scan, 0)
    close_pair(odd_accs, OWN_ROWS - 1, OWN_ROWS - 1)
    rank, face = decode(raw_pen[...], raw_key[...])
    ow_sf[0] = raw_pen[...]
    ow_sf[1] = raw_gap[...]
    ow_si[0] = rank
    ow_si[1] = face

    def own_copy(j):
        where = flat(dom, rep + j)
        return (
            pltpu.make_async_remote_copy(
                src_ref=ow_sf, dst_ref=ow_f.at[rep], send_sem=s_owf, recv_sem=r_owf,
                device_id=where, device_id_type=LOGICAL,
            ),
            pltpu.make_async_remote_copy(
                src_ref=ow_si, dst_ref=ow_i.at[rep], send_sem=s_owi, recv_sem=r_owi,
                device_id=where, device_id_type=LOGICAL,
            ),
        )

    for j in range(1, n_rep):
        for copy in own_copy(j):
            copy.start()
    ow_f[rep] = ow_sf[...]
    ow_i[rep] = ow_si[...]

    @pl.when(turn >= OWN_BATCHES)
    def _():
        send_up()

    nq = nq_ref[...]

    def push(step, carry):
        for i in range(FORCE_UNROLL):
            tile = step * FORCE_UNROLL + i
            cols = pl.ds(tile * TILE, TILE)
            force = jnp.dot(nq, load_ref[:, cols], preferred_element_type=jnp.float32)
            scale = wide_row(jl_ref, tile)[0:1] * -PENALTY
            force_ref[:, cols] = ((force[:k_size] + force[k_size:]) * scale).astype(jnp.bfloat16)
        return carry

    lax.fori_loop(0, tiles // FORCE_UNROLL, push, 0)

    def encode(rank, face):
        return jnp.where(rank < 0, KEY_LOW, ((rank - 2) << 30) + (FACE_MASK - face))

    def settle(ref, sem):
        pltpu.make_async_copy(ref, ref, sem).wait()

    settle(ow_f.at[pl.ds(0, n_rep - 1)], r_owf)
    settle(ow_i.at[pl.ds(0, n_rep - 1)], r_owi)
    pen_o, gap_o = ow_f[0, 0], ow_f[0, 1]
    key_o = encode(ow_i[0, 0], ow_i[0, 1])
    for r in range(1, n_rep):
        pen_o = jnp.maximum(pen_o, ow_f[r, 0])
        gap_o = gap_o + ow_f[r, 1]
        key_o = jnp.maximum(key_o, encode(ow_i[r, 0], ow_i[r, 1]))

    settle(sp_f, s_spf)
    settle(sp_i, s_spi)
    settle(ow_f.at[pl.ds(0, n_rep - 1)], s_owf)
    settle(ow_i.at[pl.ds(0, n_rep - 1)], s_owi)
    first_copy.wait_send()
    settle(t2_d.at[pl.ds(0, pairs - 1), :], s_t2)

    settle(t2_d.at[pl.ds(0, pairs - 1), :], r_t2)
    settle(sp_f, r_spf)
    settle(sp_i, r_spi)
    whole = jnp.sum(t2_d[...], axis=0, keepdims=True)
    out_mean[...] = whole[:, 0:1] / whole[:, 1:2]

    g = SPILL_ROWS
    pen_s, gap_s = sp_f[0, 0:g], sp_f[0, g:]
    key_s = encode(sp_i[0, 0:g], sp_i[0, g:])
    for r in range(1, n_rep):
        pen_s = jnp.maximum(pen_s, sp_f[r, 0:g])
        gap_s = gap_s + sp_f[r, g:]
        key_s = jnp.maximum(key_s, encode(sp_i[r, 0:g], sp_i[r, g:]))

    def finish(at, pen, key, gap):
        none = pen < LOWEST_FILL * 0.5
        out_pen[at, :] = jnp.where(none, 0.0, pen)
        out_face[at, :] = jnp.where(none, -1, FACE_MASK - (key & FACE_MASK))
        out_gap[at, :] = jnp.where(none, 0.0, gap)

    finish(
        slice(0, g), jnp.maximum(pen_o[:g], pen_s), jnp.maximum(key_o[:g], key_s), gap_o[:g] + gap_s
    )
    finish(slice(g, OWN_ROWS), pen_o[g:], key_o[g:], gap_o[g:])


def finish_kernel(force_ref, pen_ref, face_ref, gap_ref, mean_ref, force_h, pen_h, face_h, gap_h, mean_h, sems, s_force):
    copies = [
        pltpu.make_async_copy(held, out, sems.at[i])
        for i, (held, out) in enumerate((
            (pen_ref, pen_h), (face_ref, face_h), (gap_ref, gap_h), (mean_ref, mean_h)
        ))
    ]
    for at in range(0, force_ref.shape[0], SUB):
        part = (slice(at, at + SUB), slice(None))
        pltpu.make_async_copy(force_ref.at[part], force_h.at[part], s_force).start()
    for copy in copies:
        copy.start()
    for copy in copies:
        copy.wait()
    pltpu.make_async_copy(force_ref, force_h, s_force).wait()


def solution(mesh):
    n_dom, n_rep = mesh.shape["dom"], mesh.shape["rep"]
    vmem = pl.BlockSpec(memory_space=pltpu.VMEM)
    anywhere = pl.BlockSpec(memory_space=pl.ANY)
    dma = pltpu.SemaphoreType.DMA

    def kept(x):
        return pltpu.with_memory_space_constraint(x, pltpu.VMEM)

    def streamed(x):
        return pltpu.with_memory_space_constraint(x, pltpu.HBM)

    def shards(ns, nm, sec, mst, off, qw, jac, slot, face, rank, live):
        k_size, p_size = ns.shape
        rows = sec.shape[1]
        lines = rows // LANES
        depth = 2 * k_size + EXTRA
        f32, i32, bf16 = jnp.float32, jnp.int32, jnp.bfloat16

        off, jac, slot, face, rank = (x.reshape(lines, LANES) for x in (off, jac, slot, face, rank))

        def packs(deep):
            return [pltpu.VMEM((deep + SUB, LANES), t) for t in (i32, f32, i32, f32)]

        def lanes():
            return [pltpu.VMEM((LANES, LANES), t) for t in (f32, i32, f32)]

        held = pl.pallas_call(
            prep_kernel,
            out_shape=(
                pltpu.VMEM((2 * k_size, rows), bf16),
                pltpu.VMEM((p_size + EXTRA, depth), bf16),
                pltpu.VMEM((2 * k_size, p_size), bf16),
                pltpu.VMEM((lines, LANES), f32),
                pltpu.VMEM((lines, LANES), f32),
                pltpu.VMEM((lines, LANES), i32),
                pltpu.VMEM((lines, LANES), i32),
                pltpu.VMEM((lines, LANES), i32),
                pltpu.VMEM((ALL_ROWS, LANES), f32),
                pltpu.VMEM((ALL_ROWS, LANES), i32),
                pltpu.VMEM((ALL_ROWS, LANES), f32),
                pltpu.VMEM((1, LANES), f32),
            ),
            in_specs=[anywhere] * 11,
            out_specs=(vmem,) * 12,
            scratch_shapes=[
                pltpu.VMEM((1, 1), i32),
                pltpu.VMEM((k_size, p_size), bf16),
                pltpu.VMEM((k_size, p_size), bf16),
                pltpu.VMEM((1, p_size), f32),
                pltpu.VMEM((lines, LANES), f32),
                pltpu.VMEM((lines, LANES), i32),
                pltpu.VMEM((lines, LANES), i32),
                pltpu.VMEM((lines, LANES), f32),
                pltpu.VMEM((lines, LANES), f32),
                packs(SUB),
                lanes(),
                dma((9,)),
                dma,
            ],
            compiler_params=pltpu.CompilerParams(vmem_limit_bytes=VMEM_LIMIT),
        )(
            live.reshape(1, 1),
            *(streamed(x) for x in (ns, nm, qw.reshape(1, p_size), sec, mst, off, jac, slot, face, rank)),
        )

        spill = (2 * SPILL_ROWS, LANES)
        own = (2, OWN_ROWS, LANES)
        pairs = n_dom * n_rep // 2
        results = pl.pallas_call(
            functools.partial(main_kernel, n_dom, n_rep),
            out_shape=(
                pltpu.VMEM((k_size, rows), bf16),
                pltpu.VMEM((OWN_ROWS, LANES), f32),
                pltpu.VMEM((OWN_ROWS, LANES), i32),
                pltpu.VMEM((OWN_ROWS, LANES), f32),
                pltpu.VMEM((1, 1), f32),
            ),
            in_specs=[vmem] * 12,
            out_specs=(vmem,) * 5,
            scratch_shapes=[
                pltpu.VMEM((p_size, rows), bf16),
                pltpu.VMEM((lines, LANES), f32),
                pltpu.VMEM((lines, LANES), f32),
                packs(BATCH * DEPTH),
                lanes(),
                lanes(),
                pltpu.VMEM((OWN_ROWS, LANES), f32),
                pltpu.VMEM((OWN_ROWS, LANES), i32),
                pltpu.VMEM((OWN_ROWS, LANES), f32),
                pltpu.VMEM(spill, f32),
                pltpu.VMEM(spill, i32),
                pltpu.VMEM(own, f32),
                pltpu.VMEM(own, i32),
                pltpu.VMEM((1, LANES), f32),
                pltpu.VMEM((1, LANES), f32),
                pltpu.VMEM((n_rep,) + spill, f32),
                pltpu.VMEM((n_rep,) + spill, i32),
                pltpu.VMEM((n_rep,) + own, f32),
                pltpu.VMEM((n_rep,) + own, i32),
                pltpu.VMEM((1, LANES), f32),
                pltpu.VMEM((pairs, LANES), f32),
            ] + [dma] * 12 + [pltpu.SemaphoreType.REGULAR],
            compiler_params=pltpu.CompilerParams(
                collective_id=0, has_side_effects=True, vmem_limit_bytes=VMEM_LIMIT
            ),
        )(*(kept(x) for x in held))

        force, seg_pen, seg_face, seg_gap, mean = pl.pallas_call(
            finish_kernel,
            out_shape=tuple(jax.ShapeDtypeStruct(x.shape, x.dtype) for x in results),
            in_specs=[vmem] * 5,
            out_specs=(anywhere,) * 5,
            scratch_shapes=[dma((4,)), dma],
            compiler_params=pltpu.CompilerParams(vmem_limit_bytes=VMEM_LIMIT),
        )(*(kept(x) for x in results))
        seg_pen, seg_face, seg_gap = (x.reshape(SEG_DEV) for x in (seg_pen, seg_face, seg_gap))
        return force, seg_pen, seg_face, seg_gap, mean.reshape(())

    rows_spec, wide_spec = P(("dom", "rep")), P(None, ("dom", "rep"))
    return jax.shard_map(
        shards,
        mesh=mesh,
        in_specs=(P(), P(), wide_spec, wide_spec, rows_spec, P()) + (rows_spec,) * 5,
        out_specs=(wide_spec, P("dom"), P("dom"), P("dom"), P()),
        check_vma=False,
    )
```

```python
import functools

import jax
import jax.numpy as jnp
from jax import lax
from jax.experimental import pallas as pl
from jax.experimental.pallas import tpu as pltpu
from jax.sharding import PartitionSpec as P

SEG_DEV = 1024
SPILL = 256
LANES = 128
SUB = 8
WIDTH = 64
PER_ROW = LANES // WIDTH
GROUPS = (SEG_DEV + SPILL) // WIDTH
OWN_GROUPS = SEG_DEV // WIDTH
SPILL_GROUPS = SPILL // WIDTH
OWN_ROWS = SEG_DEV // LANES
SPILL_ROWS = SPILL // LANES
ALL_ROWS = 16
CODE = 32

PENALTY = 400.0
LOWEST_FILL = -1e30
FACE_LIMIT = 1073741824
FACE_MASK = FACE_LIMIT - 1
KEY_LOW = -2147483648
LOGICAL = pl.DeviceIdType.LOGICAL
TILE = 256
DEPTH = 12
BATCH = 4
OWN_BATCHES = OWN_GROUPS // BATCH
UNROLL = 32
CHAINS = 4
FORCE_UNROLL = 8
SEG_UNROLL = 16
LOOP_UNROLL = 4
EXTRA = 16
VMEM_LIMIT = 32 << 20


def split3(x):
    a = x.astype(jnp.bfloat16)
    rest = x - a.astype(jnp.float32)
    b = rest.astype(jnp.bfloat16)
    c = (rest - b.astype(jnp.float32)).astype(jnp.bfloat16)
    return a, b, c


def row(ref, at):
    return ref[pl.ds(at, SUB, stride=0), :]


def pull_groups(first, count, depth0, depth, code_ref, sources, packs):
    all_lines = code_ref.shape[0]
    sub = lax.broadcasted_iota(jnp.int32, (SUB, LANES), 0)
    blocks = -(-count * depth // SUB)
    wants = []
    for b in range(blocks):
        line = sub + SUB * b
        want = jnp.full((SUB, LANES), -2, jnp.int32)
        for q in range(count):
            inside = (line >= q * depth) & (line < (q + 1) * depth)
            want = jnp.where(inside, (line + (depth0 - q * depth)) * CODE + (first + q), want)
        wants.append(want)
    fills = (-1, LOWEST_FILL, -1)

    def pull(i, carry):
        parts = [list(part) for part in carry]
        code = row(code_ref, i)
        values = [row(ref, i) for ref in sources]
        for b in range(blocks):
            hit = code == wants[b]
            for part, value in zip(parts, values):
                part[b] = jnp.where(hit, value, part[b])
        return tuple(tuple(part) for part in parts)

    start = tuple(
        (jnp.full((SUB, LANES), fill, ref.dtype),) * blocks for fill, ref in zip(fills, sources)
    )
    pulled = lax.fori_loop(0, all_lines, pull, start, unroll=8)
    for ref, parts in zip(packs, pulled):
        for b in range(blocks):
            ref[SUB * b : SUB * (b + 1), :] = parts[b]


def match_group(g, at, depth, packs, unroll):
    sub = lax.broadcasted_iota(jnp.int32, (SUB, LANES), 0)
    tiles = WIDTH // SUB
    marks = [sub + (g * WIDTH + SUB * q) for q in range(tiles)]
    start = (
        (jnp.full((SUB, LANES), LOWEST_FILL, jnp.float32),) * tiles,
        (jnp.full((SUB, LANES), KEY_LOW, jnp.int32),) * tiles,
    )

    def one(j, carry):
        pens, keys = (list(part) for part in carry)
        slot, pen, key = (row(ref, at + j) for ref in packs)
        for q in range(tiles):
            hit = slot == marks[q]
            pens[q] = jnp.maximum(pens[q], jnp.where(hit, pen, LOWEST_FILL))
            keys[q] = jnp.maximum(keys[q], jnp.where(hit, key, KEY_LOW))
        return tuple(pens), tuple(keys)

    if unroll == depth:
        for j in range(depth):
            start = one(j, start)
        return start
    return lax.fori_loop(0, depth, one, start, unroll=unroll)


def keep_group(accs, side, parts):
    for ref, part in zip(accs, parts):
        for q in range(WIDTH // SUB):
            at = side * WIDTH + q * SUB
            ref[at : at + SUB, :] = part[q]


def across(accs):
    pens, keys = (ref[...].T for ref in accs)
    return jnp.max(pens, axis=0, keepdims=True), jnp.max(keys, axis=0, keepdims=True)


def project(wt, x_ref, off_ref, tile):
    cols = pl.ds(tile * TILE, TILE)
    per_tile = TILE // LANES
    offset = jnp.concatenate([row(off_ref, tile * per_tile + i) for i in range(per_tile)], axis=1)
    sub = lax.broadcasted_iota(jnp.int32, (SUB, TILE), 0)
    a, b, c = (part.astype(jnp.float32) for part in split3(offset))
    extra = jnp.where(sub == 0, a, jnp.where(sub == 1, b, jnp.where(sub == 2, c, 0.0)))
    extra = jnp.concatenate([extra, jnp.zeros((EXTRA - SUB, TILE), jnp.float32)], axis=0)
    x = jnp.concatenate([x_ref[:, cols], extra.astype(jnp.bfloat16)], axis=0)
    return jnp.dot(wt, x, preferred_element_type=jnp.float32)


def store_row(ref, tile, value):
    per_tile = TILE // LANES
    for i in range(per_tile):
        ref[pl.ds(tile * per_tile + i, 1), :] = value[:, i * LANES : (i + 1) * LANES]


def reduce_field(field, p_size, tile, pen_ref, gap_ref):
    low = [field[SUB * j : SUB * (j + 1)] for j in range(CHAINS)]
    for j in range(CHAINS, p_size // SUB):
        low[j % CHAINS] = jnp.minimum(low[j % CHAINS], field[SUB * j : SUB * (j + 1)])
    store_row(pen_ref, tile, -jnp.min(functools.reduce(jnp.minimum, low), axis=0, keepdims=True))
    store_row(gap_ref, tile, jnp.sum(field[p_size : p_size + SUB], axis=0, keepdims=True))


def prep_kernel(
    live_h, ns_h, nm_h, qw_h, sec_h, mst_h, off_h, jac_h, slot_h, face_h, rank_h,
    x_ref, wt_ref, nq_ref, off_ref, jl_ref, slot_ref, code_ref, key_ref, over_pen, over_key, area_ref,
    live_s, ns_ref, nm_ref, qw_ref, jac_ref, face_ref, rank_ref, pen_ref, gap_ref, packs, accs, s_small, s_big,
):
    lines = slot_ref.shape[0]
    k_size, p_size = ns_ref.shape
    rows = x_ref.shape[1]

    small = [
        pltpu.make_async_copy(source, held, s_small.at[i])
        for i, (source, held) in enumerate((
            (slot_h, slot_ref), (live_h, live_s), (ns_h, ns_ref), (nm_h, nm_ref), (qw_h, qw_ref),
            (face_h, face_ref), (rank_h, rank_ref), (jac_h, jac_ref), (off_h, off_ref),
        ))
    ]
    for copy in small:
        copy.start()
    for base, source in ((0, sec_h), (k_size, mst_h)):
        for at in range(0, k_size, 2 * SUB):
            pltpu.make_async_copy(
                source.at[at : at + 2 * SUB, :], x_ref.at[base + at : base + at + 2 * SUB, :], s_big
            ).start(priority=1)
    for copy in small:
        copy.wait()

    row_id = (
        lax.broadcasted_iota(jnp.int32, (lines, LANES), 0) * LANES
        + lax.broadcasted_iota(jnp.int32, (lines, LANES), 1)
    )
    alive = row_id < live_s[...]
    group = jnp.where(alive, slot_ref[...] // WIDTH, -1)
    before = (
        lax.broadcasted_iota(jnp.int32, (lines, lines), 1)
        < lax.broadcasted_iota(jnp.int32, (lines, lines), 0)
    )
    before = jnp.where(before, 1.0, 0.0).astype(jnp.bfloat16)
    place = jnp.zeros((lines, LANES), jnp.float32)
    for g in range(0, GROUPS, 2):
        mine = [group == g, group == g + 1]
        seen = jnp.concatenate([jnp.where(m, 1.0, 0.0).astype(jnp.bfloat16) for m in mine], axis=1)
        found = jnp.dot(before, seen, preferred_element_type=jnp.float32)
        place = jnp.where(mine[0], found[:, :LANES], jnp.where(mine[1], found[:, LANES:], place))
    code = jnp.where(alive, place.astype(jnp.int32) * CODE + group, -1)
    code_ref[...] = code
    worst = jnp.max(code)

    w = jnp.concatenate([ns_ref[...], -nm_ref[...]], axis=0).astype(jnp.float32)
    qrow = qw_ref[...]
    wt = w.T
    qmat = jnp.broadcast_to(qrow, (LANES, p_size)).T
    v = jnp.sum(wt * qmat, axis=0, keepdims=True)
    qsum = jnp.sum(qmat, axis=0, keepdims=True)
    depth = wt_ref.shape[1]
    pick = lax.broadcasted_iota(jnp.int32, (EXTRA, depth), 0)
    column = lax.broadcasted_iota(jnp.int32, (p_size, depth - 2 * k_size), 1)
    wt_ref[0:p_size, 0 : 2 * k_size] = wt.astype(jnp.bfloat16)
    wt_ref[0:p_size, 2 * k_size :] = jnp.where(column < 3, 1.0, 0.0).astype(jnp.bfloat16)
    lane_row = lax.broadcasted_iota(jnp.int32, (1, LANES), 1)
    tail = jnp.where(lane_row < 3, qsum, 0.0)[:, : depth - 2 * k_size]
    a, b, c = (part.astype(jnp.float32) for part in split3(jnp.concatenate([v, tail], axis=1)))
    stacked = jnp.where(pick == 0, a, jnp.where(pick == 1, b, jnp.where(pick == 2, c, 0.0)))
    wt_ref[p_size:, :] = stacked.astype(jnp.bfloat16)
    scaled = ns_ref[...].astype(jnp.float32) * qrow
    top = scaled.astype(jnp.bfloat16)
    low = (scaled - top.astype(jnp.float32)).astype(jnp.bfloat16)
    nq_ref[...] = jnp.concatenate([top, low], axis=0)

    key_ref[...] = ((rank_ref[...] - 2) << 30) + (FACE_MASK - face_ref[...])
    jl = jnp.where(alive, jac_ref[...], 0.0)
    jl_ref[...] = jl
    area_ref[...] = jnp.sum(jl, axis=0, keepdims=True) * jnp.sum(qrow, axis=1, keepdims=True)
    over_pen[...] = jnp.full(over_pen.shape, LOWEST_FILL, jnp.float32)
    over_key[...] = jnp.full(over_key.shape, KEY_LOW, jnp.int32)

    pltpu.make_async_copy(x_ref, x_ref, s_big).wait()

    @pl.when(worst >= DEPTH * CODE)
    def _():
        weights = wt_ref[...]
        work = face_ref
        line_id = lax.broadcasted_iota(jnp.int32, (lines, LANES), 0)
        work[...] = jnp.where(code >= DEPTH * CODE, line_id * CODE + (code & (CODE - 1)), -1)

        def one(mark):
            line, g = mark // CODE, mark & (CODE - 1)
            tile = line // (TILE // LANES)
            reduce_field(project(weights, x_ref, off_ref, tile), p_size, tile, pen_ref, gap_ref)
            here = row(work, line) == mark
            values = (row(slot_ref, line), row(pen_ref, line), row(key_ref, line))
            for ref, value in zip(packs, values):
                ref[0:SUB, :] = jnp.where(here, value, -1) if ref is packs[0] else value
            found = match_group(g, 0, 1, packs, 1)
            odd = jnp.full((SUB, LANES), g & 1, jnp.int32)
            for side in range(PER_ROW):
                keep_group(accs, side, [
                    [jnp.where(odd == side, x, fill) for x in part]
                    for part, fill in zip(found, (LOWEST_FILL, KEY_LOW))
                ])
            pen, key = across(accs)
            at = pl.ds(g // PER_ROW, 1)
            over_pen[at, :] = jnp.maximum(over_pen[at, :], pen)
            over_key[at, :] = jnp.maximum(over_key[at, :], key)
            left = jnp.where(work[...] == mark, -1, work[...])
            work[...] = left
            return jnp.max(left)

        lax.while_loop(lambda mark: mark >= 0, one, jnp.max(work[...]))


def main_kernel(
    n_dom, n_rep,
    x_ref, wt_ref, nq_ref, off_ref, jl_ref, slot_ref, code_ref, key_ref, over_pen, over_key, area_ref,
    force_ref, out_pen, out_face, out_gap, out_mean,
    load_ref, pen_ref, gap_ref, packs, even_accs, odd_accs, raw_pen, raw_key, seg_ref,
    sp_sf, sp_sg, sp_si, ow_sf, ow_si, t1_s, t2_s, sp_f, sp_g, sp_i, ow_f, ow_i, t1_d, t2_d,
    s_spf, r_spf, s_spg, r_spg, s_spi, r_spi, s_owf, r_owf, s_owi, r_owi, s_t1, r_t1, s_t2, r_t2, inside,
):
    dom = lax.axis_index("dom")
    rep = lax.axis_index("rep")
    k_size = force_ref.shape[0]
    rows = force_ref.shape[1]
    p_size = load_ref.shape[0]
    per_tile = TILE // LANES
    tiles = rows // TILE
    count = n_dom * n_rep
    me = dom * n_rep + rep

    def flat(d, r):
        return lax.rem(d + n_dom, n_dom) * n_rep + lax.rem(r + n_rep, n_rep)

    barrier = pltpu.get_barrier_semaphore()

    def signal(sem, first, last, step=1, at=0):
        def one(i, carry):
            pl.semaphore_signal(sem, inc=1, device_id=i * step + at, device_id_type=LOGICAL)
            return carry

        lax.fori_loop(first, last, one, 0)

    signal(barrier, me + 1, count)
    signal(barrier, dom * n_rep, me)
    signal(barrier, jnp.maximum(dom - 1, 0) * n_rep, dom * n_rep)

    wt = wt_ref[...]

    def wide_row(ref, tile):
        return jnp.concatenate([row(ref, tile * per_tile + i) for i in range(per_tile)], axis=1)

    pairs = count // 2
    pair = lax.div(me, 2)
    odd = lax.rem(rep, 2)
    mate = rep + 1 - 2 * odd

    def batch(step, carry):
        for i in range(UNROLL):
            tile = step * UNROLL + i
            cols = pl.ds(tile * TILE, TILE)
            field = project(wt, x_ref, off_ref, tile)
            for at in range(0, p_size, 2 * SUB):
                load_ref[at : at + 2 * SUB, cols] = jnp.minimum(field[at : at + 2 * SUB].astype(jnp.bfloat16), 0)
            reduce_field(field, p_size, tile, pen_ref, gap_ref)
        return carry

    lax.fori_loop(0, tiles // UNROLL, batch, 0)
    row_gap = gap_ref[...] * jl_ref[...]
    gap_ref[...] = row_gap
    total_gap = jnp.sum(jnp.sum(row_gap, axis=0, keepdims=True), axis=1, keepdims=True)
    total_area = jnp.sum(area_ref[...], axis=1, keepdims=True)
    lane = lax.broadcasted_iota(jnp.int32, (1, LANES), 1)
    t1_s[...] = jnp.where(lane == 0, total_gap, jnp.where(lane == 1, total_area, 0.0))

    after = n_rep * jnp.where(dom == n_dom - 1, 0, 1)
    pl.semaphore_wait(barrier, me + (n_rep - 1 - rep) + after)
    first_copy = pltpu.make_async_remote_copy(
        src_ref=t1_s, dst_ref=t1_d, send_sem=s_t1, recv_sem=r_t1,
        device_id=flat(dom, mate), device_id_type=LOGICAL,
    )
    first_copy.start()
    signal(inside, 0, pair, 2, odd)

    def pull_batch(first):
        pull_groups(first, BATCH, 0, DEPTH, code_ref, (slot_ref, pen_ref, key_ref), packs)

    def match_pair(first, i, accs, last_accs, over, at):
        g = first + i * PER_ROW
        keep_group(accs, 0, match_group(g, i * PER_ROW * DEPTH, DEPTH, packs, LOOP_UNROLL))
        if last_accs is not None:
            close_pair(last_accs, over, at)
        keep_group(accs, 1, match_group(g + 1, (i * PER_ROW + 1) * DEPTH, DEPTH, packs, DEPTH))

    def close_pair(accs, over, at):
        pen, key = across(accs)
        over, at = pl.ds(over, 1), pl.ds(at, 1)
        raw_pen[at, :] = jnp.maximum(pen, over_pen[over, :])
        raw_key[at, :] = jnp.maximum(key, over_key[over, :])

    def decode(top, best):
        none = top < LOWEST_FILL * 0.5
        rank = jnp.where(none, -1, (best >> 30) + 2)
        face = jnp.where(none, FACE_LIMIT, FACE_MASK - (best & FACE_MASK))
        return rank, face

    pull_batch(OWN_GROUPS)
    match_pair(OWN_GROUPS, 0, even_accs, None, 0, 0)
    match_pair(OWN_GROUPS, 1, odd_accs, even_accs, OWN_ROWS, 0)
    close_pair(odd_accs, OWN_ROWS + 1, 1)
    part = slice(0, SPILL_ROWS)
    rank, face = decode(raw_pen[part, :], raw_key[part, :])
    sp_sf[...] = raw_pen[part, :]
    sp_si[0:SPILL_ROWS, :] = rank
    sp_si[SPILL_ROWS:, :] = face

    def spill_copy(j):
        where = flat(dom + 1, rep + j)
        return (
            pltpu.make_async_remote_copy(
                src_ref=sp_sf, dst_ref=sp_f.at[rep], send_sem=s_spf, recv_sem=r_spf,
                device_id=where, device_id_type=LOGICAL,
            ),
            pltpu.make_async_remote_copy(
                src_ref=sp_si, dst_ref=sp_i.at[rep], send_sem=s_spi, recv_sem=r_spi,
                device_id=where, device_id_type=LOGICAL,
            ),
        )

    for j in range(n_rep):
        for copy in spill_copy(j):
            copy.start()

    first_copy.wait_recv()
    both = t1_s[...] + t1_d[...]
    t2_s[...] = both
    t2_d[pl.ds(pair, 1), :] = both

    def send_pairs(first, last):
        def one(other, carry):
            pltpu.make_async_remote_copy(
                src_ref=t2_s, dst_ref=t2_d.at[pl.ds(pair, 1), :], send_sem=s_t2, recv_sem=r_t2,
                device_id=other * 2 + odd, device_id_type=LOGICAL,
            ).start()
            return carry

        lax.fori_loop(first, last, one, 0)

    send_pairs(0, pair)

    def send_up():
        @pl.when(pair < pairs - 1)
        def _():
            pl.semaphore_wait(inside, pairs - 1 - pair)

        send_pairs(pair + 1, pairs)

    quarter = lax.div(me * 4, count)
    turn = OWN_BATCHES - quarter - jnp.where(quarter >= 2, 1, 0)

    hi_id = lax.broadcasted_iota(jnp.int32, (ALL_ROWS, TILE), 0)
    lo_id = lax.broadcasted_iota(jnp.int32, (LANES, TILE), 0)

    def total_up(step, total):
        for i in range(SEG_UNROLL):
            tile = step * SEG_UNROLL + i
            slot = wide_row(slot_ref, tile)[0:1]
            spread = jnp.where(hi_id == slot // LANES, wide_row(gap_ref, tile)[0:1], 0.0)
            left = jnp.concatenate(split3(spread)[:2], axis=0)
            right = jnp.where(lo_id == (slot & (LANES - 1)), 1.0, 0.0).astype(jnp.bfloat16)
            total = total + lax.dot_general(
                left, right, (((1,), (1,)), ((), ())), preferred_element_type=jnp.float32
            )
        return total

    total = lax.fori_loop(0, tiles // SEG_UNROLL, total_up, jnp.zeros((2 * ALL_ROWS, LANES), jnp.float32))
    seg_ref[...] = total[:ALL_ROWS] + total[ALL_ROWS:]
    sp_sg[...] = seg_ref[OWN_ROWS : OWN_ROWS + SPILL_ROWS, :]
    for j in range(n_rep):
        pltpu.make_async_remote_copy(
            src_ref=sp_sg, dst_ref=sp_g.at[rep], send_sem=s_spg, recv_sem=r_spg,
            device_id=flat(dom + 1, rep + j), device_id_type=LOGICAL,
        ).start()

    def own_scan(i, carry):
        @pl.when(i == turn)
        def _():
            send_up()

        first = i * BATCH
        last = lax.rem(2 * i + OWN_ROWS - 1, OWN_ROWS)
        pull_batch(first)
        match_pair(first, 0, even_accs, odd_accs, last, last)
        match_pair(first, 1, odd_accs, even_accs, 2 * i, 2 * i)
        return carry

    lax.fori_loop(0, OWN_BATCHES, own_scan, 0)
    close_pair(odd_accs, OWN_ROWS - 1, OWN_ROWS - 1)
    rank, face = decode(raw_pen[...], raw_key[...])
    ow_sf[0] = raw_pen[...]
    ow_sf[1] = seg_ref[0:OWN_ROWS, :]
    ow_si[0] = rank
    ow_si[1] = face

    def own_copy(j):
        where = flat(dom, rep + j)
        return (
            pltpu.make_async_remote_copy(
                src_ref=ow_sf, dst_ref=ow_f.at[rep], send_sem=s_owf, recv_sem=r_owf,
                device_id=where, device_id_type=LOGICAL,
            ),
            pltpu.make_async_remote_copy(
                src_ref=ow_si, dst_ref=ow_i.at[rep], send_sem=s_owi, recv_sem=r_owi,
                device_id=where, device_id_type=LOGICAL,
            ),
        )

    for j in range(1, n_rep):
        for copy in own_copy(j):
            copy.start()
    ow_f[rep] = ow_sf[...]
    ow_i[rep] = ow_si[...]

    @pl.when(turn >= OWN_BATCHES)
    def _():
        send_up()

    nq = nq_ref[...]

    def push(step, carry):
        for i in range(FORCE_UNROLL):
            tile = step * FORCE_UNROLL + i
            cols = pl.ds(tile * TILE, TILE)
            force = jnp.dot(nq, load_ref[:, cols], preferred_element_type=jnp.float32)
            scale = wide_row(jl_ref, tile)[0:1] * -PENALTY
            force_ref[:, cols] = ((force[:k_size] + force[k_size:]) * scale).astype(jnp.bfloat16)
        return carry

    lax.fori_loop(0, tiles // FORCE_UNROLL, push, 0)

    def encode(rank, face):
        return jnp.where(rank < 0, KEY_LOW, ((rank - 2) << 30) + (FACE_MASK - face))

    def settle(ref, sem):
        pltpu.make_async_copy(ref, ref, sem).wait()

    settle(ow_f.at[pl.ds(0, n_rep - 1)], r_owf)
    settle(ow_i.at[pl.ds(0, n_rep - 1)], r_owi)
    pen_o, gap_o = ow_f[0, 0], ow_f[0, 1]
    key_o = encode(ow_i[0, 0], ow_i[0, 1])
    for r in range(1, n_rep):
        pen_o = jnp.maximum(pen_o, ow_f[r, 0])
        gap_o = gap_o + ow_f[r, 1]
        key_o = jnp.maximum(key_o, encode(ow_i[r, 0], ow_i[r, 1]))

    settle(sp_f, s_spf)
    settle(sp_g, s_spg)
    settle(sp_i, s_spi)
    settle(ow_f.at[pl.ds(0, n_rep - 1)], s_owf)
    settle(ow_i.at[pl.ds(0, n_rep - 1)], s_owi)
    first_copy.wait_send()
    settle(t2_d.at[pl.ds(0, pairs - 1), :], s_t2)

    settle(t2_d.at[pl.ds(0, pairs - 1), :], r_t2)
    settle(sp_f, r_spf)
    settle(sp_g, r_spg)
    settle(sp_i, r_spi)
    whole = jnp.sum(t2_d[...], axis=0, keepdims=True)
    out_mean[...] = whole[:, 0:1] / whole[:, 1:2]

    g = SPILL_ROWS
    pen_s, gap_s = sp_f[0], sp_g[0]
    key_s = encode(sp_i[0, 0:g], sp_i[0, g:])
    for r in range(1, n_rep):
        pen_s = jnp.maximum(pen_s, sp_f[r])
        gap_s = gap_s + sp_g[r]
        key_s = jnp.maximum(key_s, encode(sp_i[r, 0:g], sp_i[r, g:]))

    def finish(at, pen, key, gap):
        none = pen < LOWEST_FILL * 0.5
        out_pen[at, :] = jnp.where(none, 0.0, pen)
        out_face[at, :] = jnp.where(none, -1, FACE_MASK - (key & FACE_MASK))
        out_gap[at, :] = jnp.where(none, 0.0, gap)

    finish(
        slice(0, g), jnp.maximum(pen_o[:g], pen_s), jnp.maximum(key_o[:g], key_s), gap_o[:g] + gap_s
    )
    finish(slice(g, OWN_ROWS), pen_o[g:], key_o[g:], gap_o[g:])


def finish_kernel(force_ref, pen_ref, face_ref, gap_ref, mean_ref, force_h, pen_h, face_h, gap_h, mean_h, sems, s_force):
    copies = [
        pltpu.make_async_copy(held, out, sems.at[i])
        for i, (held, out) in enumerate((
            (pen_ref, pen_h), (face_ref, face_h), (gap_ref, gap_h), (mean_ref, mean_h)
        ))
    ]
    for at in range(0, force_ref.shape[0], SUB):
        part = (slice(at, at + SUB), slice(None))
        pltpu.make_async_copy(force_ref.at[part], force_h.at[part], s_force).start()
    for copy in copies:
        copy.start()
    for copy in copies:
        copy.wait()
    pltpu.make_async_copy(force_ref, force_h, s_force).wait()


def solution(mesh):
    n_dom, n_rep = mesh.shape["dom"], mesh.shape["rep"]
    vmem = pl.BlockSpec(memory_space=pltpu.VMEM)
    anywhere = pl.BlockSpec(memory_space=pl.ANY)
    dma = pltpu.SemaphoreType.DMA

    def kept(x):
        return pltpu.with_memory_space_constraint(x, pltpu.VMEM)

    def streamed(x):
        return pltpu.with_memory_space_constraint(x, pltpu.HBM)

    def shards(ns, nm, sec, mst, off, qw, jac, slot, face, rank, live):
        k_size, p_size = ns.shape
        rows = sec.shape[1]
        lines = rows // LANES
        depth = 2 * k_size + EXTRA
        f32, i32, bf16 = jnp.float32, jnp.int32, jnp.bfloat16

        off, jac, slot, face, rank = (x.reshape(lines, LANES) for x in (off, jac, slot, face, rank))

        def packs(deep):
            return [pltpu.VMEM((deep + SUB, LANES), t) for t in (i32, f32, i32)]

        def lanes():
            return [pltpu.VMEM((LANES, LANES), t) for t in (f32, i32)]

        held = pl.pallas_call(
            prep_kernel,
            out_shape=(
                pltpu.VMEM((2 * k_size, rows), bf16),
                pltpu.VMEM((p_size + EXTRA, depth), bf16),
                pltpu.VMEM((2 * k_size, p_size), bf16),
                pltpu.VMEM((lines, LANES), f32),
                pltpu.VMEM((lines, LANES), f32),
                pltpu.VMEM((lines, LANES), i32),
                pltpu.VMEM((lines, LANES), i32),
                pltpu.VMEM((lines, LANES), i32),
                pltpu.VMEM((ALL_ROWS, LANES), f32),
                pltpu.VMEM((ALL_ROWS, LANES), i32),
                pltpu.VMEM((1, LANES), f32),
            ),
            in_specs=[anywhere] * 11,
            out_specs=(vmem,) * 11,
            scratch_shapes=[
                pltpu.VMEM((1, 1), i32),
                pltpu.VMEM((k_size, p_size), bf16),
                pltpu.VMEM((k_size, p_size), bf16),
                pltpu.VMEM((1, p_size), f32),
                pltpu.VMEM((lines, LANES), f32),
                pltpu.VMEM((lines, LANES), i32),
                pltpu.VMEM((lines, LANES), i32),
                pltpu.VMEM((lines, LANES), f32),
                pltpu.VMEM((lines, LANES), f32),
                packs(SUB),
                lanes(),
                dma((9,)),
                dma,
            ],
            compiler_params=pltpu.CompilerParams(vmem_limit_bytes=VMEM_LIMIT),
        )(
            live.reshape(1, 1),
            *(streamed(x) for x in (ns, nm, qw.reshape(1, p_size), sec, mst, off, jac, slot, face, rank)),
        )

        spill = (2 * SPILL_ROWS, LANES)
        own = (2, OWN_ROWS, LANES)
        pairs = n_dom * n_rep // 2
        results = pl.pallas_call(
            functools.partial(main_kernel, n_dom, n_rep),
            out_shape=(
                pltpu.VMEM((k_size, rows), bf16),
                pltpu.VMEM((OWN_ROWS, LANES), f32),
                pltpu.VMEM((OWN_ROWS, LANES), i32),
                pltpu.VMEM((OWN_ROWS, LANES), f32),
                pltpu.VMEM((1, 1), f32),
            ),
            in_specs=[vmem] * 11,
            out_specs=(vmem,) * 5,
            scratch_shapes=[
                pltpu.VMEM((p_size, rows), bf16),
                pltpu.VMEM((lines, LANES), f32),
                pltpu.VMEM((lines, LANES), f32),
                packs(BATCH * DEPTH),
                lanes(),
                lanes(),
                pltpu.VMEM((OWN_ROWS, LANES), f32),
                pltpu.VMEM((OWN_ROWS, LANES), i32),
                pltpu.VMEM((ALL_ROWS, LANES), f32),
                pltpu.VMEM((SPILL_ROWS, LANES), f32),
                pltpu.VMEM((SPILL_ROWS, LANES), f32),
                pltpu.VMEM(spill, i32),
                pltpu.VMEM(own, f32),
                pltpu.VMEM(own, i32),
                pltpu.VMEM((1, LANES), f32),
                pltpu.VMEM((1, LANES), f32),
                pltpu.VMEM((n_rep, SPILL_ROWS, LANES), f32),
                pltpu.VMEM((n_rep, SPILL_ROWS, LANES), f32),
                pltpu.VMEM((n_rep,) + spill, i32),
                pltpu.VMEM((n_rep,) + own, f32),
                pltpu.VMEM((n_rep,) + own, i32),
                pltpu.VMEM((1, LANES), f32),
                pltpu.VMEM((pairs, LANES), f32),
            ] + [dma] * 14 + [pltpu.SemaphoreType.REGULAR],
            compiler_params=pltpu.CompilerParams(
                collective_id=0, has_side_effects=True, vmem_limit_bytes=VMEM_LIMIT
            ),
        )(*(kept(x) for x in held))

        force, seg_pen, seg_face, seg_gap, mean = pl.pallas_call(
            finish_kernel,
            out_shape=tuple(jax.ShapeDtypeStruct(x.shape, x.dtype) for x in results),
            in_specs=[vmem] * 5,
            out_specs=(anywhere,) * 5,
            scratch_shapes=[dma((4,)), dma],
            compiler_params=pltpu.CompilerParams(vmem_limit_bytes=VMEM_LIMIT),
        )(*(kept(x) for x in results))
        seg_pen, seg_face, seg_gap = (x.reshape(SEG_DEV) for x in (seg_pen, seg_face, seg_gap))
        return force, seg_pen, seg_face, seg_gap, mean.reshape(())

    rows_spec, wide_spec = P(("dom", "rep")), P(None, ("dom", "rep"))
    return jax.shard_map(
        shards,
        mesh=mesh,
        in_specs=(P(), P(), wide_spec, wide_spec, rows_spec, P()) + (rows_spec,) * 5,
        out_specs=(wide_spec, P("dom"), P("dom"), P("dom"), P()),
        check_vma=False,
    )
```

```python
import functools

import jax
import jax.numpy as jnp
from jax import lax
from jax.experimental import pallas as pl
from jax.experimental.pallas import tpu as pltpu
from jax.sharding import PartitionSpec as P

SEG_DEV = 1024
SPILL = 256
LANES = 128
SUB = 8
WIDTH = 64
PER_ROW = LANES // WIDTH
GROUPS = (SEG_DEV + SPILL) // WIDTH
OWN_GROUPS = SEG_DEV // WIDTH
SPILL_GROUPS = SPILL // WIDTH
OWN_ROWS = SEG_DEV // LANES
SPILL_ROWS = SPILL // LANES
ALL_ROWS = 16
CODE = 32

PENALTY = 400.0
LOWEST_FILL = -1e30
FACE_LIMIT = 1073741824
FACE_MASK = FACE_LIMIT - 1
KEY_LOW = -2147483648
LOGICAL = pl.DeviceIdType.LOGICAL
TILE = 256
DEPTH = 12
BATCH = 4
OWN_BATCHES = OWN_GROUPS // BATCH
UNROLL = 32
CHAINS = 4
FORCE_UNROLL = 8
LOOP_UNROLL = 4
EXTRA = 16
VMEM_LIMIT = 32 << 20


def split3(x):
    a = x.astype(jnp.bfloat16)
    rest = x - a.astype(jnp.float32)
    b = rest.astype(jnp.bfloat16)
    c = (rest - b.astype(jnp.float32)).astype(jnp.bfloat16)
    return a, b, c


def row(ref, at):
    return ref[pl.ds(at, SUB, stride=0), :]


def pull_groups(first, count, depth0, depth, code_ref, sources, packs):
    all_lines = code_ref.shape[0]
    sub = lax.broadcasted_iota(jnp.int32, (SUB, LANES), 0)
    blocks = -(-count * depth // SUB)
    wants = []
    for b in range(blocks):
        line = sub + SUB * b
        want = jnp.full((SUB, LANES), -2, jnp.int32)
        for q in range(count):
            inside = (line >= q * depth) & (line < (q + 1) * depth)
            want = jnp.where(inside, (line + (depth0 - q * depth)) * CODE + (first + q), want)
        wants.append(want)
    fills = (-1, LOWEST_FILL, -1, 0.0)

    def pull(i, carry):
        parts = [list(part) for part in carry]
        code = row(code_ref, i)
        values = [row(ref, i) for ref in sources]
        for b in range(blocks):
            hit = code == wants[b]
            for part, value in zip(parts, values):
                part[b] = jnp.where(hit, value, part[b])
        return tuple(tuple(part) for part in parts)

    start = tuple(
        (jnp.full((SUB, LANES), fill, ref.dtype),) * blocks for fill, ref in zip(fills, sources)
    )
    pulled = lax.fori_loop(0, all_lines, pull, start, unroll=8)
    for ref, parts in zip(packs, pulled):
        for b in range(blocks):
            ref[SUB * b : SUB * (b + 1), :] = parts[b]


def match_group(g, at, depth, packs, unroll):
    sub = lax.broadcasted_iota(jnp.int32, (SUB, LANES), 0)
    tiles = WIDTH // SUB
    marks = [sub + (g * WIDTH + SUB * q) for q in range(tiles)]
    start = (
        (jnp.full((SUB, LANES), LOWEST_FILL, jnp.float32),) * tiles,
        (jnp.full((SUB, LANES), KEY_LOW, jnp.int32),) * tiles,
        (jnp.zeros((SUB, LANES), jnp.float32),) * tiles,
    )

    def one(j, carry):
        pens, keys, gaps = (list(part) for part in carry)
        slot, pen, key, gap = (row(ref, at + j) for ref in packs)
        for q in range(tiles):
            hit = slot == marks[q]
            pens[q] = jnp.maximum(pens[q], jnp.where(hit, pen, LOWEST_FILL))
            keys[q] = jnp.maximum(keys[q], jnp.where(hit, key, KEY_LOW))
            gaps[q] = gaps[q] + jnp.where(hit, gap, 0.0)
        return tuple(pens), tuple(keys), tuple(gaps)

    if unroll == depth:
        for j in range(depth):
            start = one(j, start)
        return start
    return lax.fori_loop(0, depth, one, start, unroll=unroll)


def keep_group(accs, side, parts):
    for ref, part in zip(accs, parts):
        for q in range(WIDTH // SUB):
            at = side * WIDTH + q * SUB
            ref[at : at + SUB, :] = part[q]


def across(accs):
    pens, keys, gaps = (ref[...].T for ref in accs)
    return (
        jnp.max(pens, axis=0, keepdims=True),
        jnp.max(keys, axis=0, keepdims=True),
        jnp.sum(gaps, axis=0, keepdims=True),
    )


def project(wt, x_ref, off_ref, tile):
    cols = pl.ds(tile * TILE, TILE)
    per_tile = TILE // LANES
    offset = jnp.concatenate([row(off_ref, tile * per_tile + i) for i in range(per_tile)], axis=1)
    sub = lax.broadcasted_iota(jnp.int32, (SUB, TILE), 0)
    a, b, c = (part.astype(jnp.float32) for part in split3(offset))
    extra = jnp.where(sub == 0, a, jnp.where(sub == 1, b, jnp.where(sub == 2, c, 0.0)))
    extra = jnp.concatenate([extra, jnp.zeros((EXTRA - SUB, TILE), jnp.float32)], axis=0)
    x = jnp.concatenate([x_ref[:, cols], extra.astype(jnp.bfloat16)], axis=0)
    return jnp.dot(wt, x, preferred_element_type=jnp.float32)


def store_row(ref, tile, value):
    per_tile = TILE // LANES
    for i in range(per_tile):
        ref[pl.ds(tile * per_tile + i, 1), :] = value[:, i * LANES : (i + 1) * LANES]


def reduce_field(field, p_size, tile, pen_ref, gap_ref):
    low = [field[SUB * j : SUB * (j + 1)] for j in range(CHAINS)]
    for j in range(CHAINS, p_size // SUB):
        low[j % CHAINS] = jnp.minimum(low[j % CHAINS], field[SUB * j : SUB * (j + 1)])
    store_row(pen_ref, tile, -jnp.min(functools.reduce(jnp.minimum, low), axis=0, keepdims=True))
    store_row(gap_ref, tile, jnp.sum(field[p_size : p_size + SUB], axis=0, keepdims=True))


def prep_kernel(
    live_h, ns_h, nm_h, qw_h, sec_h, mst_h, off_h, jac_h, slot_h, face_h, rank_h,
    x_ref, wt_ref, nq_ref, off_ref, jl_ref, slot_ref, code_ref, key_ref, over_pen, over_key, over_gap, area_ref,
    live_s, ns_ref, nm_ref, qw_ref, jac_ref, face_ref, rank_ref, pen_ref, gap_ref, packs, accs, s_small, s_big,
):
    lines = slot_ref.shape[0]
    k_size, p_size = ns_ref.shape
    rows = x_ref.shape[1]

    small = [
        pltpu.make_async_copy(source, held, s_small.at[i])
        for i, (source, held) in enumerate((
            (slot_h, slot_ref), (live_h, live_s), (ns_h, ns_ref), (nm_h, nm_ref), (qw_h, qw_ref),
            (face_h, face_ref), (rank_h, rank_ref), (jac_h, jac_ref), (off_h, off_ref),
        ))
    ]
    for copy in small:
        copy.start()
    for base, source in ((0, sec_h), (k_size, mst_h)):
        for at in range(0, k_size, 2 * SUB):
            pltpu.make_async_copy(
                source.at[at : at + 2 * SUB, :], x_ref.at[base + at : base + at + 2 * SUB, :], s_big
            ).start(priority=1)
    for copy in small:
        copy.wait()

    row_id = (
        lax.broadcasted_iota(jnp.int32, (lines, LANES), 0) * LANES
        + lax.broadcasted_iota(jnp.int32, (lines, LANES), 1)
    )
    alive = row_id < live_s[...]
    group = jnp.where(alive, slot_ref[...] // WIDTH, -1)
    before = (
        lax.broadcasted_iota(jnp.int32, (lines, lines), 1)
        < lax.broadcasted_iota(jnp.int32, (lines, lines), 0)
    )
    before = jnp.where(before, 1.0, 0.0).astype(jnp.bfloat16)
    place = jnp.zeros((lines, LANES), jnp.float32)
    for g in range(0, GROUPS, 2):
        mine = [group == g, group == g + 1]
        seen = jnp.concatenate([jnp.where(m, 1.0, 0.0).astype(jnp.bfloat16) for m in mine], axis=1)
        found = jnp.dot(before, seen, preferred_element_type=jnp.float32)
        place = jnp.where(mine[0], found[:, :LANES], jnp.where(mine[1], found[:, LANES:], place))
    code = jnp.where(alive, place.astype(jnp.int32) * CODE + group, -1)
    code_ref[...] = code
    worst = jnp.max(code)

    w = jnp.concatenate([ns_ref[...], -nm_ref[...]], axis=0).astype(jnp.float32)
    qrow = qw_ref[...]
    wt = w.T
    qmat = jnp.broadcast_to(qrow, (LANES, p_size)).T
    v = jnp.sum(wt * qmat, axis=0, keepdims=True)
    qsum = jnp.sum(qmat, axis=0, keepdims=True)
    depth = wt_ref.shape[1]
    pick = lax.broadcasted_iota(jnp.int32, (EXTRA, depth), 0)
    column = lax.broadcasted_iota(jnp.int32, (p_size, depth - 2 * k_size), 1)
    wt_ref[0:p_size, 0 : 2 * k_size] = wt.astype(jnp.bfloat16)
    wt_ref[0:p_size, 2 * k_size :] = jnp.where(column < 3, 1.0, 0.0).astype(jnp.bfloat16)
    lane_row = lax.broadcasted_iota(jnp.int32, (1, LANES), 1)
    tail = jnp.where(lane_row < 3, qsum, 0.0)[:, : depth - 2 * k_size]
    a, b, c = (part.astype(jnp.float32) for part in split3(jnp.concatenate([v, tail], axis=1)))
    stacked = jnp.where(pick == 0, a, jnp.where(pick == 1, b, jnp.where(pick == 2, c, 0.0)))
    wt_ref[p_size:, :] = stacked.astype(jnp.bfloat16)
    scaled = ns_ref[...].astype(jnp.float32) * qrow
    top = scaled.astype(jnp.bfloat16)
    low = (scaled - top.astype(jnp.float32)).astype(jnp.bfloat16)
    nq_ref[...] = jnp.concatenate([top, low], axis=0)

    key_ref[...] = ((rank_ref[...] - 2) << 30) + (FACE_MASK - face_ref[...])
    jl = jnp.where(alive, jac_ref[...], 0.0)
    jl_ref[...] = jl
    area_ref[...] = jnp.sum(jl, axis=0, keepdims=True) * jnp.sum(qrow, axis=1, keepdims=True)
    over_pen[...] = jnp.full(over_pen.shape, LOWEST_FILL, jnp.float32)
    over_key[...] = jnp.full(over_key.shape, KEY_LOW, jnp.int32)
    over_gap[...] = jnp.zeros(over_gap.shape, jnp.float32)

    pltpu.make_async_copy(x_ref, x_ref, s_big).wait()

    @pl.when(worst >= DEPTH * CODE)
    def _():
        weights = wt_ref[...]
        work = face_ref
        line_id = lax.broadcasted_iota(jnp.int32, (lines, LANES), 0)
        work[...] = jnp.where(code >= DEPTH * CODE, line_id * CODE + (code & (CODE - 1)), -1)

        def one(mark):
            line, g = mark // CODE, mark & (CODE - 1)
            tile = line // (TILE // LANES)
            reduce_field(project(weights, x_ref, off_ref, tile), p_size, tile, pen_ref, gap_ref)
            here = row(work, line) == mark
            values = (
                row(slot_ref, line), row(pen_ref, line), row(key_ref, line), row(gap_ref, line) * row(jl_ref, line)
            )
            for ref, value in zip(packs, values):
                ref[0:SUB, :] = jnp.where(here, value, -1) if ref is packs[0] else value
            found = match_group(g, 0, 1, packs, 1)
            odd = jnp.full((SUB, LANES), g & 1, jnp.int32)
            for side in range(PER_ROW):
                keep_group(accs, side, [
                    [jnp.where(odd == side, x, fill) for x in part]
                    for part, fill in zip(found, (LOWEST_FILL, KEY_LOW, 0.0))
                ])
            pen, key, gap = across(accs)
            at = pl.ds(g // PER_ROW, 1)
            over_pen[at, :] = jnp.maximum(over_pen[at, :], pen)
            over_key[at, :] = jnp.maximum(over_key[at, :], key)
            over_gap[at, :] = over_gap[at, :] + gap
            left = jnp.where(work[...] == mark, -1, work[...])
            work[...] = left
            return jnp.max(left)

        lax.while_loop(lambda mark: mark >= 0, one, jnp.max(work[...]))


def main_kernel(
    n_dom, n_rep,
    x_ref, wt_ref, nq_ref, off_ref, jl_ref, slot_ref, code_ref, key_ref, over_pen, over_key, over_gap, area_ref,
    force_ref, out_pen, out_face, out_gap, out_mean,
    load_ref, pen_ref, gap_ref, packs, even_accs, odd_accs, raw_pen, raw_key, raw_gap,
    sp_sf, sp_si, ow_sf, ow_si, t1_s, t2_s, sp_f, sp_i, ow_f, ow_i, t1_d, t2_d,
    s_spf, r_spf, s_spi, r_spi, s_owf, r_owf, s_owi, r_owi, s_t1, r_t1, s_t2, r_t2, inside,
):
    dom = lax.axis_index("dom")
    rep = lax.axis_index("rep")
    k_size = force_ref.shape[0]
    rows = force_ref.shape[1]
    p_size = load_ref.shape[0]
    per_tile = TILE // LANES
    tiles = rows // TILE
    count = n_dom * n_rep
    me = dom * n_rep + rep

    def flat(d, r):
        return lax.rem(d + n_dom, n_dom) * n_rep + lax.rem(r + n_rep, n_rep)

    barrier = pltpu.get_barrier_semaphore()

    def signal(sem, first, last, step=1, at=0):
        def one(i, carry):
            pl.semaphore_signal(sem, inc=1, device_id=i * step + at, device_id_type=LOGICAL)
            return carry

        lax.fori_loop(first, last, one, 0)

    signal(barrier, me + 1, count)
    signal(barrier, dom * n_rep, me)
    signal(barrier, jnp.maximum(dom - 1, 0) * n_rep, dom * n_rep)

    wt = wt_ref[...]

    def wide_row(ref, tile):
        return jnp.concatenate([row(ref, tile * per_tile + i) for i in range(per_tile)], axis=1)

    pairs = count // 2
    pair = lax.div(me, 2)
    odd = lax.rem(rep, 2)
    mate = rep + 1 - 2 * odd

    def batch(step, carry):
        for i in range(UNROLL):
            tile = step * UNROLL + i
            cols = pl.ds(tile * TILE, TILE)
            field = project(wt, x_ref, off_ref, tile)
            for at in range(0, p_size, 2 * SUB):
                load_ref[at : at + 2 * SUB, cols] = jnp.minimum(field[at : at + 2 * SUB].astype(jnp.bfloat16), 0)
            reduce_field(field, p_size, tile, pen_ref, gap_ref)
        return carry

    lax.fori_loop(0, tiles // UNROLL, batch, 0)
    row_gap = gap_ref[...] * jl_ref[...]
    gap_ref[...] = row_gap
    total_gap = jnp.sum(jnp.sum(row_gap, axis=0, keepdims=True), axis=1, keepdims=True)
    total_area = jnp.sum(area_ref[...], axis=1, keepdims=True)
    lane = lax.broadcasted_iota(jnp.int32, (1, LANES), 1)
    t1_s[0:1, :] = jnp.where(lane == 0, total_gap, 0.0)
    t1_s[1:2, :] = jnp.where(lane == 0, total_area, 1.0)

    after = n_rep * jnp.where(dom == n_dom - 1, 0, 1)
    pl.semaphore_wait(barrier, me + (n_rep - 1 - rep) + after)
    first_copy = pltpu.make_async_remote_copy(
        src_ref=t1_s, dst_ref=t1_d, send_sem=s_t1, recv_sem=r_t1,
        device_id=flat(dom, mate), device_id_type=LOGICAL,
    )
    first_copy.start()
    signal(inside, 0, pair, 2, odd)

    def pull_batch(first):
        pull_groups(first, BATCH, 0, DEPTH, code_ref, (slot_ref, pen_ref, key_ref, gap_ref), packs)

    def match_pair(first, i, accs, last_accs, over, at):
        g = first + i * PER_ROW
        keep_group(accs, 0, match_group(g, i * PER_ROW * DEPTH, DEPTH, packs, LOOP_UNROLL))
        if last_accs is not None:
            close_pair(last_accs, over, at)
        unroll = LOOP_UNROLL if last_accs is None else DEPTH
        keep_group(accs, 1, match_group(g + 1, (i * PER_ROW + 1) * DEPTH, DEPTH, packs, unroll))

    def close_pair(accs, over, at):
        pen, key, gap = across(accs)
        over, at = pl.ds(over, 1), pl.ds(at, 1)
        raw_pen[at, :] = jnp.maximum(pen, over_pen[over, :])
        raw_key[at, :] = jnp.maximum(key, over_key[over, :])
        raw_gap[at, :] = gap + over_gap[over, :]

    def decode(top, best):
        none = top < LOWEST_FILL * 0.5
        rank = jnp.where(none, -1, (best >> 30) + 2)
        face = jnp.where(none, FACE_LIMIT, FACE_MASK - (best & FACE_MASK))
        return rank, face

    pull_batch(OWN_GROUPS)
    match_pair(OWN_GROUPS, 0, even_accs, None, 0, 0)
    match_pair(OWN_GROUPS, 1, odd_accs, even_accs, OWN_ROWS, 0)
    close_pair(odd_accs, OWN_ROWS + 1, 1)
    part = slice(0, SPILL_ROWS)
    rank, face = decode(raw_pen[part, :], raw_key[part, :])
    sp_sf[0:SPILL_ROWS, :] = raw_pen[part, :]
    sp_sf[SPILL_ROWS:, :] = raw_gap[part, :]
    sp_si[0:SPILL_ROWS, :] = rank
    sp_si[SPILL_ROWS:, :] = face

    def spill_copy(j):
        where = flat(dom + 1, rep + j)
        return (
            pltpu.make_async_remote_copy(
                src_ref=sp_sf, dst_ref=sp_f.at[rep], send_sem=s_spf, recv_sem=r_spf,
                device_id=where, device_id_type=LOGICAL,
            ),
            pltpu.make_async_remote_copy(
                src_ref=sp_si, dst_ref=sp_i.at[rep], send_sem=s_spi, recv_sem=r_spi,
                device_id=where, device_id_type=LOGICAL,
            ),
        )

    for j in range(n_rep):
        for copy in spill_copy(j):
            copy.start()

    first_copy.wait_recv()
    both = t1_s[...] + t1_d[...]
    t2_s[...] = both
    t2_d[pair] = both

    def send_pairs(first, last):
        def one(other, carry):
            pltpu.make_async_remote_copy(
                src_ref=t2_s, dst_ref=t2_d.at[pair], send_sem=s_t2, recv_sem=r_t2,
                device_id=other * 2 + odd, device_id_type=LOGICAL,
            ).start()
            return carry

        lax.fori_loop(first, last, one, 0)

    send_pairs(0, pair)

    def send_up():
        @pl.when(pair < pairs - 1)
        def _():
            pl.semaphore_wait(inside, pairs - 1 - pair)

        send_pairs(pair + 1, pairs)

    quarter = lax.div(me * 4, count)
    turn = OWN_BATCHES - quarter - jnp.where(quarter >= 2, 1, 0)

    def own_scan(i, carry):
        @pl.when(i == turn)
        def _():
            send_up()

        first = i * BATCH
        last = lax.rem(2 * i + OWN_ROWS - 1, OWN_ROWS)
        pull_batch(first)
        match_pair(first, 0, even_accs, odd_accs, last, last)
        match_pair(first, 1, odd_accs, even_accs, 2 * i, 2 * i)
        return carry

    lax.fori_loop(0, OWN_BATCHES, own_scan, 0)
    close_pair(odd_accs, OWN_ROWS - 1, OWN_ROWS - 1)
    rank, face = decode(raw_pen[...], raw_key[...])
    ow_sf[0] = raw_pen[...]
    ow_sf[1] = raw_gap[...]
    ow_si[0] = rank
    ow_si[1] = face

    def own_copy(j):
        where = flat(dom, rep + j)
        return (
            pltpu.make_async_remote_copy(
                src_ref=ow_sf, dst_ref=ow_f.at[rep], send_sem=s_owf, recv_sem=r_owf,
                device_id=where, device_id_type=LOGICAL,
            ),
            pltpu.make_async_remote_copy(
                src_ref=ow_si, dst_ref=ow_i.at[rep], send_sem=s_owi, recv_sem=r_owi,
                device_id=where, device_id_type=LOGICAL,
            ),
        )

    for j in range(1, n_rep):
        for copy in own_copy(j):
            copy.start()
    ow_f[rep] = ow_sf[...]
    ow_i[rep] = ow_si[...]

    @pl.when(turn >= OWN_BATCHES)
    def _():
        send_up()

    nq = nq_ref[...]

    def push(step, carry):
        for i in range(FORCE_UNROLL):
            tile = step * FORCE_UNROLL + i
            cols = pl.ds(tile * TILE, TILE)
            force = jnp.dot(nq, load_ref[:, cols], preferred_element_type=jnp.float32)
            scale = wide_row(jl_ref, tile)[0:1] * -PENALTY
            force_ref[:, cols] = ((force[:k_size] + force[k_size:]) * scale).astype(jnp.bfloat16)
        return carry

    lax.fori_loop(0, tiles // FORCE_UNROLL, push, 0)

    def encode(rank, face):
        return jnp.where(rank < 0, KEY_LOW, ((rank - 2) << 30) + (FACE_MASK - face))

    def settle(ref, sem):
        pltpu.make_async_copy(ref, ref, sem).wait()

    settle(ow_f.at[pl.ds(0, n_rep - 1)], r_owf)
    settle(ow_i.at[pl.ds(0, n_rep - 1)], r_owi)
    pen_o, gap_o = ow_f[0, 0], ow_f[0, 1]
    key_o = encode(ow_i[0, 0], ow_i[0, 1])
    for r in range(1, n_rep):
        pen_o = jnp.maximum(pen_o, ow_f[r, 0])
        gap_o = gap_o + ow_f[r, 1]
        key_o = jnp.maximum(key_o, encode(ow_i[r, 0], ow_i[r, 1]))

    settle(sp_f, s_spf)
    settle(sp_i, s_spi)
    settle(ow_f.at[pl.ds(0, n_rep - 1)], s_owf)
    settle(ow_i.at[pl.ds(0, n_rep - 1)], s_owi)
    first_copy.wait_send()
    settle(t2_d.at[pl.ds(0, pairs - 1)], s_t2)

    settle(t2_d.at[pl.ds(0, pairs - 1)], r_t2)
    settle(sp_f, r_spf)
    settle(sp_i, r_spi)
    whole = jnp.sum(t2_d[...], axis=0)
    out_mean[...] = (whole[0:1] / whole[1:2])[:, 0:1]

    g = SPILL_ROWS
    pen_s, gap_s = sp_f[0, 0:g], sp_f[0, g:]
    key_s = encode(sp_i[0, 0:g], sp_i[0, g:])
    for r in range(1, n_rep):
        pen_s = jnp.maximum(pen_s, sp_f[r, 0:g])
        gap_s = gap_s + sp_f[r, g:]
        key_s = jnp.maximum(key_s, encode(sp_i[r, 0:g], sp_i[r, g:]))

    def finish(at, pen, key, gap):
        none = pen < LOWEST_FILL * 0.5
        out_pen[at, :] = jnp.where(none, 0.0, pen)
        out_face[at, :] = jnp.where(none, -1, FACE_MASK - (key & FACE_MASK))
        out_gap[at, :] = jnp.where(none, 0.0, gap)

    finish(
        slice(0, g), jnp.maximum(pen_o[:g], pen_s), jnp.maximum(key_o[:g], key_s), gap_o[:g] + gap_s
    )
    finish(slice(g, OWN_ROWS), pen_o[g:], key_o[g:], gap_o[g:])


def finish_kernel(force_ref, pen_ref, face_ref, gap_ref, mean_ref, force_h, pen_h, face_h, gap_h, mean_h, sems, s_force):
    copies = [
        pltpu.make_async_copy(held, out, sems.at[i])
        for i, (held, out) in enumerate((
            (pen_ref, pen_h), (face_ref, face_h), (gap_ref, gap_h), (mean_ref, mean_h)
        ))
    ]
    for at in range(0, force_ref.shape[0], SUB):
        part = (slice(at, at + SUB), slice(None))
        pltpu.make_async_copy(force_ref.at[part], force_h.at[part], s_force).start()
    for copy in copies:
        copy.start()
    for copy in copies:
        copy.wait()
    pltpu.make_async_copy(force_ref, force_h, s_force).wait()


def solution(mesh):
    n_dom, n_rep = mesh.shape["dom"], mesh.shape["rep"]
    vmem = pl.BlockSpec(memory_space=pltpu.VMEM)
    anywhere = pl.BlockSpec(memory_space=pl.ANY)
    dma = pltpu.SemaphoreType.DMA

    def kept(x):
        return pltpu.with_memory_space_constraint(x, pltpu.VMEM)

    def streamed(x):
        return pltpu.with_memory_space_constraint(x, pltpu.HBM)

    def shards(ns, nm, sec, mst, off, qw, jac, slot, face, rank, live):
        k_size, p_size = ns.shape
        rows = sec.shape[1]
        lines = rows // LANES
        depth = 2 * k_size + EXTRA
        f32, i32, bf16 = jnp.float32, jnp.int32, jnp.bfloat16

        off, jac, slot, face, rank = (x.reshape(lines, LANES) for x in (off, jac, slot, face, rank))

        def packs(deep):
            return [pltpu.VMEM((deep + SUB, LANES), t) for t in (i32, f32, i32, f32)]

        def lanes():
            return [pltpu.VMEM((LANES, LANES), t) for t in (f32, i32, f32)]

        held = pl.pallas_call(
            prep_kernel,
            out_shape=(
                pltpu.VMEM((2 * k_size, rows), bf16),
                pltpu.VMEM((p_size + EXTRA, depth), bf16),
                pltpu.VMEM((2 * k_size, p_size), bf16),
                pltpu.VMEM((lines, LANES), f32),
                pltpu.VMEM((lines, LANES), f32),
                pltpu.VMEM((lines, LANES), i32),
                pltpu.VMEM((lines, LANES), i32),
                pltpu.VMEM((lines, LANES), i32),
                pltpu.VMEM((ALL_ROWS, LANES), f32),
                pltpu.VMEM((ALL_ROWS, LANES), i32),
                pltpu.VMEM((ALL_ROWS, LANES), f32),
                pltpu.VMEM((1, LANES), f32),
            ),
            in_specs=[anywhere] * 11,
            out_specs=(vmem,) * 12,
            scratch_shapes=[
                pltpu.VMEM((1, 1), i32),
                pltpu.VMEM((k_size, p_size), bf16),
                pltpu.VMEM((k_size, p_size), bf16),
                pltpu.VMEM((1, p_size), f32),
                pltpu.VMEM((lines, LANES), f32),
                pltpu.VMEM((lines, LANES), i32),
                pltpu.VMEM((lines, LANES), i32),
                pltpu.VMEM((lines, LANES), f32),
                pltpu.VMEM((lines, LANES), f32),
                packs(SUB),
                lanes(),
                dma((9,)),
                dma,
            ],
            compiler_params=pltpu.CompilerParams(vmem_limit_bytes=VMEM_LIMIT),
        )(
            live.reshape(1, 1),
            *(streamed(x) for x in (ns, nm, qw.reshape(1, p_size), sec, mst, off, jac, slot, face, rank)),
        )

        spill = (2 * SPILL_ROWS, LANES)
        own = (2, OWN_ROWS, LANES)
        pairs = n_dom * n_rep // 2
        results = pl.pallas_call(
            functools.partial(main_kernel, n_dom, n_rep),
            out_shape=(
                pltpu.VMEM((k_size, rows), bf16),
                pltpu.VMEM((OWN_ROWS, LANES), f32),
                pltpu.VMEM((OWN_ROWS, LANES), i32),
                pltpu.VMEM((OWN_ROWS, LANES), f32),
                pltpu.VMEM((1, 1), f32),
            ),
            in_specs=[vmem] * 12,
            out_specs=(vmem,) * 5,
            scratch_shapes=[
                pltpu.VMEM((p_size, rows), bf16),
                pltpu.VMEM((lines, LANES), f32),
                pltpu.VMEM((lines, LANES), f32),
                packs(BATCH * DEPTH),
                lanes(),
                lanes(),
                pltpu.VMEM((OWN_ROWS, LANES), f32),
                pltpu.VMEM((OWN_ROWS, LANES), i32),
                pltpu.VMEM((OWN_ROWS, LANES), f32),
                pltpu.VMEM(spill, f32),
                pltpu.VMEM(spill, i32),
                pltpu.VMEM(own, f32),
                pltpu.VMEM(own, i32),
                pltpu.VMEM((2, LANES), f32),
                pltpu.VMEM((2, LANES), f32),
                pltpu.VMEM((n_rep,) + spill, f32),
                pltpu.VMEM((n_rep,) + spill, i32),
                pltpu.VMEM((n_rep,) + own, f32),
                pltpu.VMEM((n_rep,) + own, i32),
                pltpu.VMEM((2, LANES), f32),
                pltpu.VMEM((pairs, 2, LANES), f32),
            ] + [dma] * 12 + [pltpu.SemaphoreType.REGULAR],
            compiler_params=pltpu.CompilerParams(
                collective_id=0, has_side_effects=True, vmem_limit_bytes=VMEM_LIMIT
            ),
        )(*(kept(x) for x in held))

        force, seg_pen, seg_face, seg_gap, mean = pl.pallas_call(
            finish_kernel,
            out_shape=tuple(jax.ShapeDtypeStruct(x.shape, x.dtype) for x in results),
            in_specs=[vmem] * 5,
            out_specs=(anywhere,) * 5,
            scratch_shapes=[dma((4,)), dma],
            compiler_params=pltpu.CompilerParams(vmem_limit_bytes=VMEM_LIMIT),
        )(*(kept(x) for x in results))
        seg_pen, seg_face, seg_gap = (x.reshape(SEG_DEV) for x in (seg_pen, seg_face, seg_gap))
        return force, seg_pen, seg_face, seg_gap, mean.reshape(())

    rows_spec, wide_spec = P(("dom", "rep")), P(None, ("dom", "rep"))
    return jax.shard_map(
        shards,
        mesh=mesh,
        in_specs=(P(), P(), wide_spec, wide_spec, rows_spec, P()) + (rows_spec,) * 5,
        out_specs=(wide_spec, P("dom"), P("dom"), P("dom"), P()),
        check_vma=False,
    )
```

```python
import functools

import jax
import jax.numpy as jnp
from jax import lax
from jax.experimental import pallas as pl
from jax.experimental.pallas import tpu as pltpu
from jax.sharding import PartitionSpec as P

SEG_DEV = 1024
SPILL = 256
LANES = 128
SUB = 8
WIDTH = 64
PER_ROW = LANES // WIDTH
GROUPS = (SEG_DEV + SPILL) // WIDTH
OWN_GROUPS = SEG_DEV // WIDTH
SPILL_GROUPS = SPILL // WIDTH
OWN_ROWS = SEG_DEV // LANES
SPILL_ROWS = SPILL // LANES
ALL_ROWS = 16
CODE = 32

PENALTY = 400.0
LOWEST_FILL = -1e30
FACE_LIMIT = 1073741824
FACE_MASK = FACE_LIMIT - 1
KEY_LOW = -2147483648
LOGICAL = pl.DeviceIdType.LOGICAL
TILE = 256
DEPTH = 12
BATCH = 4
OWN_BATCHES = OWN_GROUPS // BATCH
UNROLL = 32
CHAINS = 4
FORCE_UNROLL = 8
LOOP_UNROLL = 4
EXTRA = 16
VMEM_LIMIT = 32 << 20


def split3(x):
    a = x.astype(jnp.bfloat16)
    rest = x - a.astype(jnp.float32)
    b = rest.astype(jnp.bfloat16)
    c = (rest - b.astype(jnp.float32)).astype(jnp.bfloat16)
    return a, b, c


def row(ref, at):
    return ref[pl.ds(at, SUB, stride=0), :]


def pull_groups(first, count, depth0, depth, code_ref, sources, packs):
    all_lines = code_ref.shape[0]
    sub = lax.broadcasted_iota(jnp.int32, (SUB, LANES), 0)
    blocks = -(-count * depth // SUB)
    wants = []
    for b in range(blocks):
        line = sub + SUB * b
        want = jnp.full((SUB, LANES), -2, jnp.int32)
        for q in range(count):
            inside = (line >= q * depth) & (line < (q + 1) * depth)
            want = jnp.where(inside, (line + (depth0 - q * depth)) * CODE + (first + q), want)
        wants.append(want)
    fills = (-1, LOWEST_FILL, -1, 0.0)

    def pull(i, carry):
        parts = [list(part) for part in carry]
        code = row(code_ref, i)
        values = [row(ref, i) for ref in sources]
        for b in range(blocks):
            hit = code == wants[b]
            for part, value in zip(parts, values):
                part[b] = jnp.where(hit, value, part[b])
        return tuple(tuple(part) for part in parts)

    start = tuple(
        (jnp.full((SUB, LANES), fill, ref.dtype),) * blocks for fill, ref in zip(fills, sources)
    )
    pulled = lax.fori_loop(0, all_lines, pull, start, unroll=8)
    for ref, parts in zip(packs, pulled):
        for b in range(blocks):
            ref[SUB * b : SUB * (b + 1), :] = parts[b]


def match_group(g, at, depth, packs, unroll):
    sub = lax.broadcasted_iota(jnp.int32, (SUB, LANES), 0)
    tiles = WIDTH // SUB
    marks = [sub + (g * WIDTH + SUB * q) for q in range(tiles)]
    start = (
        (jnp.full((SUB, LANES), LOWEST_FILL, jnp.float32),) * tiles,
        (jnp.full((SUB, LANES), KEY_LOW, jnp.int32),) * tiles,
        (jnp.zeros((SUB, LANES), jnp.float32),) * tiles,
    )

    def one(j, carry):
        pens, keys, gaps = (list(part) for part in carry)
        slot, pen, key, gap = (row(ref, at + j) for ref in packs)
        for q in range(tiles):
            hit = slot == marks[q]
            pens[q] = jnp.maximum(pens[q], jnp.where(hit, pen, LOWEST_FILL))
            keys[q] = jnp.maximum(keys[q], jnp.where(hit, key, KEY_LOW))
            gaps[q] = gaps[q] + jnp.where(hit, gap, 0.0)
        return tuple(pens), tuple(keys), tuple(gaps)

    if unroll == depth:
        for j in range(depth):
            start = one(j, start)
        return start
    return lax.fori_loop(0, depth, one, start, unroll=unroll)


def keep_group(accs, side, parts):
    for ref, part in zip(accs, parts):
        for q in range(WIDTH // SUB):
            at = side * WIDTH + q * SUB
            ref[at : at + SUB, :] = part[q]


def across(accs):
    pens, keys, gaps = (ref[...].T for ref in accs)
    return (
        jnp.max(pens, axis=0, keepdims=True),
        jnp.max(keys, axis=0, keepdims=True),
        jnp.sum(gaps, axis=0, keepdims=True),
    )


def project(wt, x_ref, off_ref, tile):
    cols = pl.ds(tile * TILE, TILE)
    per_tile = TILE // LANES
    offset = jnp.concatenate([row(off_ref, tile * per_tile + i) for i in range(per_tile)], axis=1)
    sub = lax.broadcasted_iota(jnp.int32, (SUB, TILE), 0)
    a, b, c = (part.astype(jnp.float32) for part in split3(offset))
    extra = jnp.where(sub == 0, a, jnp.where(sub == 1, b, jnp.where(sub == 2, c, 0.0)))
    extra = jnp.concatenate([extra, jnp.zeros((EXTRA - SUB, TILE), jnp.float32)], axis=0)
    x = jnp.concatenate([x_ref[:, cols], extra.astype(jnp.bfloat16)], axis=0)
    return jnp.dot(wt, x, preferred_element_type=jnp.float32)


def store_row(ref, tile, value):
    per_tile = TILE // LANES
    for i in range(per_tile):
        ref[pl.ds(tile * per_tile + i, 1), :] = value[:, i * LANES : (i + 1) * LANES]


def reduce_field(field, p_size, tile, pen_ref, gap_ref):
    low = [field[SUB * j : SUB * (j + 1)] for j in range(CHAINS)]
    for j in range(CHAINS, p_size // SUB):
        low[j % CHAINS] = jnp.minimum(low[j % CHAINS], field[SUB * j : SUB * (j + 1)])
    store_row(pen_ref, tile, -jnp.min(functools.reduce(jnp.minimum, low), axis=0, keepdims=True))
    store_row(gap_ref, tile, jnp.sum(field[p_size : p_size + SUB], axis=0, keepdims=True))


def prep_kernel(
    live_h, ns_h, nm_h, qw_h, sec_h, mst_h, off_h, jac_h, slot_h, face_h, rank_h,
    x_ref, wt_ref, nq_ref, off_ref, jl_ref, slot_ref, code_ref, key_ref, over_pen, over_key, over_gap, area_ref,
    live_s, ns_ref, nm_ref, qw_ref, jac_ref, face_ref, rank_ref, pen_ref, gap_ref, packs, accs, s_small, s_big,
):
    lines = slot_ref.shape[0]
    k_size, p_size = ns_ref.shape
    rows = x_ref.shape[1]

    small = [
        pltpu.make_async_copy(source, held, s_small.at[i])
        for i, (source, held) in enumerate((
            (slot_h, slot_ref), (live_h, live_s), (ns_h, ns_ref), (nm_h, nm_ref), (qw_h, qw_ref),
            (face_h, face_ref), (rank_h, rank_ref), (jac_h, jac_ref), (off_h, off_ref),
        ))
    ]
    for copy in small:
        copy.start()
    for base, source in ((0, sec_h), (k_size, mst_h)):
        for at in range(0, k_size, 2 * SUB):
            pltpu.make_async_copy(
                source.at[at : at + 2 * SUB, :], x_ref.at[base + at : base + at + 2 * SUB, :], s_big
            ).start(priority=1)
    for copy in small:
        copy.wait()

    row_id = (
        lax.broadcasted_iota(jnp.int32, (lines, LANES), 0) * LANES
        + lax.broadcasted_iota(jnp.int32, (lines, LANES), 1)
    )
    alive = row_id < live_s[...]
    group = jnp.where(alive, slot_ref[...] // WIDTH, -1)
    before = (
        lax.broadcasted_iota(jnp.int32, (lines, lines), 1)
        < lax.broadcasted_iota(jnp.int32, (lines, lines), 0)
    )
    before = jnp.where(before, 1.0, 0.0).astype(jnp.bfloat16)
    place = jnp.zeros((lines, LANES), jnp.float32)
    for g in range(0, GROUPS, 2):
        mine = [group == g, group == g + 1]
        seen = jnp.concatenate([jnp.where(m, 1.0, 0.0).astype(jnp.bfloat16) for m in mine], axis=1)
        found = jnp.dot(before, seen, preferred_element_type=jnp.float32)
        place = jnp.where(mine[0], found[:, :LANES], jnp.where(mine[1], found[:, LANES:], place))
    code = jnp.where(alive, place.astype(jnp.int32) * CODE + group, -1)
    code_ref[...] = code
    worst = jnp.max(code)

    w = jnp.concatenate([ns_ref[...], -nm_ref[...]], axis=0).astype(jnp.float32)
    qrow = qw_ref[...]
    wt = w.T
    qmat = jnp.broadcast_to(qrow, (LANES, p_size)).T
    v = jnp.sum(wt * qmat, axis=0, keepdims=True)
    qsum = jnp.sum(qmat, axis=0, keepdims=True)
    depth = wt_ref.shape[1]
    pick = lax.broadcasted_iota(jnp.int32, (EXTRA, depth), 0)
    column = lax.broadcasted_iota(jnp.int32, (p_size, depth - 2 * k_size), 1)
    wt_ref[0:p_size, 0 : 2 * k_size] = wt.astype(jnp.bfloat16)
    wt_ref[0:p_size, 2 * k_size :] = jnp.where(column < 3, 1.0, 0.0).astype(jnp.bfloat16)
    lane_row = lax.broadcasted_iota(jnp.int32, (1, LANES), 1)
    tail = jnp.where(lane_row < 3, qsum, 0.0)[:, : depth - 2 * k_size]
    a, b, c = (part.astype(jnp.float32) for part in split3(jnp.concatenate([v, tail], axis=1)))
    stacked = jnp.where(pick == 0, a, jnp.where(pick == 1, b, jnp.where(pick == 2, c, 0.0)))
    wt_ref[p_size:, :] = stacked.astype(jnp.bfloat16)
    scaled = ns_ref[...].astype(jnp.float32) * qrow
    top = scaled.astype(jnp.bfloat16)
    low = (scaled - top.astype(jnp.float32)).astype(jnp.bfloat16)
    nq_ref[...] = jnp.concatenate([top, low], axis=0)

    key_ref[...] = ((rank_ref[...] - 2) << 30) + (FACE_MASK - face_ref[...])
    jl = jnp.where(alive, jac_ref[...], 0.0)
    jl_ref[...] = jl
    area_ref[...] = jnp.sum(jl, axis=0, keepdims=True) * jnp.sum(qrow, axis=1, keepdims=True)
    over_pen[...] = jnp.full(over_pen.shape, LOWEST_FILL, jnp.float32)
    over_key[...] = jnp.full(over_key.shape, KEY_LOW, jnp.int32)
    over_gap[...] = jnp.zeros(over_gap.shape, jnp.float32)

    pltpu.make_async_copy(x_ref, x_ref, s_big).wait()

    @pl.when(worst >= DEPTH * CODE)
    def _():
        weights = wt_ref[...]
        work = face_ref
        line_id = lax.broadcasted_iota(jnp.int32, (lines, LANES), 0)
        work[...] = jnp.where(code >= DEPTH * CODE, line_id * CODE + (code & (CODE - 1)), -1)

        def one(mark):
            line, g = mark // CODE, mark & (CODE - 1)
            tile = line // (TILE // LANES)
            reduce_field(project(weights, x_ref, off_ref, tile), p_size, tile, pen_ref, gap_ref)
            here = row(work, line) == mark
            values = (
                row(slot_ref, line), row(pen_ref, line), row(key_ref, line), row(gap_ref, line) * row(jl_ref, line)
            )
            for ref, value in zip(packs, values):
                ref[0:SUB, :] = jnp.where(here, value, -1) if ref is packs[0] else value
            found = match_group(g, 0, 1, packs, 1)
            odd = jnp.full((SUB, LANES), g & 1, jnp.int32)
            for side in range(PER_ROW):
                keep_group(accs, side, [
                    [jnp.where(odd == side, x, fill) for x in part]
                    for part, fill in zip(found, (LOWEST_FILL, KEY_LOW, 0.0))
                ])
            pen, key, gap = across(accs)
            at = pl.ds(g // PER_ROW, 1)
            over_pen[at, :] = jnp.maximum(over_pen[at, :], pen)
            over_key[at, :] = jnp.maximum(over_key[at, :], key)
            over_gap[at, :] = over_gap[at, :] + gap
            left = jnp.where(work[...] == mark, -1, work[...])
            work[...] = left
            return jnp.max(left)

        lax.while_loop(lambda mark: mark >= 0, one, jnp.max(work[...]))


def main_kernel(
    n_dom, n_rep,
    x_ref, wt_ref, nq_ref, off_ref, jl_ref, slot_ref, code_ref, key_ref, over_pen, over_key, over_gap, area_ref,
    force_ref, out_pen, out_face, out_gap, out_mean,
    load_ref, pen_ref, gap_ref, packs, even_accs, odd_accs, raw_pen, raw_key, raw_gap,
    sp_sf, sp_si, ow_sf, ow_si, t1_s, t2_s, sp_f, sp_i, ow_f, ow_i, t1_d, t2_d,
    s_spf, r_spf, s_spi, r_spi, s_owf, r_owf, s_owi, r_owi, s_t1, r_t1, s_t2, r_t2, inside,
):
    dom = lax.axis_index("dom")
    rep = lax.axis_index("rep")
    k_size = force_ref.shape[0]
    rows = force_ref.shape[1]
    p_size = load_ref.shape[0]
    per_tile = TILE // LANES
    tiles = rows // TILE
    count = n_dom * n_rep
    me = dom * n_rep + rep

    def flat(d, r):
        return lax.rem(d + n_dom, n_dom) * n_rep + lax.rem(r + n_rep, n_rep)

    barrier = pltpu.get_barrier_semaphore()

    def signal(sem, first, last, step=1, at=0):
        def one(i, carry):
            pl.semaphore_signal(sem, inc=1, device_id=i * step + at, device_id_type=LOGICAL)
            return carry

        lax.fori_loop(first, last, one, 0)

    signal(barrier, me + 1, count)
    signal(barrier, dom * n_rep, me)
    signal(barrier, jnp.maximum(dom - 1, 0) * n_rep, dom * n_rep)

    wt = wt_ref[...]

    def wide_row(ref, tile):
        return jnp.concatenate([row(ref, tile * per_tile + i) for i in range(per_tile)], axis=1)

    pairs = count // 2
    pair = lax.div(me, 2)
    odd = lax.rem(rep, 2)
    mate = rep + 1 - 2 * odd

    def batch(step, carry):
        for i in range(UNROLL):
            tile = step * UNROLL + i
            cols = pl.ds(tile * TILE, TILE)
            field = project(wt, x_ref, off_ref, tile)
            for at in range(0, p_size, 2 * SUB):
                load_ref[at : at + 2 * SUB, cols] = jnp.minimum(field[at : at + 2 * SUB].astype(jnp.bfloat16), 0)
            reduce_field(field, p_size, tile, pen_ref, gap_ref)
        return carry

    lax.fori_loop(0, tiles // UNROLL, batch, 0)
    row_gap = gap_ref[...] * jl_ref[...]
    gap_ref[...] = row_gap
    total_gap = jnp.sum(jnp.sum(row_gap, axis=0, keepdims=True), axis=1, keepdims=True)
    total_area = jnp.sum(area_ref[...], axis=1, keepdims=True)
    lane = lax.broadcasted_iota(jnp.int32, (1, LANES), 1)
    t1_s[0:1, :] = jnp.where(lane == 0, total_gap, 0.0)
    t1_s[1:2, :] = jnp.where(lane == 0, total_area, 1.0)

    after = n_rep * jnp.where(dom == n_dom - 1, 0, 1)
    pl.semaphore_wait(barrier, me + (n_rep - 1 - rep) + after)
    first_copy = pltpu.make_async_remote_copy(
        src_ref=t1_s, dst_ref=t1_d, send_sem=s_t1, recv_sem=r_t1,
        device_id=flat(dom, mate), device_id_type=LOGICAL,
    )
    first_copy.start()
    last_dom = dom == n_dom - 1
    signal(inside, 0, jnp.where(last_dom, 0, pair), 2, odd)

    def pull_batch(first):
        pull_groups(first, BATCH, 0, DEPTH, code_ref, (slot_ref, pen_ref, key_ref, gap_ref), packs)

    def match_pair(first, i, accs, last_accs, over, at):
        g = first + i * PER_ROW
        keep_group(accs, 0, match_group(g, i * PER_ROW * DEPTH, DEPTH, packs, LOOP_UNROLL))
        if last_accs is not None:
            close_pair(last_accs, over, at)
        unroll = LOOP_UNROLL if last_accs is None else DEPTH
        keep_group(accs, 1, match_group(g + 1, (i * PER_ROW + 1) * DEPTH, DEPTH, packs, unroll))

    def close_pair(accs, over, at):
        pen, key, gap = across(accs)
        over, at = pl.ds(over, 1), pl.ds(at, 1)
        raw_pen[at, :] = jnp.maximum(pen, over_pen[over, :])
        raw_key[at, :] = jnp.maximum(key, over_key[over, :])
        raw_gap[at, :] = gap + over_gap[over, :]

    def decode(top, best):
        none = top < LOWEST_FILL * 0.5
        rank = jnp.where(none, -1, (best >> 30) + 2)
        face = jnp.where(none, FACE_LIMIT, FACE_MASK - (best & FACE_MASK))
        return rank, face

    pull_batch(OWN_GROUPS)
    match_pair(OWN_GROUPS, 0, even_accs, None, 0, 0)
    match_pair(OWN_GROUPS, 1, odd_accs, even_accs, OWN_ROWS, 0)
    close_pair(odd_accs, OWN_ROWS + 1, 1)
    part = slice(0, SPILL_ROWS)
    rank, face = decode(raw_pen[part, :], raw_key[part, :])
    sp_sf[0:SPILL_ROWS, :] = raw_pen[part, :]
    sp_sf[SPILL_ROWS:, :] = raw_gap[part, :]
    sp_si[0:SPILL_ROWS, :] = rank
    sp_si[SPILL_ROWS:, :] = face

    def spill_copy(j):
        where = flat(dom + 1, rep + j)
        return (
            pltpu.make_async_remote_copy(
                src_ref=sp_sf, dst_ref=sp_f.at[rep], send_sem=s_spf, recv_sem=r_spf,
                device_id=where, device_id_type=LOGICAL,
            ),
            pltpu.make_async_remote_copy(
                src_ref=sp_si, dst_ref=sp_i.at[rep], send_sem=s_spi, recv_sem=r_spi,
                device_id=where, device_id_type=LOGICAL,
            ),
        )

    for j in range(n_rep):
        for copy in spill_copy(j):
            copy.start()

    signal(inside, 0, jnp.where(last_dom, pair, 0), 2, odd)
    first_copy.wait_recv()
    both = t1_s[...] + t1_d[...]
    t2_s[...] = both
    t2_d[pair] = both

    def send_pairs(first, last):
        def one(other, carry):
            pltpu.make_async_remote_copy(
                src_ref=t2_s, dst_ref=t2_d.at[pair], send_sem=s_t2, recv_sem=r_t2,
                device_id=other * 2 + odd, device_id_type=LOGICAL,
            ).start()
            return carry

        lax.fori_loop(first, last, one, 0)

    send_pairs(0, pair)

    def send_up():
        @pl.when(pair < pairs - 1)
        def _():
            pl.semaphore_wait(inside, pairs - 1 - pair)

        send_pairs(pair + 1, pairs)

    quarter = lax.div(me * 4, count)
    turn = OWN_BATCHES - quarter - jnp.where(quarter >= 2, 1, 0)

    def own_scan(i, carry):
        @pl.when(i == turn)
        def _():
            send_up()

        first = i * BATCH
        last = lax.rem(2 * i + OWN_ROWS - 1, OWN_ROWS)
        pull_batch(first)
        match_pair(first, 0, even_accs, odd_accs, last, last)
        match_pair(first, 1, odd_accs, even_accs, 2 * i, 2 * i)
        return carry

    lax.fori_loop(0, OWN_BATCHES, own_scan, 0)
    close_pair(odd_accs, OWN_ROWS - 1, OWN_ROWS - 1)
    rank, face = decode(raw_pen[...], raw_key[...])
    ow_sf[0] = raw_pen[...]
    ow_sf[1] = raw_gap[...]
    ow_si[0] = rank
    ow_si[1] = face

    def own_copy(j):
        where = flat(dom, rep + j)
        return (
            pltpu.make_async_remote_copy(
                src_ref=ow_sf, dst_ref=ow_f.at[rep], send_sem=s_owf, recv_sem=r_owf,
                device_id=where, device_id_type=LOGICAL,
            ),
            pltpu.make_async_remote_copy(
                src_ref=ow_si, dst_ref=ow_i.at[rep], send_sem=s_owi, recv_sem=r_owi,
                device_id=where, device_id_type=LOGICAL,
            ),
        )

    for j in range(1, n_rep):
        for copy in own_copy(j):
            copy.start()
    ow_f[rep] = ow_sf[...]
    ow_i[rep] = ow_si[...]

    @pl.when(turn >= OWN_BATCHES)
    def _():
        send_up()

    nq = nq_ref[...]

    def push(step, carry):
        for i in range(FORCE_UNROLL):
            tile = step * FORCE_UNROLL + i
            cols = pl.ds(tile * TILE, TILE)
            force = jnp.dot(nq, load_ref[:, cols], preferred_element_type=jnp.float32)
            scale = wide_row(jl_ref, tile)[0:1] * -PENALTY
            force_ref[:, cols] = ((force[:k_size] + force[k_size:]) * scale).astype(jnp.bfloat16)
        return carry

    lax.fori_loop(0, tiles // FORCE_UNROLL, push, 0)

    def encode(rank, face):
        return jnp.where(rank < 0, KEY_LOW, ((rank - 2) << 30) + (FACE_MASK - face))

    def settle(ref, sem):
        pltpu.make_async_copy(ref, ref, sem).wait()

    settle(ow_f.at[pl.ds(0, n_rep - 1)], r_owf)
    settle(ow_i.at[pl.ds(0, n_rep - 1)], r_owi)
    pen_o, gap_o = ow_f[0, 0], ow_f[0, 1]
    key_o = encode(ow_i[0, 0], ow_i[0, 1])
    for r in range(1, n_rep):
        pen_o = jnp.maximum(pen_o, ow_f[r, 0])
        gap_o = gap_o + ow_f[r, 1]
        key_o = jnp.maximum(key_o, encode(ow_i[r, 0], ow_i[r, 1]))

    settle(sp_f, s_spf)
    settle(sp_i, s_spi)
    settle(ow_f.at[pl.ds(0, n_rep - 1)], s_owf)
    settle(ow_i.at[pl.ds(0, n_rep - 1)], s_owi)
    first_copy.wait_send()
    settle(t2_d.at[pl.ds(0, pairs - 1)], s_t2)

    settle(t2_d.at[pl.ds(0, pairs - 1)], r_t2)
    settle(sp_f, r_spf)
    settle(sp_i, r_spi)
    whole = jnp.sum(t2_d[...], axis=0)
    out_mean[...] = (whole[0:1] / whole[1:2])[:, 0:1]

    g = SPILL_ROWS
    pen_s, gap_s = sp_f[0, 0:g], sp_f[0, g:]
    key_s = encode(sp_i[0, 0:g], sp_i[0, g:])
    for r in range(1, n_rep):
        pen_s = jnp.maximum(pen_s, sp_f[r, 0:g])
        gap_s = gap_s + sp_f[r, g:]
        key_s = jnp.maximum(key_s, encode(sp_i[r, 0:g], sp_i[r, g:]))

    def finish(at, pen, key, gap):
        none = pen < LOWEST_FILL * 0.5
        out_pen[at, :] = jnp.where(none, 0.0, pen)
        out_face[at, :] = jnp.where(none, -1, FACE_MASK - (key & FACE_MASK))
        out_gap[at, :] = jnp.where(none, 0.0, gap)

    finish(
        slice(0, g), jnp.maximum(pen_o[:g], pen_s), jnp.maximum(key_o[:g], key_s), gap_o[:g] + gap_s
    )
    finish(slice(g, OWN_ROWS), pen_o[g:], key_o[g:], gap_o[g:])


def finish_kernel(force_ref, pen_ref, face_ref, gap_ref, mean_ref, force_h, pen_h, face_h, gap_h, mean_h, sems, s_force):
    copies = [
        pltpu.make_async_copy(held, out, sems.at[i])
        for i, (held, out) in enumerate((
            (pen_ref, pen_h), (face_ref, face_h), (gap_ref, gap_h), (mean_ref, mean_h)
        ))
    ]
    for at in range(0, force_ref.shape[0], SUB):
        part = (slice(at, at + SUB), slice(None))
        pltpu.make_async_copy(force_ref.at[part], force_h.at[part], s_force).start()
    for copy in copies:
        copy.start()
    for copy in copies:
        copy.wait()
    pltpu.make_async_copy(force_ref, force_h, s_force).wait()


def solution(mesh):
    n_dom, n_rep = mesh.shape["dom"], mesh.shape["rep"]
    vmem = pl.BlockSpec(memory_space=pltpu.VMEM)
    anywhere = pl.BlockSpec(memory_space=pl.ANY)
    dma = pltpu.SemaphoreType.DMA

    def kept(x):
        return pltpu.with_memory_space_constraint(x, pltpu.VMEM)

    def streamed(x):
        return pltpu.with_memory_space_constraint(x, pltpu.HBM)

    def shards(ns, nm, sec, mst, off, qw, jac, slot, face, rank, live):
        k_size, p_size = ns.shape
        rows = sec.shape[1]
        lines = rows // LANES
        depth = 2 * k_size + EXTRA
        f32, i32, bf16 = jnp.float32, jnp.int32, jnp.bfloat16

        off, jac, slot, face, rank = (x.reshape(lines, LANES) for x in (off, jac, slot, face, rank))

        def packs(deep):
            return [pltpu.VMEM((deep + SUB, LANES), t) for t in (i32, f32, i32, f32)]

        def lanes():
            return [pltpu.VMEM((LANES, LANES), t) for t in (f32, i32, f32)]

        held = pl.pallas_call(
            prep_kernel,
            out_shape=(
                pltpu.VMEM((2 * k_size, rows), bf16),
                pltpu.VMEM((p_size + EXTRA, depth), bf16),
                pltpu.VMEM((2 * k_size, p_size), bf16),
                pltpu.VMEM((lines, LANES), f32),
                pltpu.VMEM((lines, LANES), f32),
                pltpu.VMEM((lines, LANES), i32),
                pltpu.VMEM((lines, LANES), i32),
                pltpu.VMEM((lines, LANES), i32),
                pltpu.VMEM((ALL_ROWS, LANES), f32),
                pltpu.VMEM((ALL_ROWS, LANES), i32),
                pltpu.VMEM((ALL_ROWS, LANES), f32),
                pltpu.VMEM((1, LANES), f32),
            ),
            in_specs=[anywhere] * 11,
            out_specs=(vmem,) * 12,
            scratch_shapes=[
                pltpu.VMEM((1, 1), i32),
                pltpu.VMEM((k_size, p_size), bf16),
                pltpu.VMEM((k_size, p_size), bf16),
                pltpu.VMEM((1, p_size), f32),
                pltpu.VMEM((lines, LANES), f32),
                pltpu.VMEM((lines, LANES), i32),
                pltpu.VMEM((lines, LANES), i32),
                pltpu.VMEM((lines, LANES), f32),
                pltpu.VMEM((lines, LANES), f32),
                packs(SUB),
                lanes(),
                dma((9,)),
                dma,
            ],
            compiler_params=pltpu.CompilerParams(vmem_limit_bytes=VMEM_LIMIT),
        )(
            live.reshape(1, 1),
            *(streamed(x) for x in (ns, nm, qw.reshape(1, p_size), sec, mst, off, jac, slot, face, rank)),
        )

        spill = (2 * SPILL_ROWS, LANES)
        own = (2, OWN_ROWS, LANES)
        pairs = n_dom * n_rep // 2
        results = pl.pallas_call(
            functools.partial(main_kernel, n_dom, n_rep),
            out_shape=(
                pltpu.VMEM((k_size, rows), bf16),
                pltpu.VMEM((OWN_ROWS, LANES), f32),
                pltpu.VMEM((OWN_ROWS, LANES), i32),
                pltpu.VMEM((OWN_ROWS, LANES), f32),
                pltpu.VMEM((1, 1), f32),
            ),
            in_specs=[vmem] * 12,
            out_specs=(vmem,) * 5,
            scratch_shapes=[
                pltpu.VMEM((p_size, rows), bf16),
                pltpu.VMEM((lines, LANES), f32),
                pltpu.VMEM((lines, LANES), f32),
                packs(BATCH * DEPTH),
                lanes(),
                lanes(),
                pltpu.VMEM((OWN_ROWS, LANES), f32),
                pltpu.VMEM((OWN_ROWS, LANES), i32),
                pltpu.VMEM((OWN_ROWS, LANES), f32),
                pltpu.VMEM(spill, f32),
                pltpu.VMEM(spill, i32),
                pltpu.VMEM(own, f32),
                pltpu.VMEM(own, i32),
                pltpu.VMEM((2, LANES), f32),
                pltpu.VMEM((2, LANES), f32),
                pltpu.VMEM((n_rep,) + spill, f32),
                pltpu.VMEM((n_rep,) + spill, i32),
                pltpu.VMEM((n_rep,) + own, f32),
                pltpu.VMEM((n_rep,) + own, i32),
                pltpu.VMEM((2, LANES), f32),
                pltpu.VMEM((pairs, 2, LANES), f32),
            ] + [dma] * 12 + [pltpu.SemaphoreType.REGULAR],
            compiler_params=pltpu.CompilerParams(
                collective_id=0, has_side_effects=True, vmem_limit_bytes=VMEM_LIMIT
            ),
        )(*(kept(x) for x in held))

        force, seg_pen, seg_face, seg_gap, mean = pl.pallas_call(
            finish_kernel,
            out_shape=tuple(jax.ShapeDtypeStruct(x.shape, x.dtype) for x in results),
            in_specs=[vmem] * 5,
            out_specs=(anywhere,) * 5,
            scratch_shapes=[dma((4,)), dma],
            compiler_params=pltpu.CompilerParams(vmem_limit_bytes=VMEM_LIMIT),
        )(*(kept(x) for x in results))
        seg_pen, seg_face, seg_gap = (x.reshape(SEG_DEV) for x in (seg_pen, seg_face, seg_gap))
        return force, seg_pen, seg_face, seg_gap, mean.reshape(())

    rows_spec, wide_spec = P(("dom", "rep")), P(None, ("dom", "rep"))
    return jax.shard_map(
        shards,
        mesh=mesh,
        in_specs=(P(), P(), wide_spec, wide_spec, rows_spec, P()) + (rows_spec,) * 5,
        out_specs=(wide_spec, P("dom"), P("dom"), P("dom"), P()),
        check_vma=False,
    )
```
